32 devices in a mesh: blk: 16 (over z, x, core), rep: 2 (over y).
Axes of the slice: x: 2, y: 2, z: 4, core: 2. Of those that a mesh axis runs over, the one named last changes fastest.
Arguments:
- captions: bfloat16 [6144, 768], P(('blk', 'rep')), may hold values from -512 to 512
- images: bfloat16 [6144, 768], P(('blk', 'rep')), may hold values from -512 to 512
- positives: int32 [6144], P(('blk', 'rep')), may hold values from 0 to 6143, each once
- valid: int32 [6144], P(('blk', 'rep')), may hold values from 0 to 1, as said below
Outputs:
- caption_loss: float32 [6144], P(('blk', 'rep'))
- image_loss: float32 [6144], P(('blk', 'rep'))
- loss: float32 [], replicated
The draws below stay inside these ranges and needn't reach their ends.
Inputs may be any that keep to these rules, and one draw needn't show every extreme that they name: `positives`: each image row is the positive of exactly one caption; a program may pack several of these indices into one sent element. `valid`: the last image row is always real; a program may pack several of these flags into one sent element.
All inputs are finite; a program needn't handle non-finite values.
Results may differ from the reference program's by a relative error of at most 0.0003.
Values may be sent and summed in bfloat16 or wider, within the bound.
A program may use at most 128 MiB of HBM per device.

```python
import math
import jax
import jax.numpy as jnp
from jax import lax

E = 768
PAIRS = 6144


def pair_fields(key):
    base_key = jax.random.fold_in(key, 11)
    caption_key, image_key = jax.random.split(base_key, 2)
    caption_rows = jax.random.normal(caption_key, (PAIRS, E), jnp.float32)
    image_rows = jax.random.normal(image_key, (PAIRS, E), jnp.float32) * (3.0 / math.sqrt(E))
    return (caption_rows.astype(jnp.bfloat16), image_rows.astype(jnp.bfloat16))


def draw_captions(key, part):
    return pair_fields(key)[0]


def draw_images(key, part):
    return pair_fields(key)[1]


def draw_valid(key, part):
    position = jax.lax.iota(jnp.int32, PAIRS)
    rolled = jax.random.randint(jax.random.fold_in(key, 23), (PAIRS,), 0, 4 * PAIRS)
    flags = (rolled < PAIRS + 2 * position).astype(jnp.int32)
    return flags.at[PAIRS - 1].set(1)


def setup_inputs(seed: int = 0) -> dict:
    keys = jax.random.split(jax.random.key(seed), 5)
    captions = draw_captions(jax.random.fold_in(keys[4], 71), 0)
    images = draw_images(jax.random.fold_in(keys[4], 71), 0)
    positives = jax.random.permutation(keys[2], PAIRS).astype(jnp.int32)
    valid = draw_valid(jax.random.fold_in(keys[4], 71), 0)
    return {"captions": captions, "images": images, "positives": positives, "valid": valid}


very_low = -1.0e30


def reference(captions, images, positives, valid):
    pair_count = captions.shape[0]
    block_size = math.gcd(pair_count, 1024)
    image_ok = valid.astype(jnp.float32)
    caption_ok = jnp.take(image_ok, positives, axis=0)
    usable = image_ok[None, :] > 0
    columns = lax.iota(jnp.int32, pair_count)

    def one_block(running, block_index):
        column_peak, column_total, column_match = running
        offset = (block_index * block_size).astype(jnp.int32)
        caption_rows = lax.dynamic_slice_in_dim(captions, offset, block_size)
        match_rows = lax.dynamic_slice_in_dim(positives, offset, block_size)
        ok_rows = lax.dynamic_slice_in_dim(caption_ok, offset, block_size)
        scores = jnp.dot(caption_rows, images.T, preferred_element_type=jnp.float32)
        is_positive = match_rows[:, None] == columns[None, :]
        picked = jnp.where(is_positive, scores, 0.0)
        highest = jnp.max(jnp.where(usable, scores, very_low), axis=1)
        row_total = jnp.sum(jnp.where(usable, jnp.exp(scores - highest[:, None]), 0.0), axis=1)
        row_loss = ok_rows * (highest + jnp.log(row_total) - jnp.sum(picked, axis=1))
        caption_live = ok_rows[:, None] > 0
        column_high = jnp.max(jnp.where(caption_live, scores, very_low), axis=0)
        renewed = jnp.maximum(column_peak, column_high)
        powers = jnp.where(caption_live, jnp.exp(scores - renewed[None, :]), 0.0)
        column_total = column_total * jnp.exp(column_peak - renewed) + jnp.sum(powers, axis=0)
        column_match = column_match + jnp.sum(picked, axis=0)
        return (renewed, column_total, column_match), row_loss

    started = (jnp.full((pair_count,), very_low, jnp.float32), jnp.zeros((pair_count,), jnp.float32), jnp.zeros((pair_count,), jnp.float32))
    finished, row_losses = lax.scan(one_block, started, jnp.arange(pair_count // block_size, dtype=jnp.int32))
    caption_loss = row_losses.reshape(pair_count)
    image_loss = image_ok * (finished[0] + jnp.log(finished[1]) - finished[2])
    loss = (jnp.sum(caption_loss) + jnp.sum(image_loss)) / (2.0 * jnp.sum(image_ok))
    return (caption_loss, image_loss, loss)
```

```python
import functools

import jax
import jax.numpy as jnp
from jax import lax
from jax.experimental import pallas as pl
from jax.experimental.pallas import tpu as pltpu
from jax.sharding import PartitionSpec as P

very_low = -1e30
floor = -1e29
IMAGE_PIECES = 4
CAPTION_PIECES = 4
LAST_PIECES = 2


def grid_of(blk, rep):
    chips = (blk // 2) * rep
    planes = 1
    while (planes * 2) ** 2 <= chips and (blk // 2) % (planes * 2) == 0:
        planes *= 2
    return planes, blk // 2 // planes


def mod(a, b):
    return a & (b - 1) if b & (b - 1) == 0 else lax.rem(a, b)


def div(a, b):
    return a >> (b.bit_length() - 1) if b & (b - 1) == 0 else lax.div(a, b)


def kernel(
    blk, rep, cap_ref, img_ref, pos_ref, val_ref, closs_ref, iloss_ref, loss_ref,
    mine, caps, imgs, vbuf, image_ok, image_ids, target, caption_ok, own_ok,
    row_peak, row_total, row_match, colacc, rowsend, rowrecv, colsend, colrecv, part, closs, iloss,
    loc_sem, out_sem, img_recv, imgz_send, imgv_send, imgd_send, cap_recv, capz_send, capr_send,
    val_send, val_recv, plane_send, plane_recv,
    row_send, row_recv, col_send, col_recv, part_send, part_recv,
):
    U, V = grid_of(blk, rep)
    N = blk * rep
    G = N // U
    H = U // 2
    B = V * 2
    n, width = cap_ref.shape
    C = B * n
    b, r = lax.axis_index("blk"), lax.axis_index("rep")
    c = mod(b, 2)
    u = div(b, 2 * V)
    v = mod(div(b, 2), V)
    me = b * rep + r
    g = mod(me, G)
    half, h = div(u, H), mod(u, H)
    near = jnp.where(u > 2 * h, 1, 0)
    far = 1 - near
    keeps_own = div(u, 2) == h

    def member(uu, vv, cc, rr):
        return ((uu * V + vv) * 2 + cc) * rep + rr

    def remote(src, dst, ss, rs, to):
        return pltpu.make_async_remote_copy(
            src_ref=src, dst_ref=dst, send_sem=ss, recv_sem=rs, device_id=to,
            device_id_type=pl.DeviceIdType.LOGICAL,
        )

    barrier = pltpu.get_barrier_semaphore()
    others = [u * G + mod(g + k, G) for k in range(1, G)]
    others += [mod(u + k, U) * G + g for k in range(1, U)]
    for to in others:
        pl.semaphore_signal(
            barrier, inc=1, device_id=to, device_id_type=pl.DeviceIdType.LOGICAL
        )

    load_val = pltpu.make_async_copy(val_ref, vbuf.at[me, 0], loc_sem.at[0])
    load_pos = pltpu.make_async_copy(pos_ref, vbuf.at[me, 1], loc_sem.at[1])
    load_img = pltpu.make_async_copy(img_ref, imgs.at[h, v, c], loc_sem.at[2])
    load_cap = pltpu.make_async_copy(cap_ref, mine, loc_sem.at[3])
    keep_cap = pltpu.make_async_copy(cap_ref, caps.at[mod(u, 2), r], loc_sem.at[4])
    load_val.start()
    load_pos.start()
    load_img.start()
    load_cap.start()

    @pl.when(keeps_own)
    def _():
        keep_cap.start()

    load_val.wait()
    load_pos.wait()
    load_img.wait()
    load_cap.wait()

    @pl.when(keeps_own)
    def _():
        keep_cap.wait()

    pl.semaphore_wait(barrier, len(others))

    def image_rows(k):
        return pl.ds(k * (n // IMAGE_PIECES), n // IMAGE_PIECES)

    def caption_rows(k):
        return pl.ds(k * (n // CAPTION_PIECES), n // CAPTION_PIECES)

    def img_copy(i, vv, cc, k, ss, to):
        block = imgs.at[i, vv, cc, image_rows(k)]
        return remote(block, block, ss, img_recv.at[((i * V + vv) * 2 + cc) * IMAGE_PIECES + k], to)

    def img_along(d, k):
        to = member(half * H + mod(h + d, H), v, c, r)
        return img_copy(h, v, c, k, imgz_send.at[d * IMAGE_PIECES + k], to)

    def img_across(i, d, k):
        to = member(u, mod(v + d, V), c, r)
        return img_copy(i, v, c, k, imgv_send.at[(i * V + d) * IMAGE_PIECES + k], to)

    def img_beside(i, vv, k):
        to = member(u, v, 1 - c, r)
        return img_copy(i, vv, c, k, imgd_send.at[(i * V + vv) * IMAGE_PIECES + k], to)

    def img_arrival(i, vv, cc, k):
        return img_copy(i, vv, cc, k, imgd_send.at[0], member(u, v, 1 - c, r))

    def cap_along(t, k):
        rows = caption_rows(k)
        return remote(
            mine.at[rows], caps.at[mod(u, 2), r, rows], capz_send.at[t * CAPTION_PIECES + k],
            cap_recv.at[(mod(u, 2) * rep + r) * CAPTION_PIECES + k],
            member(t * H + div(u, 2), v, c, r),
        )

    def cap_across(q, d, k):
        block = caps.at[q, r, caption_rows(k)]
        return remote(
            block, block, capr_send.at[(q * rep + d) * CAPTION_PIECES + k],
            cap_recv.at[(q * rep + r) * CAPTION_PIECES + k], member(u, v, c, mod(r + d, rep)),
        )

    def cap_arrival(q, rr, k):
        block = caps.at[q, rr, caption_rows(k)]
        return remote(
            block, block, capr_send.at[0], cap_recv.at[(q * rep + rr) * CAPTION_PIECES + k],
            member(u, v, 1 - c, r),
        )

    def val_copy(k):
        return remote(
            vbuf.at[me], vbuf.at[me], val_send.at[k], val_recv.at[g], u * G + mod(g + k, G)
        )

    def plane_copy(k):
        rows = pl.ds(u * G, G)
        return remote(
            vbuf.at[rows], vbuf.at[rows], plane_send.at[k], plane_recv.at[u],
            mod(u + k, U) * G + g,
        )

    for k in range(1, G):
        val_copy(k).start()
    for k in range(IMAGE_PIECES):
        for d in range(1, H):
            img_along(d, k).start()
        for d in range(1, V):
            img_across(h, d, k).start()
        img_beside(h, v, k).start()
    for k in range(CAPTION_PIECES):
        for t in range(2):
            @pl.when(t * H + div(u, 2) != u)
            def _():
                cap_along(t, k).start()

        @pl.when(keeps_own)
        def _():
            for d in range(1, rep):
                cap_across(mod(u, 2), d, k).start()

    for k in range(1, G):
        slot = mod(g + k, G)
        remote(
            vbuf.at[me], vbuf.at[u * G + slot], val_send.at[k], val_recv.at[slot], u * G + slot
        ).wait_recv()
    for k in range(1, U):
        plane_copy(k).start()

    def relay_images(k):
        for d in range(1, H):
            i = mod(h + d, H)
            img_arrival(i, v, c, k).wait_recv()
            for dv in range(1, V):
                img_across(i, dv, k).start()
            img_beside(i, v, k).start()

    def relay_beside(i, k):
        for dv in range(1, V):
            vv = mod(v + dv, V)
            img_arrival(i, vv, c, k).wait_recv()
            img_beside(i, vv, k).start()

    def relay_captions(q, k):
        cap_arrival(q, r, k).wait_recv()
        for d in range(1, rep):
            cap_across(q, d, k).start()

    for k in range(IMAGE_PIECES):
        relay_images(k)
        relay_beside(h, k)
        if k < CAPTION_PIECES:
            @pl.when(jnp.logical_not(keeps_own))
            def _():
                relay_captions(near, k)

    for k in range(IMAGE_PIECES, CAPTION_PIECES):
        @pl.when(jnp.logical_not(keeps_own))
        def _():
            relay_captions(near, k)

    for k in range(1, U):
        slot = mod(u + k, U)
        rows = pl.ds(slot * G, G)
        remote(
            vbuf.at[rows], vbuf.at[rows], plane_send.at[k], plane_recv.at[slot], slot * G + g
        ).wait_recv()

    eye = lax.broadcasted_iota(jnp.int32, (n, n), 0) == lax.broadcasted_iota(jnp.int32, (n, n), 1)

    def to_column(row):
        return jnp.sum(jnp.where(eye, row, 0.0), axis=1, keepdims=True)

    def to_row(column):
        return jnp.sum(jnp.where(eye, column, 0.0), axis=0, keepdims=True)

    flags = vbuf[:, 0, 0, :].astype(jnp.float32)
    image_total = jnp.sum(jnp.sum(flags, axis=1, keepdims=True), axis=0, keepdims=True)
    starts = lax.broadcasted_iota(jnp.int32, (n, N), 1) * n
    lanes = lax.broadcasted_iota(jnp.int32, (n, n), 1)

    def caption_state(row):
        aim = to_column(row.astype(jnp.float32)).astype(jnp.int32)
        inside = (aim >= starts) & (aim < starts + n)
        picked = jnp.dot(
            jnp.where(inside, 1.0, 0.0).astype(jnp.bfloat16), flags.astype(jnp.bfloat16),
            preferred_element_type=jnp.float32,
        )
        start = jnp.sum(jnp.where(inside, starts, 0).astype(jnp.float32), axis=1, keepdims=True)
        low = aim - start.astype(jnp.int32)
        ok = jnp.sum(jnp.where(lanes == low, picked, 0.0), axis=1, keepdims=True)
        return aim, ok

    @pl.loop(0, 2 * rep)
    def _(s):
        aim, ok = caption_state(vbuf[member(2 * h + div(s, rep), v, c, mod(s, rep)), 1])
        target[s] = aim
        caption_ok[s] = ok

    own_ok[...] = to_row(caption_state(vbuf[me, 1])[1])
    for i in range(H):
        base = (half * H + i) * G
        for s in range(B):
            at = base + s * rep + r
            cols = slice(s * n, (s + 1) * n)
            image_ok[i, :, cols] = vbuf[at, 0].astype(jnp.float32)
            image_ids[i, :, cols] = at * n + lax.broadcasted_iota(jnp.int32, (1, n), 1)
    colacc[:, 0:1, :] = jnp.full((H, 1, C), floor, jnp.float32)
    colacc[:, 1:3, :] = jnp.zeros((H, 2, C), jnp.float32)
    row_peak[...] = jnp.full(row_peak.shape, floor, jnp.float32)
    row_total[...] = jnp.zeros(row_total.shape, jnp.float32)
    row_match[...] = jnp.zeros(row_match.shape, jnp.float32)

    def score(q, rr, i, start, rows):
        s = q * rep + rr
        part_rows = pl.ds(start, rows)
        scores = lax.dot_general(
            caps[q, rr, part_rows], imgs[i].reshape(C, width), (((1,), (1,)), ((), ())),
            preferred_element_type=jnp.float32,
        )
        usable = jnp.where(image_ok[i] > 0, scores, very_low)
        old = row_peak[s, part_rows]
        peak = jnp.maximum(jnp.max(usable, axis=1, keepdims=True), old)
        total = jnp.sum(jnp.exp(usable - peak), axis=1, keepdims=True)
        row_total[s, part_rows] = row_total[s, part_rows] * jnp.exp(old - peak) + total
        row_peak[s, part_rows] = peak
        picked = jnp.where(target[s, part_rows] == image_ids[i], scores, 0.0)
        row_match[s, part_rows] = row_match[s, part_rows] + jnp.sum(picked, axis=1, keepdims=True)
        live = jnp.where(caption_ok[s, part_rows] > 0, scores, very_low)
        old_peak = colacc[i, 0:1, :]
        peak = jnp.maximum(jnp.max(live, axis=0, keepdims=True), old_peak)
        total = jnp.sum(jnp.exp(live - peak), axis=0, keepdims=True)
        colacc[i, 1:2, :] = colacc[i, 1:2, :] * jnp.exp(old_peak - peak) + total
        colacc[i, 0:1, :] = peak
        colacc[i, 2:3, :] = colacc[i, 2:3, :] + jnp.sum(picked, axis=0, keepdims=True)

    def wait_beside(i):
        for vv in range(V):
            for k in range(IMAGE_PIECES):
                img_arrival(i, vv, 1 - c, k).wait_recv()

    wait_beside(h)

    @pl.loop(0, rep)
    def _(d):
        rr = mod(r + d, rep)

        @pl.when(d > 0)
        def _():
            for k in range(CAPTION_PIECES):
                cap_arrival(near, rr, k).wait_recv()
        score(near, rr, h, 0, n)

    for k in range(CAPTION_PIECES):
        relay_captions(far, k)
        if k < IMAGE_PIECES:
            for d in range(1, H):
                relay_beside(mod(h + d, H), k)
    for k in range(CAPTION_PIECES, IMAGE_PIECES):
        for d in range(1, H):
            relay_beside(mod(h + d, H), k)

    @pl.loop(0, 1 + (H - 1) * (rep + 1))
    def _(t):
        first = t == 0
        e = jnp.maximum(t - 1, 0)
        i = mod(h + jnp.where(first, 0, 1 + div(e, rep + 1)), H)
        d = jnp.where(first, rep, lax.rem(e, rep + 1))

        @pl.when(jnp.logical_not(first) & (d == 0))
        def _():
            wait_beside(i)
        score(jnp.where(d == rep, far, near), mod(r + d, rep), i, 0, n)

    def row_copy(s):
        q, rr = div(s, rep), mod(s, rep)
        return remote(
            rowsend.at[s], rowrecv.at[half * rep + r], row_send.at[s],
            row_recv.at[half * rep + r], member(2 * h + q, v, c, rr),
        )

    def send_rows(s):
        rowsend[s, 0:1, :] = to_row(row_peak[s])
        rowsend[s, 1:2, :] = to_row(row_total[s])
        rowsend[s, 2:3, :] = to_row(row_match[s])

        @pl.when((2 * h + div(s, rep) != u) | (mod(s, rep) != r))
        def _():
            row_copy(s).start()

        @pl.when((2 * h + div(s, rep) == u) & (mod(s, rep) == r))
        def _():
            rowrecv[half * rep + r] = rowsend[s]

    @pl.loop(0, rep + 1)
    def _(d):
        send_rows(jnp.where(d == rep, far, near) * rep + mod(r + d, rep))

    @pl.loop(1, rep)
    def _(d):
        rr = mod(r + d, rep)

        @pl.loop(0, LAST_PIECES)
        def _(k):
            for j in range(CAPTION_PIECES // LAST_PIECES):
                cap_arrival(far, rr, k * (CAPTION_PIECES // LAST_PIECES) + j).wait_recv()

            @pl.loop(0, H)
            def _(e):
                score(far, rr, mod(h + e, H), k * (n // LAST_PIECES), n // LAST_PIECES)
        send_rows(far * rep + rr)

    for i in range(H):
        for s in range(B):
            colsend[i * B + s, 0:3, :] = colacc[i, 0:3, s * n : (s + 1) * n]

    own_at = h * B + v * 2 + c

    def col_copy(k):
        slot = mod(own_at + k, H * B)
        i, s = div(slot, B), mod(slot, B)
        return remote(
            colsend.at[slot], colrecv.at[own_at], col_send.at[k], col_recv.at[own_at],
            (half * H + i) * G + s * rep + r,
        )

    for k in range(1, H * B):
        col_copy(k).start()
    colrecv[own_at] = colsend[own_at]

    def joined(parts, count):
        peak = parts[0, 0:1, :]
        for s in range(1, count):
            peak = jnp.maximum(peak, parts[s, 0:1, :])
        total = jnp.zeros_like(peak)
        match = jnp.zeros_like(peak)
        for s in range(count):
            total += parts[s, 1:2, :] * jnp.exp(parts[s, 0:1, :] - peak)
            match += parts[s, 2:3, :]
        return peak + jnp.log(total) - match

    for t in range(2):
        for rr in range(rep):
            @pl.when((t * H + div(u, 2) != u) | (rr != r))
            def _():
                remote(
                    rowsend.at[0], rowrecv.at[t * rep + rr], row_send.at[0],
                    row_recv.at[t * rep + rr], member(u, v, 1 - c, r),
                ).wait_recv()
    caption_loss = own_ok[...] * joined(rowrecv, 2 * rep)
    closs[...] = caption_loss
    put_caption = pltpu.make_async_copy(closs, closs_ref, out_sem.at[0])
    put_caption.start()
    for k in range(1, H * B):
        slot = mod(own_at + k, H * B)
        remote(
            colsend.at[slot], colrecv.at[slot], col_send.at[k], col_recv.at[slot],
            member(u, v, 1 - c, r),
        ).wait_recv()
    image_loss = vbuf[me, 0].astype(jnp.float32) * joined(colrecv, H * B)
    iloss[...] = image_loss
    put_image = pltpu.make_async_copy(iloss, iloss_ref, out_sem.at[1])
    put_image.start()
    own_sum = jnp.sum(caption_loss + image_loss, axis=1, keepdims=True)
    part[me] = jnp.broadcast_to(own_sum, (1, 128))

    def part_copy(k):
        return remote(
            part.at[me], part.at[me], part_send.at[k], part_recv.at[me], mod(me + k, N)
        )

    @pl.loop(1, N)
    def _(k):
        part_copy(k).start()

    for k in range(1, G):
        val_copy(k).wait_send()
    for k in range(1, U):
        plane_copy(k).wait_send()
    for k in range(IMAGE_PIECES):
        for d in range(1, H):
            img_along(d, k).wait_send()
        for i in range(H):
            for d in range(1, V):
                img_across(i, d, k).wait_send()
            for vv in range(V):
                img_beside(i, vv, k).wait_send()
    for k in range(CAPTION_PIECES):
        for t in range(2):
            @pl.when(t * H + div(u, 2) != u)
            def _():
                cap_along(t, k).wait_send()
        for q in range(2):
            for d in range(1, rep):
                cap_across(q, d, k).wait_send()

    @pl.loop(0, 2 * rep)
    def _(s):
        @pl.when((2 * h + div(s, rep) != u) | (mod(s, rep) != r))
        def _():
            row_copy(s).wait_send()
    for k in range(1, H * B):
        col_copy(k).wait_send()
    put_caption.wait()
    put_image.wait()

    @pl.loop(1, N)
    def _(k):
        slot = mod(me + k, N)
        remote(
            part.at[slot], part.at[slot], part_send.at[k], part_recv.at[slot], slot
        ).wait_recv()

    whole = jnp.sum(part[:, 0, :], axis=0, keepdims=True)
    loss_ref[...] = whole[:, 0:1] / (2.0 * image_total)

    @pl.loop(1, N)
    def _(k):
        part_copy(k).wait_send()


def local(blk, rep, captions, images, positives, valid):
    n, width = captions.shape
    U, V = grid_of(blk, rep)
    N = blk * rep
    G = N // U
    H, B = U // 2, V * 2
    C = B * n
    f32, i32 = jnp.float32, jnp.int32
    dma = lambda count: pltpu.SemaphoreType.DMA((count,))
    vmem = pl.BlockSpec(memory_space=pltpu.VMEM)
    hbm = pl.BlockSpec(memory_space=pl.ANY)
    caption_loss, image_loss, loss = pl.pallas_call(
        functools.partial(kernel, blk, rep),
        out_shape=(
            jax.ShapeDtypeStruct((1, n), f32),
            jax.ShapeDtypeStruct((1, n), f32),
            jax.ShapeDtypeStruct((1, 1), f32),
        ),
        in_specs=[hbm] * 4,
        out_specs=(hbm, hbm, vmem),
        scratch_shapes=[
            pltpu.VMEM((n, width), captions.dtype),
            pltpu.VMEM((2, rep, n, width), captions.dtype),
            pltpu.VMEM((H, V, 2, n, width), images.dtype),
            pltpu.VMEM((N, 2, 1, n), i32),
            pltpu.VMEM((H, 1, C), f32),
            pltpu.VMEM((H, 1, C), i32),
            pltpu.VMEM((2 * rep, n, 1), i32),
            pltpu.VMEM((2 * rep, n, 1), f32),
            pltpu.VMEM((1, n), f32),
            pltpu.VMEM((2 * rep, n, 1), f32),
            pltpu.VMEM((2 * rep, n, 1), f32),
            pltpu.VMEM((2 * rep, n, 1), f32),
            pltpu.VMEM((H, 8, C), f32),
            pltpu.VMEM((2 * rep, 8, n), f32),
            pltpu.VMEM((2 * rep, 8, n), f32),
            pltpu.VMEM((H * B, 8, n), f32),
            pltpu.VMEM((H * B, 8, n), f32),
            pltpu.VMEM((N, 1, 128), f32),
            pltpu.VMEM((1, n), f32),
            pltpu.VMEM((1, n), f32),
            dma(5), dma(2),
            dma(H * B * IMAGE_PIECES), dma(H * IMAGE_PIECES), dma(H * V * IMAGE_PIECES),
            dma(H * V * IMAGE_PIECES),
            dma(2 * rep * CAPTION_PIECES), dma(2 * CAPTION_PIECES), dma(2 * rep * CAPTION_PIECES),
            dma(G), dma(G), dma(U), dma(U),
            dma(2 * rep), dma(2 * rep), dma(H * B), dma(H * B), dma(N), dma(N),
        ],
        compiler_params=pltpu.CompilerParams(collective_id=0, has_side_effects=True),
    )(captions, images, positives.reshape(1, n), valid.reshape(1, n))
    return caption_loss.reshape(n), image_loss.reshape(n), loss.reshape(())


def solution(mesh):
    placed = (
        P(("blk", "rep"), None),
        P(("blk", "rep"), None),
        P(("blk", "rep")),
        P(("blk", "rep")),
    )
    return jax.shard_map(
        functools.partial(local, mesh.shape["blk"], mesh.shape["rep"]),
        mesh=mesh,
        in_specs=placed,
        out_specs=(P(("blk", "rep")), P(("blk", "rep")), P()),
        check_vma=False,
    )
```

```python
import functools
import math

import jax
import jax.numpy as jnp
from jax import lax
from jax.experimental import pallas as pl
from jax.experimental.pallas import tpu as pltpu
from jax.sharding import PartitionSpec as P

very_low = -1e30
floor = -1e29
IMAGE_PIECES = 4
CAPTION_PIECES = 4
LAST_PIECES = 2
HELD_BACK = 1
LANES = 128
SUBLANES = 8
log2_e = math.log2(math.e)
ln_2 = math.log(2)


def grid_of(blk, rep):
    chips = (blk // 2) * rep
    planes = 1
    while (planes * 2) ** 2 <= chips and (blk // 2) % (planes * 2) == 0:
        planes *= 2
    return planes, blk // 2 // planes


def mod(a, b):
    return a & (b - 1) if b & (b - 1) == 0 else lax.rem(a, b)


def div(a, b):
    return a >> (b.bit_length() - 1) if b & (b - 1) == 0 else lax.div(a, b)


def semaphore_counts(U, V, rep):
    H = U // 2
    along = (H - 1) * IMAGE_PIECES
    across = H * (V - 1) * IMAGE_PIECES
    return along, across, along + across + H, 2 * CAPTION_PIECES + (rep - 1) * (1 + LAST_PIECES)


def kernel(
    blk, rep, cap_ref, img_ref, pos_ref, val_ref, closs_ref, iloss_ref, loss_ref,
    mine, caps, imgs, raw, words, image_bias, image_ids, target, caption_bias,
    row_peak, row_total, row_match, col_peak, col_total, col_match,
    rowsend, rowrecv, colsend, colrecv, part, closs, iloss,
    loc_sem, out_sem, img_recv, cap_recv, send_sem, recv_sem,
):
    U, V = grid_of(blk, rep)
    N = blk * rep
    G = N // U
    H = U // 2
    B = V * 2
    n, width = cap_ref.shape
    C = B * n
    along_sems, across_sems, _, _ = semaphore_counts(U, V, rep)
    b, r = lax.axis_index("blk"), lax.axis_index("rep")
    c = mod(b, 2)
    u = div(b, 2 * V)
    v = mod(div(b, 2), V)
    me = b * rep + r
    g = mod(me, G)
    half, h = div(u, H), mod(u, H)
    keeps_own = div(u, 2) == h
    img_sent, cap_sent, line_sent, plane_sent, row_sent, col_sent, part_sent = (
        send_sem.at[k] for k in range(7)
    )
    line_came, plane_came, row_came, col_came, part_came = (recv_sem.at[k] for k in range(5))

    def near_of(uu):
        return jnp.where(uu > 2 * mod(uu, H), 1, 0)

    near = near_of(u)

    def member(uu, vv, cc, rr):
        return ((uu * V + vv) * 2 + cc) * rep + rr

    def remote(src, dst, ss, rs, to):
        return pltpu.make_async_remote_copy(
            src_ref=src, dst_ref=dst, send_sem=ss, recv_sem=rs, device_id=to,
            device_id_type=pl.DeviceIdType.LOGICAL,
        )

    partner = member(u, v, 1 - c, r)

    def sent(ref, sem):
        remote(ref, ref, sem, img_recv.at[0], partner).wait_send()

    def came(ref, sem):
        remote(ref, ref, img_sent, sem, partner).wait_recv()

    barrier = pltpu.get_barrier_semaphore()
    others = [u * G + mod(g + k, G) for k in range(1, G)]
    others += [mod(u + k, U) * G + g for k in range(1, U)]
    for to in others:
        pl.semaphore_signal(
            barrier, inc=1, device_id=to, device_id_type=pl.DeviceIdType.LOGICAL
        )

    def block(i, vv, cc):
        return (i * V + vv) * 2 + cc

    load_val = pltpu.make_async_copy(val_ref, raw.at[0], loc_sem.at[0])
    load_pos = pltpu.make_async_copy(pos_ref, raw.at[1], loc_sem.at[1])
    load_img = pltpu.make_async_copy(img_ref, imgs.at[block(h, v, c)], loc_sem.at[2])
    load_cap = pltpu.make_async_copy(cap_ref, mine, loc_sem.at[3])
    keep_cap = pltpu.make_async_copy(cap_ref, caps.at[0], loc_sem.at[4])
    load_val.start()
    load_pos.start()
    load_img.start()
    load_cap.start()

    @pl.when(keeps_own)
    def _():
        keep_cap.start()

    load_val.wait()
    load_pos.wait()
    words[g * U + u] = raw[1] * 2 + raw[0]
    load_img.wait()
    load_cap.wait()

    @pl.when(keeps_own)
    def _():
        keep_cap.wait()

    pl.semaphore_wait(barrier, len(others))

    def image_rows(k):
        return pl.ds(k * (n // IMAGE_PIECES), n // IMAGE_PIECES)

    def caption_rows(k):
        return pl.ds(k * (n // CAPTION_PIECES), n // CAPTION_PIECES)

    def img_copy(at, k, sem, to):
        rows = imgs.at[at, image_rows(k)]
        return remote(rows, rows, img_sent, img_recv.at[sem], to)

    def img_along(d, k):
        to = member(half * H + mod(h + d, H), v, c, r)
        return img_copy(block(h, v, c), k, (H - d - 1) * IMAGE_PIECES + k, to)

    def img_across(di, d, k):
        at = block(mod(h + di, H), v, c)
        sem = along_sems + (di * (V - 1) + V - d - 1) * IMAGE_PIECES + k
        return img_copy(at, k, sem, member(u, mod(v + d, V), c, r))

    def img_beside(di, vv, k):
        return img_copy(block(mod(h + di, H), vv, c), k, along_sems + across_sems + di, partner)

    def along_came(di, k):
        at = block(mod(h + di, H), v, c)
        came(imgs.at[at, image_rows(k)], img_recv.at[(di - 1) * IMAGE_PIECES + k])

    def across_came(di, d, k):
        at = block(mod(h + di, H), mod(v + d, V), c)
        sem = along_sems + (di * (V - 1) + d - 1) * IMAGE_PIECES + k
        came(imgs.at[at, image_rows(k)], img_recv.at[sem])

    def beside_came(di):
        came(imgs.at[pl.ds(mod(h + di, H) * B, V)], img_recv.at[along_sems + across_sems + di])

    def cap_along(t, k):
        rows = caption_rows(k)
        to = t * H + div(u, 2)
        away = jnp.where(mod(u, 2) == near_of(to), 0, 1)
        return remote(
            mine.at[rows], caps.at[away * rep, rows], cap_sent,
            cap_recv.at[away * CAPTION_PIECES + k], member(to, v, c, r),
        )

    def cap_across(away, d, k):
        rows = caption_rows(k)
        seat = rep - d
        sem = 2 * CAPTION_PIECES + seat - 1
        if away:
            piece = k // (CAPTION_PIECES // LAST_PIECES)
            sem = 2 * CAPTION_PIECES + rep - 1 + (seat - 1) * LAST_PIECES + piece
        return remote(
            caps.at[away * rep, rows], caps.at[away * rep + seat, rows], cap_sent,
            cap_recv.at[sem], member(u, v, c, mod(r + d, rep)),
        )

    def relay_captions(away, k):
        came(caps.at[away * rep, caption_rows(k)], cap_recv.at[away * CAPTION_PIECES + k])
        for d in range(1, rep):
            cap_across(away, d, k).start()

    def line_copy(k):
        row = words.at[g * U + u]
        return remote(row, row, line_sent, line_came, mod(u + k, U) * G + g)

    def plane_copy(k):
        rows = words.at[pl.ds(g * U, U)]
        return remote(rows, rows, plane_sent, plane_came, u * G + mod(g + k, G))

    def own_across(k):
        for d in range(1, V):
            img_across(0, d, k).start()

    def own_captions_across(k):
        @pl.when(keeps_own)
        def _():
            for d in range(1, rep):
                cap_across(0, d, k).start()

    for k in range(1, U):
        line_copy(k).start()
    for k in range(IMAGE_PIECES):
        for d in range(1, H):
            img_along(d, k).start()
        if k < IMAGE_PIECES - HELD_BACK:
            own_across(k)
        img_beside(0, v, k).start()
    for k in range(CAPTION_PIECES):
        for t in range(2):
            @pl.when(t * H + div(u, 2) != u)
            def _():
                cap_along(t, k).start()
        if k < CAPTION_PIECES - HELD_BACK:
            own_captions_across(k)

    for i in range(H):
        base = (half * H + i) * G
        for s in range(B):
            cols = slice(s * n, (s + 1) * n)
            first = (base + s * rep + r) * n
            image_ids[i, :, cols] = first + lax.broadcasted_iota(jnp.int32, (1, n), 1)
    col_peak[...] = jnp.full(col_peak.shape, floor, jnp.float32)
    col_total[...] = jnp.zeros(col_total.shape, jnp.float32)
    col_match[...] = jnp.zeros(col_match.shape, jnp.float32)
    row_peak[...] = jnp.full(row_peak.shape, floor, jnp.float32)
    row_total[...] = jnp.zeros(row_total.shape, jnp.float32)
    row_match[...] = jnp.zeros(row_match.shape, jnp.float32)

    came(words.at[pl.ds(0, U - 1)], line_came)
    for k in range(1, G):
        plane_copy(k).start()
    for k in range(IMAGE_PIECES - HELD_BACK, IMAGE_PIECES):
        own_across(k)
    for k in range(CAPTION_PIECES - HELD_BACK, CAPTION_PIECES):
        own_captions_across(k)

    for k in range(max(IMAGE_PIECES, CAPTION_PIECES)):
        if k < IMAGE_PIECES:
            for di in range(1, H):
                along_came(di, k)
                for d in range(1, V):
                    img_across(di, d, k).start()
                img_beside(di, v, k).start()
            for d in range(1, V):
                across_came(0, d, k)
                img_beside(0, mod(v + d, V), k).start()
        if k < CAPTION_PIECES:
            @pl.when(jnp.logical_not(keeps_own))
            def _():
                relay_captions(0, k)

    came(words.at[pl.ds(0, (G - 1) * U)], plane_came)

    eye = lax.broadcasted_iota(jnp.int32, (n, n), 0) == lax.broadcasted_iota(jnp.int32, (n, n), 1)

    def to_column(row):
        return jnp.sum(jnp.where(eye, row, 0.0), axis=1, keepdims=True)

    def to_row(column):
        return jnp.sum(jnp.where(eye, column, 0.0), axis=0, keepdims=True)

    flags = (words[:, 0, :] & 1).astype(jnp.float32)
    image_total = jnp.sum(jnp.sum(flags, axis=1, keepdims=True), axis=0, keepdims=True)

    def seat_row(s):
        away, d = div(s, rep), mod(s, rep)
        uu = 2 * h + jnp.where(away == 0, near, 1 - near)
        return ((v * 2 + c) * rep + mod(r + d, rep)) * U + uu

    aims = [words[seat_row(s)] >> 1 for s in range(2 * rep)] + [words[g * U + u] >> 1]
    aim = jnp.concatenate(aims, axis=1)
    order = lax.broadcasted_iota(jnp.int32, (N, aim.shape[1]), 0)
    starts = (mod(order, U) * G + div(order, U)) * n
    inside = (aim >= starts) & (aim < starts + n)
    picked = jnp.dot(
        flags.T.astype(jnp.bfloat16), jnp.where(inside, 1.0, 0.0).astype(jnp.bfloat16),
        preferred_element_type=jnp.float32,
    )
    start = jnp.sum(jnp.where(inside, starts, 0).astype(jnp.float32), axis=0, keepdims=True)
    low = aim - start.astype(jnp.int32)
    depth = lax.broadcasted_iota(jnp.int32, picked.shape, 0)
    ok = jnp.sum(jnp.where(depth == low, picked, 0.0), axis=0, keepdims=True)
    own_ok = ok[:, 2 * rep * n :]
    for s in range(2 * rep):
        ok_row = ok[:, s * n : (s + 1) * n]
        bias = to_column(jnp.where(ok_row > 0, 0.0, very_low))
        caption_bias[s] = jnp.broadcast_to(bias, (n, LANES))
        aim_column = to_column(aims[s].astype(jnp.float32)).astype(jnp.int32)
        target[s] = jnp.broadcast_to(aim_column, (n, LANES))
    for i in range(H):
        for s in range(B):
            flag = words[(s * rep + r) * U + half * H + i] & 1
            image_bias[i, :, s * n : (s + 1) * n] = jnp.where(flag > 0, 0.0, very_low)

    def fold(x, op):
        y = x[:, :LANES]
        for j in range(1, C // LANES):
            y = op(y, x[:, j * LANES : (j + 1) * LANES])
        return y

    def wide(x):
        return jnp.concatenate([x] * (C // LANES), axis=1)

    def tally(s, i, scores, first, rows):
        scaled = scores * log2_e
        bias, ids = image_bias[i], image_ids[i]
        old_peak = col_peak[i]
        peak, match = old_peak, col_match[i]
        peaks = []
        for q in range(rows // SUBLANES):
            at = pl.ds(first + q * SUBLANES, SUBLANES)
            x = scaled[q * SUBLANES : (q + 1) * SUBLANES]
            peaks.append(jnp.maximum(fold(x + bias, jnp.maximum), row_peak[s, at]))
            peak = jnp.maximum(peak, x + wide(caption_bias[s, at]))
            picked = jnp.where(wide(target[s, at]) == ids, x, 0.0)
            row_match[s, at] = row_match[s, at] + fold(picked, jnp.add)
            match = match + picked
        total = col_total[i] * jnp.exp2(old_peak - peak)
        for q in range(rows // SUBLANES):
            at = pl.ds(first + q * SUBLANES, SUBLANES)
            x = scaled[q * SUBLANES : (q + 1) * SUBLANES]
            powers = jnp.exp2(x + bias - wide(peaks[q]))
            row_total[s, at] = row_total[s, at] * jnp.exp2(row_peak[s, at] - peaks[q]) + fold(
                powers, jnp.add
            )
            row_peak[s, at] = peaks[q]
            total = total + jnp.exp2(x + wide(caption_bias[s, at]) - peak)
        col_peak[i] = peak
        col_total[i] = total
        col_match[i] = match

    def score(s, count, i, first, rows):
        left = caps[pl.ds(s, count)].reshape(count * n, width) if rows == n else caps[s, pl.ds(first, rows)]
        scores = lax.dot_general(
            left, imgs[pl.ds(i * B, B)].reshape(C, width), (((1,), (1,)), ((), ())),
            preferred_element_type=jnp.float32,
        )
        for k in range(count):
            tally(s + k, i, scores[k * rows : (k + 1) * rows], first, rows)

    beside_came(0)

    @pl.loop(0, rep + 1)
    def _(e):
        for k in range(max(CAPTION_PIECES, IMAGE_PIECES)):
            @pl.when(e == min(k, rep))
            def _():
                if k < CAPTION_PIECES:
                    relay_captions(1, k)
                if k < IMAGE_PIECES:
                    for di in range(1, H):
                        for d in range(1, V):
                            across_came(di, d, k)
                            img_beside(di, mod(v + d, V), k).start()

        @pl.when((e > 0) & (e < rep))
        def _():
            came(caps.at[0], cap_recv.at[2 * CAPTION_PIECES + e - 1])
        score(e, 1, h, 0, n)

    @pl.loop(1, H)
    def _(di):
        beside_came(di)
        score(0, rep + 1, mod(h + di, H), 0, n)

    def row_copy(s):
        away, d = div(s, rep), mod(s, rep)
        uu = 2 * h + jnp.where(away == 0, near, 1 - near)
        at = half * rep + r
        return remote(
            rowsend.at[s], rowrecv.at[at], row_sent, row_came, member(uu, v, c, mod(r + d, rep))
        )

    def send_rows(s):
        peak = jnp.max(row_peak[s], axis=1, keepdims=True)
        total = jnp.sum(row_total[s] * jnp.exp2(row_peak[s] - peak), axis=1, keepdims=True)
        rowsend[s, 0:1, :] = to_row(peak)
        rowsend[s, 1:2, :] = to_row(total)
        rowsend[s, 2:3, :] = to_row(jnp.sum(row_match[s], axis=1, keepdims=True))
        stays = keeps_own & (s == 0)

        @pl.when(jnp.logical_not(stays))
        def _():
            row_copy(s).start()

        @pl.when(stays)
        def _():
            rowrecv[half * rep + r] = rowsend[s]

    @pl.loop(0, rep + 1)
    def _(s):
        send_rows(s)

    @pl.loop(1, rep)
    def _(d):
        @pl.loop(0, LAST_PIECES)
        def _(k):
            rows = n // LAST_PIECES
            came(
                caps.at[rep + d, pl.ds(0, rows)],
                cap_recv.at[2 * CAPTION_PIECES + rep - 1 + (d - 1) * LAST_PIECES + k],
            )

            @pl.loop(0, H)
            def _(e):
                score(rep + d, 1, e, k * rows, rows)
        send_rows(rep + d)

    own_at = h * B + v * 2 + c
    for i in range(H):
        peak = jnp.max(col_peak[i], axis=0, keepdims=True)
        total = jnp.sum(col_total[i] * jnp.exp2(col_peak[i] - peak), axis=0, keepdims=True)
        match = jnp.sum(col_match[i], axis=0, keepdims=True)
        for s in range(B):
            cols = slice(s * n, (s + 1) * n)
            colsend[i * B + s, 0:1, :] = peak[:, cols]
            colsend[i * B + s, 1:2, :] = total[:, cols]
            colsend[i * B + s, 2:3, :] = match[:, cols]

    def col_copy(k):
        slot = mod(own_at + k, H * B)
        i, s = div(slot, B), mod(slot, B)
        to = (half * H + i) * G + s * rep + r
        return remote(colsend.at[slot], colrecv.at[own_at], col_sent, col_came, to)

    for k in range(1, H * B):
        col_copy(k).start()
    colrecv[own_at] = colsend[own_at]

    def joined(parts, count):
        peak = parts[0, 0:1, :]
        for s in range(1, count):
            peak = jnp.maximum(peak, parts[s, 0:1, :])
        total = jnp.zeros_like(peak)
        match = jnp.zeros_like(peak)
        for s in range(count):
            total += parts[s, 1:2, :] * jnp.exp2(parts[s, 0:1, :] - peak)
            match += parts[s, 2:3, :]
        return (peak - match) * ln_2 + jnp.log(total)

    @pl.when(keeps_own)
    def _():
        came(rowrecv.at[pl.ds(0, 2 * rep - 1)], row_came)

    @pl.when(jnp.logical_not(keeps_own))
    def _():
        came(rowrecv, row_came)

    caption_loss = own_ok * joined(rowrecv, 2 * rep)
    closs[...] = caption_loss
    put_caption = pltpu.make_async_copy(closs, closs_ref, out_sem.at[0])
    put_caption.start()
    came(colrecv.at[pl.ds(0, H * B - 1)], col_came)
    image_loss = raw[0].astype(jnp.float32) * joined(colrecv, H * B)
    iloss[...] = image_loss
    put_image = pltpu.make_async_copy(iloss, iloss_ref, out_sem.at[1])
    put_image.start()
    own_sum = jnp.sum(caption_loss + image_loss, axis=1, keepdims=True)
    part[me] = jnp.broadcast_to(own_sum, (1, LANES))

    @pl.loop(1, N)
    def _(k):
        remote(part.at[me], part.at[me], part_sent, part_came, mod(me + k, N)).start()

    sent(words.at[pl.ds(0, U - 1)], line_sent)
    sent(words.at[pl.ds(0, (G - 1) * U)], plane_sent)
    sent(imgs.at[pl.ds(0, H * B - 1)], img_sent)

    @pl.when(keeps_own)
    def _():
        sent(caps.at[pl.ds(0, 2 * rep - 1)], cap_sent)
        sent(rowsend.at[pl.ds(0, 2 * rep - 1)], row_sent)

    @pl.when(jnp.logical_not(keeps_own))
    def _():
        sent(caps, cap_sent)
        sent(rowsend, row_sent)

    sent(colsend.at[pl.ds(0, H * B - 1)], col_sent)
    put_caption.wait()
    put_image.wait()
    sent(part.at[pl.ds(0, N - 1)], part_sent)
    came(part.at[pl.ds(0, N - 1)], part_came)

    whole = jnp.sum(part[:, 0, :], axis=0, keepdims=True)
    loss_ref[...] = whole[:, 0:1] / (2.0 * image_total)


def local(blk, rep, captions, images, positives, valid):
    n, width = captions.shape
    U, V = grid_of(blk, rep)
    N = blk * rep
    H, B = U // 2, V * 2
    C = B * n
    f32, i32 = jnp.float32, jnp.int32
    _, _, image_sems, caption_sems = semaphore_counts(U, V, rep)
    dma = lambda count: pltpu.SemaphoreType.DMA((count,))
    vmem = pl.BlockSpec(memory_space=pltpu.VMEM)
    hbm = pl.BlockSpec(memory_space=pl.ANY)
    caption_loss, image_loss, loss = pl.pallas_call(
        functools.partial(kernel, blk, rep),
        out_shape=(
            jax.ShapeDtypeStruct((1, n), f32),
            jax.ShapeDtypeStruct((1, n), f32),
            jax.ShapeDtypeStruct((1, 1), f32),
        ),
        in_specs=[hbm] * 4,
        out_specs=(hbm, hbm, vmem),
        scratch_shapes=[
            pltpu.VMEM((n, width), captions.dtype),
            pltpu.VMEM((2 * rep, n, width), captions.dtype),
            pltpu.VMEM((H * B, n, width), images.dtype),
            pltpu.VMEM((2, 1, n), i32),
            pltpu.VMEM((N, 1, n), i32),
            pltpu.VMEM((H, 1, C), f32),
            pltpu.VMEM((H, 1, C), i32),
            pltpu.VMEM((2 * rep, n, LANES), i32),
            pltpu.VMEM((2 * rep, n, LANES), f32),
            pltpu.VMEM((2 * rep, n, LANES), f32),
            pltpu.VMEM((2 * rep, n, LANES), f32),
            pltpu.VMEM((2 * rep, n, LANES), f32),
            pltpu.VMEM((H, SUBLANES, C), f32),
            pltpu.VMEM((H, SUBLANES, C), f32),
            pltpu.VMEM((H, SUBLANES, C), f32),
            pltpu.VMEM((2 * rep, 8, n), f32),
            pltpu.VMEM((2 * rep, 8, n), f32),
            pltpu.VMEM((H * B, 8, n), f32),
            pltpu.VMEM((H * B, 8, n), f32),
            pltpu.VMEM((N, 1, LANES), f32),
            pltpu.VMEM((1, n), f32),
            pltpu.VMEM((1, n), f32),
            dma(5), dma(2), dma(image_sems), dma(caption_sems), dma(7), dma(5),
        ],
        compiler_params=pltpu.CompilerParams(collective_id=0, has_side_effects=True),
    )(captions, images, positives.reshape(1, n), valid.reshape(1, n))
    return caption_loss.reshape(n), image_loss.reshape(n), loss.reshape(())


def solution(mesh):
    placed = (
        P(("blk", "rep"), None),
        P(("blk", "rep"), None),
        P(("blk", "rep")),
        P(("blk", "rep")),
    )
    return jax.shard_map(
        functools.partial(local, mesh.shape["blk"], mesh.shape["rep"]),
        mesh=mesh,
        in_specs=placed,
        out_specs=(P(("blk", "rep")), P(("blk", "rep")), P()),
        check_vma=False,
    )
```

```python
import functools
import math

import jax
import jax.numpy as jnp
from jax import lax
from jax.experimental import pallas as pl
from jax.experimental.pallas import tpu as pltpu
from jax.sharding import PartitionSpec as P

very_low = -1e30
floor = -1e29
IMAGE_PIECES = 4
CAPTION_PIECES = 4
LAST_PIECES = 2
HELD_BACK = 1
LANES = 128
SUBLANES = 8
log2_e = math.log2(math.e)
ln_2 = math.log(2)


def grid_of(blk, rep):
    chips = (blk // 2) * rep
    planes = 1
    while (planes * 2) ** 2 <= chips and (blk // 2) % (planes * 2) == 0:
        planes *= 2
    return planes, blk // 2 // planes


def mod(a, b):
    return a & (b - 1) if b & (b - 1) == 0 else lax.rem(a, b)


def div(a, b):
    return a >> (b.bit_length() - 1) if b & (b - 1) == 0 else lax.div(a, b)


def semaphore_counts(U, V, rep):
    H = U // 2
    along = (H - 1) * IMAGE_PIECES
    across = H * (V - 1) * IMAGE_PIECES
    return along, across, along + across + H, 2 * CAPTION_PIECES + (rep - 1) * (1 + LAST_PIECES)


def kernel(
    blk, rep, cap_ref, img_ref, pos_ref, val_ref, terms_ref,
    mine, caps, imgs, raw, words, image_bias, image_ids, target, caption_bias,
    row_peak, row_total, row_match, col_peak, col_total, col_match,
    rowsend, rowrecv, colsend, colrecv, part,
    loc_sem, img_recv, cap_recv, send_sem, recv_sem,
):
    U, V = grid_of(blk, rep)
    N = blk * rep
    G = N // U
    H = U // 2
    B = V * 2
    n, width = cap_ref.shape
    C = B * n
    along_sems, across_sems, _, _ = semaphore_counts(U, V, rep)
    b, r = lax.axis_index("blk"), lax.axis_index("rep")
    c = mod(b, 2)
    u = div(b, 2 * V)
    v = mod(div(b, 2), V)
    me = b * rep + r
    g = mod(me, G)
    half, h = div(u, H), mod(u, H)
    keeps_own = div(u, 2) == h
    img_sent, cap_sent, line_sent, plane_sent, row_sent, col_sent, part_sent = (
        send_sem.at[k] for k in range(7)
    )
    line_came, plane_came, row_came, col_came, part_came = (recv_sem.at[k] for k in range(5))

    def near_of(uu):
        return jnp.where(uu > 2 * mod(uu, H), 1, 0)

    near = near_of(u)

    def member(uu, vv, cc, rr):
        return ((uu * V + vv) * 2 + cc) * rep + rr

    def remote(src, dst, ss, rs, to):
        return pltpu.make_async_remote_copy(
            src_ref=src, dst_ref=dst, send_sem=ss, recv_sem=rs, device_id=to,
            device_id_type=pl.DeviceIdType.LOGICAL,
        )

    partner = member(u, v, 1 - c, r)

    def sent(ref, sem):
        remote(ref, ref, sem, img_recv.at[0], partner).wait_send()

    def came(ref, sem):
        remote(ref, ref, img_sent, sem, partner).wait_recv()

    barrier = pltpu.get_barrier_semaphore()
    others = [u * G + mod(g + k, G) for k in range(1, G)]
    others += [mod(u + k, U) * G + g for k in range(1, U)]
    for to in others:
        pl.semaphore_signal(
            barrier, inc=1, device_id=to, device_id_type=pl.DeviceIdType.LOGICAL
        )

    def block(i, vv, cc):
        return (i * V + vv) * 2 + cc

    load_val = pltpu.make_async_copy(val_ref, raw.at[0], loc_sem.at[0])
    load_pos = pltpu.make_async_copy(pos_ref, raw.at[1], loc_sem.at[1])
    load_img = pltpu.make_async_copy(img_ref, imgs.at[block(h, v, c)], loc_sem.at[2])
    load_cap = pltpu.make_async_copy(cap_ref, mine, loc_sem.at[3])
    keep_cap = pltpu.make_async_copy(cap_ref, caps.at[0], loc_sem.at[4])
    load_val.start()
    load_pos.start()
    load_img.start()
    load_cap.start()

    @pl.when(keeps_own)
    def _():
        keep_cap.start()

    load_val.wait()
    load_pos.wait()
    words[g * U + u] = raw[1] * 2 + raw[0]
    load_img.wait()
    load_cap.wait()

    @pl.when(keeps_own)
    def _():
        keep_cap.wait()

    pl.semaphore_wait(barrier, len(others))

    def image_rows(k):
        return pl.ds(k * (n // IMAGE_PIECES), n // IMAGE_PIECES)

    def caption_rows(k):
        return pl.ds(k * (n // CAPTION_PIECES), n // CAPTION_PIECES)

    def img_copy(at, k, sem, to):
        rows = imgs.at[at, image_rows(k)]
        return remote(rows, rows, img_sent, img_recv.at[sem], to)

    def img_along(d, k):
        to = member(half * H + mod(h + d, H), v, c, r)
        return img_copy(block(h, v, c), k, (H - d - 1) * IMAGE_PIECES + k, to)

    def img_across(di, d, k):
        at = block(mod(h + di, H), v, c)
        sem = along_sems + (di * (V - 1) + V - d - 1) * IMAGE_PIECES + k
        return img_copy(at, k, sem, member(u, mod(v + d, V), c, r))

    def img_beside(di, vv, k):
        return img_copy(block(mod(h + di, H), vv, c), k, along_sems + across_sems + di, partner)

    def along_came(di, k):
        at = block(mod(h + di, H), v, c)
        came(imgs.at[at, image_rows(k)], img_recv.at[(di - 1) * IMAGE_PIECES + k])

    def across_came(di, d, k):
        at = block(mod(h + di, H), mod(v + d, V), c)
        sem = along_sems + (di * (V - 1) + d - 1) * IMAGE_PIECES + k
        came(imgs.at[at, image_rows(k)], img_recv.at[sem])

    def beside_came(di):
        came(imgs.at[pl.ds(mod(h + di, H) * B, V)], img_recv.at[along_sems + across_sems + di])

    def cap_along(t, k):
        rows = caption_rows(k)
        to = t * H + div(u, 2)
        away = jnp.where(mod(u, 2) == near_of(to), 0, 1)
        return remote(
            mine.at[rows], caps.at[away * rep, rows], cap_sent,
            cap_recv.at[away * CAPTION_PIECES + k], member(to, v, c, r),
        )

    def cap_across(away, d, k):
        rows = caption_rows(k)
        seat = rep - d
        sem = 2 * CAPTION_PIECES + seat - 1
        if away:
            piece = k // (CAPTION_PIECES // LAST_PIECES)
            sem = 2 * CAPTION_PIECES + rep - 1 + (seat - 1) * LAST_PIECES + piece
        return remote(
            caps.at[away * rep, rows], caps.at[away * rep + seat, rows], cap_sent,
            cap_recv.at[sem], member(u, v, c, mod(r + d, rep)),
        )

    def relay_captions(away, k):
        came(caps.at[away * rep, caption_rows(k)], cap_recv.at[away * CAPTION_PIECES + k])
        for d in range(1, rep):
            cap_across(away, d, k).start()

    def line_copy(k):
        row = words.at[g * U + u]
        return remote(row, row, line_sent, line_came, mod(u + k, U) * G + g)

    def plane_copy(k):
        rows = words.at[pl.ds(g * U, U)]
        return remote(rows, rows, plane_sent, plane_came, u * G + mod(g + k, G))

    def own_across(k):
        for d in range(1, V):
            img_across(0, d, k).start()

    def own_captions_across(k):
        @pl.when(keeps_own)
        def _():
            for d in range(1, rep):
                cap_across(0, d, k).start()

    for k in range(1, U):
        line_copy(k).start()
    for k in range(IMAGE_PIECES):
        for d in range(1, H):
            img_along(d, k).start()
        if k < IMAGE_PIECES - HELD_BACK:
            own_across(k)
        img_beside(0, v, k).start()
    for k in range(CAPTION_PIECES):
        for t in range(2):
            @pl.when(t * H + div(u, 2) != u)
            def _():
                cap_along(t, k).start()
        if k < CAPTION_PIECES - HELD_BACK:
            own_captions_across(k)

    for i in range(H):
        base = (half * H + i) * G
        for s in range(B):
            cols = slice(s * n, (s + 1) * n)
            first = (base + s * rep + r) * n
            image_ids[i, :, cols] = first + lax.broadcasted_iota(jnp.int32, (1, n), 1)
    col_peak[...] = jnp.full(col_peak.shape, floor, jnp.float32)
    col_total[...] = jnp.zeros(col_total.shape, jnp.float32)
    col_match[...] = jnp.zeros(col_match.shape, jnp.float32)
    row_peak[...] = jnp.full(row_peak.shape, floor, jnp.float32)
    row_total[...] = jnp.zeros(row_total.shape, jnp.float32)
    row_match[...] = jnp.zeros(row_match.shape, jnp.float32)

    came(words.at[pl.ds(0, U - 1)], line_came)
    for k in range(1, G):
        plane_copy(k).start()
    for k in range(IMAGE_PIECES - HELD_BACK, IMAGE_PIECES):
        own_across(k)
    for k in range(CAPTION_PIECES - HELD_BACK, CAPTION_PIECES):
        own_captions_across(k)

    for k in range(max(IMAGE_PIECES, CAPTION_PIECES)):
        if k < IMAGE_PIECES:
            for di in range(1, H):
                along_came(di, k)
                for d in range(1, V):
                    img_across(di, d, k).start()
                img_beside(di, v, k).start()
            for d in range(1, V):
                across_came(0, d, k)
                img_beside(0, mod(v + d, V), k).start()
        if k < CAPTION_PIECES:
            @pl.when(jnp.logical_not(keeps_own))
            def _():
                relay_captions(0, k)

    came(words.at[pl.ds(0, (G - 1) * U)], plane_came)

    eye = lax.broadcasted_iota(jnp.int32, (n, n), 0) == lax.broadcasted_iota(jnp.int32, (n, n), 1)

    def to_column(row):
        return jnp.sum(jnp.where(eye, row, 0.0), axis=1, keepdims=True)

    def to_row(column):
        return jnp.sum(jnp.where(eye, column, 0.0), axis=0, keepdims=True)

    flags = (words[:, 0, :] & 1).astype(jnp.float32)
    image_total = jnp.sum(jnp.sum(flags, axis=1, keepdims=True), axis=0, keepdims=True)

    def seat_row(s):
        away, d = div(s, rep), mod(s, rep)
        uu = 2 * h + jnp.where(away == 0, near, 1 - near)
        return ((v * 2 + c) * rep + mod(r + d, rep)) * U + uu

    aims = [words[seat_row(s)] >> 1 for s in range(2 * rep)] + [words[g * U + u] >> 1]
    aim = jnp.concatenate(aims, axis=1)
    order = lax.broadcasted_iota(jnp.int32, (N, aim.shape[1]), 0)
    starts = (mod(order, U) * G + div(order, U)) * n
    inside = (aim >= starts) & (aim < starts + n)
    picked = jnp.dot(
        flags.T.astype(jnp.bfloat16), jnp.where(inside, 1.0, 0.0).astype(jnp.bfloat16),
        preferred_element_type=jnp.float32,
    )
    start = jnp.sum(jnp.where(inside, starts, 0).astype(jnp.float32), axis=0, keepdims=True)
    low = aim - start.astype(jnp.int32)
    depth = lax.broadcasted_iota(jnp.int32, picked.shape, 0)
    ok = jnp.sum(jnp.where(depth == low, picked, 0.0), axis=0, keepdims=True)
    own_ok = ok[:, 2 * rep * n :]
    for s in range(2 * rep):
        ok_row = ok[:, s * n : (s + 1) * n]
        bias = to_column(jnp.where(ok_row > 0, 0.0, very_low))
        caption_bias[s] = jnp.broadcast_to(bias, (n, LANES))
        aim_column = to_column(aims[s].astype(jnp.float32)).astype(jnp.int32)
        target[s] = jnp.broadcast_to(aim_column, (n, LANES))
    for i in range(H):
        for s in range(B):
            flag = words[(s * rep + r) * U + half * H + i] & 1
            image_bias[i, :, s * n : (s + 1) * n] = jnp.where(flag > 0, 0.0, very_low)

    def fold(x, op):
        y = x[:, :LANES]
        for j in range(1, C // LANES):
            y = op(y, x[:, j * LANES : (j + 1) * LANES])
        return y

    def wide(x):
        return jnp.concatenate([x] * (C // LANES), axis=1)

    def tally(s, i, scores, first, rows):
        scaled = scores * log2_e
        bias, ids = image_bias[i], image_ids[i]
        old_peak = col_peak[i]
        peak, match = old_peak, col_match[i]
        peaks = []
        for q in range(rows // SUBLANES):
            at = pl.ds(first + q * SUBLANES, SUBLANES)
            x = scaled[q * SUBLANES : (q + 1) * SUBLANES]
            peaks.append(jnp.maximum(fold(x + bias, jnp.maximum), row_peak[s, at]))
            peak = jnp.maximum(peak, x + wide(caption_bias[s, at]))
            picked = jnp.where(wide(target[s, at]) == ids, x, 0.0)
            row_match[s, at] = row_match[s, at] + fold(picked, jnp.add)
            match = match + picked
        total = col_total[i] * jnp.exp2(old_peak - peak)
        for q in range(rows // SUBLANES):
            at = pl.ds(first + q * SUBLANES, SUBLANES)
            x = scaled[q * SUBLANES : (q + 1) * SUBLANES]
            powers = jnp.exp2(x + bias - wide(peaks[q]))
            row_total[s, at] = row_total[s, at] * jnp.exp2(row_peak[s, at] - peaks[q]) + fold(
                powers, jnp.add
            )
            row_peak[s, at] = peaks[q]
            total = total + jnp.exp2(x + wide(caption_bias[s, at]) - peak)
        col_peak[i] = peak
        col_total[i] = total
        col_match[i] = match

    def score(s, count, i, first, rows):
        left = caps[pl.ds(s, count)].reshape(count * n, width) if rows == n else caps[s, pl.ds(first, rows)]
        scores = lax.dot_general(
            left, imgs[pl.ds(i * B, B)].reshape(C, width), (((1,), (1,)), ((), ())),
            preferred_element_type=jnp.float32,
        )
        for k in range(count):
            tally(s + k, i, scores[k * rows : (k + 1) * rows], first, rows)

    beside_came(0)

    @pl.loop(0, rep + 1)
    def _(e):
        for k in range(max(CAPTION_PIECES, IMAGE_PIECES)):
            @pl.when(e == min(k, rep))
            def _():
                if k < CAPTION_PIECES:
                    relay_captions(1, k)
                if k < IMAGE_PIECES:
                    for di in range(1, H):
                        for d in range(1, V):
                            across_came(di, d, k)
                            img_beside(di, mod(v + d, V), k).start()

        @pl.when((e > 0) & (e < rep))
        def _():
            came(caps.at[0], cap_recv.at[2 * CAPTION_PIECES + e - 1])
        score(e, 1, h, 0, n)

    @pl.loop(1, H)
    def _(di):
        beside_came(di)
        score(0, rep + 1, mod(h + di, H), 0, n)

    def row_copy(s):
        away, d = div(s, rep), mod(s, rep)
        uu = 2 * h + jnp.where(away == 0, near, 1 - near)
        at = half * rep + r
        return remote(
            rowsend.at[s], rowrecv.at[at], row_sent, row_came, member(uu, v, c, mod(r + d, rep))
        )

    def send_rows(s):
        peak = jnp.max(row_peak[s], axis=1, keepdims=True)
        total = jnp.sum(row_total[s] * jnp.exp2(row_peak[s] - peak), axis=1, keepdims=True)
        rowsend[s, 0:1, :] = to_row(peak)
        rowsend[s, 1:2, :] = to_row(total)
        rowsend[s, 2:3, :] = to_row(jnp.sum(row_match[s], axis=1, keepdims=True))
        stays = keeps_own & (s == 0)

        @pl.when(jnp.logical_not(stays))
        def _():
            row_copy(s).start()

        @pl.when(stays)
        def _():
            rowrecv[half * rep + r] = rowsend[s]

    @pl.loop(0, rep + 1)
    def _(s):
        send_rows(s)

    @pl.loop(1, rep)
    def _(d):
        @pl.loop(0, LAST_PIECES)
        def _(k):
            rows = n // LAST_PIECES
            came(
                caps.at[rep + d, pl.ds(0, rows)],
                cap_recv.at[2 * CAPTION_PIECES + rep - 1 + (d - 1) * LAST_PIECES + k],
            )

            @pl.loop(0, H)
            def _(e):
                score(rep + d, 1, e, k * rows, rows)
        send_rows(rep + d)

    own_at = h * B + v * 2 + c
    for i in range(H):
        peak = jnp.max(col_peak[i], axis=0, keepdims=True)
        total = jnp.sum(col_total[i] * jnp.exp2(col_peak[i] - peak), axis=0, keepdims=True)
        match = jnp.sum(col_match[i], axis=0, keepdims=True)
        for s in range(B):
            cols = slice(s * n, (s + 1) * n)
            colsend[i * B + s, 0:1, :] = peak[:, cols]
            colsend[i * B + s, 1:2, :] = total[:, cols]
            colsend[i * B + s, 2:3, :] = match[:, cols]

    def col_copy(k):
        slot = mod(own_at + k, H * B)
        i, s = div(slot, B), mod(slot, B)
        to = (half * H + i) * G + s * rep + r
        return remote(colsend.at[slot], colrecv.at[own_at], col_sent, col_came, to)

    for k in range(1, H * B):
        col_copy(k).start()
    colrecv[own_at] = colsend[own_at]

    def joined(parts, count):
        peak = parts[0, 0:1, :]
        for s in range(1, count):
            peak = jnp.maximum(peak, parts[s, 0:1, :])
        total = jnp.zeros_like(peak)
        match = jnp.zeros_like(peak)
        for s in range(count):
            total += parts[s, 1:2, :] * jnp.exp2(parts[s, 0:1, :] - peak)
            match += parts[s, 2:3, :]
        return (peak - match) * ln_2 + jnp.log(total)

    @pl.when(keeps_own)
    def _():
        came(rowrecv.at[pl.ds(0, 2 * rep - 1)], row_came)

    @pl.when(jnp.logical_not(keeps_own))
    def _():
        came(rowrecv, row_came)

    caption_loss = own_ok * joined(rowrecv, 2 * rep)
    terms_ref[0:1, :] = caption_loss
    came(colrecv.at[pl.ds(0, H * B - 1)], col_came)
    image_loss = raw[0].astype(jnp.float32) * joined(colrecv, H * B)
    terms_ref[1:2, :] = image_loss
    own_sum = jnp.sum(caption_loss + image_loss, axis=1, keepdims=True)
    part[me] = jnp.broadcast_to(own_sum, (1, LANES))

    @pl.loop(1, N)
    def _(k):
        remote(part.at[me], part.at[me], part_sent, part_came, mod(me + k, N)).start()

    sent(words.at[pl.ds(0, U - 1)], line_sent)
    sent(words.at[pl.ds(0, (G - 1) * U)], plane_sent)
    sent(imgs.at[pl.ds(0, H * B - 1)], img_sent)

    @pl.when(keeps_own)
    def _():
        sent(caps.at[pl.ds(0, 2 * rep - 1)], cap_sent)
        sent(rowsend.at[pl.ds(0, 2 * rep - 1)], row_sent)

    @pl.when(jnp.logical_not(keeps_own))
    def _():
        sent(caps, cap_sent)
        sent(rowsend, row_sent)

    sent(colsend.at[pl.ds(0, H * B - 1)], col_sent)
    sent(part.at[pl.ds(0, N - 1)], part_sent)
    came(part.at[pl.ds(0, N - 1)], part_came)

    whole = jnp.sum(part[:, 0, :], axis=0, keepdims=True)
    terms_ref[2:3, 0:1] = whole[:, 0:1] / (2.0 * image_total)


def hand_out(terms_ref, closs_ref, iloss_ref, loss_ref):
    closs_ref[...] = terms_ref[0:1, :]
    iloss_ref[...] = terms_ref[1:2, :]
    loss_ref[...] = terms_ref[2:3, 0:1]


def local(blk, rep, captions, images, positives, valid):
    n, width = captions.shape
    U, V = grid_of(blk, rep)
    N = blk * rep
    H, B = U // 2, V * 2
    C = B * n
    f32, i32 = jnp.float32, jnp.int32
    _, _, image_sems, caption_sems = semaphore_counts(U, V, rep)
    dma = lambda count: pltpu.SemaphoreType.DMA((count,))
    vmem = pl.BlockSpec(memory_space=pltpu.VMEM)
    hbm = pl.BlockSpec(memory_space=pl.ANY)
    terms = pl.pallas_call(
        functools.partial(kernel, blk, rep),
        out_shape=pltpu.VMEM((SUBLANES, n), f32),
        in_specs=[hbm] * 4,
        out_specs=vmem,
        scratch_shapes=[
            pltpu.VMEM((n, width), captions.dtype),
            pltpu.VMEM((2 * rep, n, width), captions.dtype),
            pltpu.VMEM((H * B, n, width), images.dtype),
            pltpu.VMEM((2, 1, n), i32),
            pltpu.VMEM((N, 1, n), i32),
            pltpu.VMEM((H, 1, C), f32),
            pltpu.VMEM((H, 1, C), i32),
            pltpu.VMEM((2 * rep, n, LANES), i32),
            pltpu.VMEM((2 * rep, n, LANES), f32),
            pltpu.VMEM((2 * rep, n, LANES), f32),
            pltpu.VMEM((2 * rep, n, LANES), f32),
            pltpu.VMEM((2 * rep, n, LANES), f32),
            pltpu.VMEM((H, SUBLANES, C), f32),
            pltpu.VMEM((H, SUBLANES, C), f32),
            pltpu.VMEM((H, SUBLANES, C), f32),
            pltpu.VMEM((2 * rep, 8, n), f32),
            pltpu.VMEM((2 * rep, 8, n), f32),
            pltpu.VMEM((H * B, 8, n), f32),
            pltpu.VMEM((H * B, 8, n), f32),
            pltpu.VMEM((N, 1, LANES), f32),
            dma(5), dma(image_sems), dma(caption_sems), dma(7), dma(5),
        ],
        compiler_params=pltpu.CompilerParams(collective_id=0, has_side_effects=True),
    )(captions, images, positives.reshape(1, n), valid.reshape(1, n))
    caption_loss, image_loss, loss = pl.pallas_call(
        hand_out,
        out_shape=(
            jax.ShapeDtypeStruct((1, n), f32),
            jax.ShapeDtypeStruct((1, n), f32),
            jax.ShapeDtypeStruct((1, 1), f32),
        ),
        in_specs=[vmem],
        out_specs=(vmem,) * 3,
    )(pltpu.with_memory_space_constraint(terms, pltpu.VMEM))
    return caption_loss.reshape(n), image_loss.reshape(n), loss.reshape(())


def solution(mesh):
    placed = (
        P(("blk", "rep"), None),
        P(("blk", "rep"), None),
        P(("blk", "rep")),
        P(("blk", "rep")),
    )
    return jax.shard_map(
        functools.partial(local, mesh.shape["blk"], mesh.shape["rep"]),
        mesh=mesh,
        in_specs=placed,
        out_specs=(P(("blk", "rep")), P(("blk", "rep")), P()),
        check_vma=False,
    )
```

```python
import functools
import math

import jax
import jax.numpy as jnp
from jax import lax
from jax.experimental import pallas as pl
from jax.experimental.pallas import tpu as pltpu
from jax.sharding import PartitionSpec as P

very_low = -1e30
floor = -1e29
IMAGE_PIECES = 4
CAPTION_PIECES = 6
LAST_PIECES = 2
IMAGES_HELD = 1
CAPTIONS_HELD = 2
LANES = 128
SUBLANES = 8
log2_e = math.log2(math.e)
ln_2 = math.log(2)


def grid_of(blk, rep):
    chips = (blk // 2) * rep
    planes = 1
    while (planes * 2) ** 2 <= chips and (blk // 2) % (planes * 2) == 0:
        planes *= 2
    return planes, blk // 2 // planes


def mod(a, b):
    return a & (b - 1) if b & (b - 1) == 0 else lax.rem(a, b)


def div(a, b):
    return a >> (b.bit_length() - 1) if b & (b - 1) == 0 else lax.div(a, b)


def semaphore_counts(U, V, rep):
    H = U // 2
    along = (H - 1) * IMAGE_PIECES
    across = H * (V - 1) * IMAGE_PIECES
    return along, across, along + across + H * V, 2 * CAPTION_PIECES + (rep - 1) * (1 + LAST_PIECES)


def group_at(V, H, di, dv):
    if di == 0:
        return dv
    if dv == 0:
        return V + di - 1
    return V + H - 1 + (di - 1) * (V - 1) + dv - 1


def kernel(
    blk, rep, cap_ref, img_ref, pos_ref, val_ref, terms_ref,
    mine, caps, imgs, raw, words, image_bias, image_ids, target, caption_bias,
    row_peak, row_total, row_match, col_peak, col_total, col_match,
    rowsend, rowrecv, colsend, colrecv, part,
    loc_sem, img_recv, cap_recv, send_sem, recv_sem,
):
    U, V = grid_of(blk, rep)
    N = blk * rep
    G = N // U
    H = U // 2
    B = V * 2
    n, width = cap_ref.shape
    early = (V + H - 1) * 2 * n
    C = H * B * n
    along_sems, across_sems, _, _ = semaphore_counts(U, V, rep)
    b, r = lax.axis_index("blk"), lax.axis_index("rep")
    c = mod(b, 2)
    u = div(b, 2 * V)
    v = mod(div(b, 2), V)
    me = b * rep + r
    g = mod(me, G)
    half, h = div(u, H), mod(u, H)
    keeps_own = div(u, 2) == h
    img_sent, cap_sent, line_sent, plane_sent, row_sent, col_sent, part_sent = (
        send_sem.at[k] for k in range(7)
    )
    line_came, plane_came, row_came, col_came, part_came = (recv_sem.at[k] for k in range(5))

    def near_of(uu):
        return jnp.where(uu > 2 * mod(uu, H), 1, 0)

    near = near_of(u)

    def member(uu, vv, cc, rr):
        return ((uu * V + vv) * 2 + cc) * rep + rr

    def remote(src, dst, ss, rs, to):
        return pltpu.make_async_remote_copy(
            src_ref=src, dst_ref=dst, send_sem=ss, recv_sem=rs, device_id=to,
            device_id_type=pl.DeviceIdType.LOGICAL,
        )

    partner = member(u, v, 1 - c, r)

    def sent(ref, sem):
        remote(ref, ref, sem, img_recv.at[0], partner).wait_send()

    def came(ref, sem):
        remote(ref, ref, img_sent, sem, partner).wait_recv()

    barrier = pltpu.get_barrier_semaphore()
    others = [u * G + mod(g + k, G) for k in range(1, G)]
    others += [mod(u + k, U) * G + g for k in range(1, U)]
    for to in others:
        pl.semaphore_signal(
            barrier, inc=1, device_id=to, device_id_type=pl.DeviceIdType.LOGICAL
        )

    def group(di, dv):
        return group_at(V, H, di, dv)

    offsets = sorted((group(di, dv), di, dv) for di in range(H) for dv in range(V))

    def image_member(di, dv, k):
        return member(half * H + mod(h + di, H), mod(v + dv, V), c if k == 0 else 1 - c, r)

    load_val = pltpu.make_async_copy(val_ref, raw.at[0], loc_sem.at[0])
    load_pos = pltpu.make_async_copy(pos_ref, raw.at[1], loc_sem.at[1])
    load_img = pltpu.make_async_copy(img_ref, imgs.at[0], loc_sem.at[2])
    load_cap = pltpu.make_async_copy(cap_ref, mine, loc_sem.at[3])
    keep_cap = pltpu.make_async_copy(cap_ref, caps.at[0], loc_sem.at[4])
    load_val.start()
    load_pos.start()
    load_img.start()
    load_cap.start()

    @pl.when(keeps_own)
    def _():
        keep_cap.start()

    load_val.wait()
    load_pos.wait()
    words[g * U + u] = raw[1] * 2 + raw[0]
    load_img.wait()
    load_cap.wait()

    @pl.when(keeps_own)
    def _():
        keep_cap.wait()

    pl.semaphore_wait(barrier, len(others))

    def image_rows(k):
        return pl.ds(k * (n // IMAGE_PIECES), n // IMAGE_PIECES)

    def caption_rows(k):
        return pl.ds(k * (n // CAPTION_PIECES), n // CAPTION_PIECES)

    def img_copy(at, to_at, k, sem, to):
        rows = image_rows(k)
        return remote(imgs.at[at, rows], imgs.at[to_at, rows], img_sent, img_recv.at[sem], to)

    def across_sem(di, dv, k):
        return along_sems + (di * (V - 1) + dv - 1) * IMAGE_PIECES + k

    def img_along(d, k):
        to = member(half * H + mod(h + d, H), v, c, r)
        return img_copy(0, group(H - d, 0) * 2, k, (H - d - 1) * IMAGE_PIECES + k, to)

    def img_across(di, d, k):
        to = member(u, mod(v + d, V), c, r)
        return img_copy(
            group(di, 0) * 2, group(di, V - d) * 2, k, across_sem(di, V - d, k), to
        )

    def img_beside(di, dv, k):
        at = group(di, dv)
        return img_copy(at * 2, at * 2 + 1, k, along_sems + across_sems + at, partner)

    def along_came(di, k):
        came(imgs.at[group(di, 0) * 2, image_rows(k)], img_recv.at[(di - 1) * IMAGE_PIECES + k])

    def across_came(di, dv, k):
        came(imgs.at[group(di, dv) * 2, image_rows(k)], img_recv.at[across_sem(di, dv, k)])

    def beside_came(at):
        came(imgs.at[at * 2 + 1], img_recv.at[along_sems + across_sems + at])

    def cap_along(t, k):
        rows = caption_rows(k)
        to = t * H + div(u, 2)
        away = jnp.where(mod(u, 2) == near_of(to), 0, 1)
        return remote(
            mine.at[rows], caps.at[away * rep, rows], cap_sent,
            cap_recv.at[away * CAPTION_PIECES + k], member(to, v, c, r),
        )

    def cap_across(away, d, k):
        rows = caption_rows(k)
        seat = rep - d
        sem = 2 * CAPTION_PIECES + seat - 1
        if away:
            piece = k // (CAPTION_PIECES // LAST_PIECES)
            sem = 2 * CAPTION_PIECES + rep - 1 + (seat - 1) * LAST_PIECES + piece
        return remote(
            caps.at[away * rep, rows], caps.at[away * rep + seat, rows], cap_sent,
            cap_recv.at[sem], member(u, v, c, mod(r + d, rep)),
        )

    def relay_captions(away, k):
        came(caps.at[away * rep, caption_rows(k)], cap_recv.at[away * CAPTION_PIECES + k])
        for d in range(1, rep):
            cap_across(away, d, k).start()

    def line_copy(k):
        row = words.at[g * U + u]
        return remote(row, row, line_sent, line_came, mod(u + k, U) * G + g)

    def plane_copy(k):
        rows = words.at[pl.ds(g * U, U)]
        return remote(rows, rows, plane_sent, plane_came, u * G + mod(g + k, G))

    def own_across(k):
        for d in range(1, V):
            img_across(0, d, k).start()

    def own_captions_across(k):
        @pl.when(keeps_own)
        def _():
            for d in range(1, rep):
                cap_across(0, d, k).start()

    for k in range(1, U):
        line_copy(k).start()
    for k in range(IMAGE_PIECES):
        for d in range(1, H):
            img_along(d, k).start()
        if k < IMAGE_PIECES - IMAGES_HELD:
            own_across(k)
        img_beside(0, 0, k).start()
    for k in range(CAPTION_PIECES):
        for t in range(2):
            @pl.when(t * H + div(u, 2) != u)
            def _():
                cap_along(t, k).start()
        if k < CAPTION_PIECES - CAPTIONS_HELD:
            own_captions_across(k)

    for at, di, dv in offsets:
        for k in range(2):
            cols = slice((at * 2 + k) * n, (at * 2 + k + 1) * n)
            first = image_member(di, dv, k) * n
            image_ids[:, cols] = first + lax.broadcasted_iota(jnp.int32, (1, n), 1)
    col_peak[...] = jnp.full(col_peak.shape, floor, jnp.float32)
    col_total[...] = jnp.zeros(col_total.shape, jnp.float32)
    col_match[...] = jnp.zeros(col_match.shape, jnp.float32)
    row_peak[...] = jnp.full(row_peak.shape, floor, jnp.float32)
    row_total[...] = jnp.zeros(row_total.shape, jnp.float32)
    row_match[...] = jnp.zeros(row_match.shape, jnp.float32)

    came(words.at[pl.ds(0, U - 1)], line_came)
    for k in range(1, G):
        plane_copy(k).start()
    for k in range(IMAGE_PIECES - IMAGES_HELD, IMAGE_PIECES):
        own_across(k)
    for k in range(CAPTION_PIECES - CAPTIONS_HELD, CAPTION_PIECES):
        own_captions_across(k)

    pieces = [((k + 1) / IMAGE_PIECES, 0, k) for k in range(IMAGE_PIECES)]
    pieces += [((k + 1) / CAPTION_PIECES, 1, k) for k in range(CAPTION_PIECES)]
    pieces.sort()
    for _, is_caption, k in pieces:
        if is_caption:
            @pl.when(jnp.logical_not(keeps_own))
            def _():
                relay_captions(0, k)
        else:
            for di in range(1, H):
                along_came(di, k)
                for d in range(1, V):
                    img_across(di, d, k).start()
                img_beside(di, 0, k).start()
            for dv in range(1, V):
                across_came(0, dv, k)
                img_beside(0, dv, k).start()

    came(words.at[pl.ds(0, (G - 1) * U)], plane_came)

    eye = lax.broadcasted_iota(jnp.int32, (n, n), 0) == lax.broadcasted_iota(jnp.int32, (n, n), 1)

    def to_column(row):
        return jnp.sum(jnp.where(eye, row, 0.0), axis=1, keepdims=True)

    def to_row(column):
        return jnp.sum(jnp.where(eye, column, 0.0), axis=0, keepdims=True)

    flags = (words[:, 0, :] & 1).astype(jnp.float32)
    image_total = jnp.sum(jnp.sum(flags, axis=1, keepdims=True), axis=0, keepdims=True)

    def seat_row(s):
        away, d = div(s, rep), mod(s, rep)
        uu = 2 * h + jnp.where(away == 0, near, 1 - near)
        return ((v * 2 + c) * rep + mod(r + d, rep)) * U + uu

    aims = [words[seat_row(s)] >> 1 for s in range(2 * rep)] + [words[g * U + u] >> 1]
    aim = jnp.concatenate(aims, axis=1)
    order = lax.broadcasted_iota(jnp.int32, (N, aim.shape[1]), 0)
    starts = (mod(order, U) * G + div(order, U)) * n
    inside = (aim >= starts) & (aim < starts + n)
    picked = jnp.dot(
        flags.T.astype(jnp.bfloat16), jnp.where(inside, 1.0, 0.0).astype(jnp.bfloat16),
        preferred_element_type=jnp.float32,
    )
    start = jnp.sum(jnp.where(inside, starts, 0).astype(jnp.float32), axis=0, keepdims=True)
    low = aim - start.astype(jnp.int32)
    depth = lax.broadcasted_iota(jnp.int32, picked.shape, 0)
    ok = jnp.sum(jnp.where(depth == low, picked, 0.0), axis=0, keepdims=True)
    own_ok = ok[:, 2 * rep * n :]
    for s in range(2 * rep):
        ok_row = ok[:, s * n : (s + 1) * n]
        bias = to_column(jnp.where(ok_row > 0, 0.0, very_low))
        caption_bias[s] = jnp.broadcast_to(bias, (n, LANES))
        aim_column = to_column(aims[s].astype(jnp.float32)).astype(jnp.int32)
        target[s] = jnp.broadcast_to(aim_column, (n, LANES))
    for at, di, dv in offsets:
        for k in range(2):
            to = image_member(di, dv, k)
            flag = words[mod(to, G) * U + div(to, G)] & 1
            cols = slice((at * 2 + k) * n, (at * 2 + k + 1) * n)
            image_bias[:, cols] = jnp.where(flag > 0, 0.0, very_low)

    def fold(x, op):
        y = x[:, :LANES]
        for j in range(1, x.shape[1] // LANES):
            y = op(y, x[:, j * LANES : (j + 1) * LANES])
        return y

    def tally(s, cols, scores, first, rows):
        scaled = scores * log2_e
        bias, ids = image_bias[:, cols], image_ids[:, cols]
        old_peak = col_peak[:, cols]
        peak, match = old_peak, col_match[:, cols]
        wide = lambda x: jnp.concatenate([x] * (scores.shape[1] // LANES), axis=1)
        peaks = []
        for q in range(rows // SUBLANES):
            at = pl.ds(first + q * SUBLANES, SUBLANES)
            x = scaled[q * SUBLANES : (q + 1) * SUBLANES]
            peaks.append(jnp.maximum(fold(x + bias, jnp.maximum), row_peak[s, at]))
            peak = jnp.maximum(peak, x + wide(caption_bias[s, at]))
            picked = jnp.where(wide(target[s, at]) == ids, x, 0.0)
            row_match[s, at] = row_match[s, at] + fold(picked, jnp.add)
            match = match + picked
        total = col_total[:, cols] * jnp.exp2(old_peak - peak)
        for q in range(rows // SUBLANES):
            at = pl.ds(first + q * SUBLANES, SUBLANES)
            x = scaled[q * SUBLANES : (q + 1) * SUBLANES]
            powers = jnp.exp2(x + bias - wide(peaks[q]))
            row_total[s, at] = row_total[s, at] * jnp.exp2(row_peak[s, at] - peaks[q]) + fold(
                powers, jnp.add
            )
            row_peak[s, at] = peaks[q]
            total = total + jnp.exp2(x + wide(caption_bias[s, at]) - peak)
        col_peak[:, cols] = peak
        col_total[:, cols] = total
        col_match[:, cols] = match

    def score(s, count, start, stop, first, rows):
        left = caps[pl.ds(s, count), pl.ds(first, rows)].reshape(count * rows, width)
        right = imgs[start // n : stop // n].reshape(stop - start, width)
        scores = lax.dot_general(
            left, right, (((1,), (1,)), ((), ())), preferred_element_type=jnp.float32
        )
        for k in range(count):
            tally(s + k, slice(start, stop), scores[k * rows : (k + 1) * rows], first, rows)

    for at in range(early // (2 * n)):
        beside_came(at)

    @pl.loop(0, rep + 1)
    def _(e):
        for step in range(rep + 1):
            @pl.when(e == step)
            def _():
                for share, is_caption, k in pieces:
                    if min(rep, 1 + math.ceil(share * rep - 1) if k else is_caption ^ 1) != step:
                        continue
                    if is_caption:
                        relay_captions(1, k)
                    else:
                        for di in range(1, H):
                            for dv in range(1, V):
                                across_came(di, dv, k)
                                img_beside(di, dv, k).start()

        @pl.when((e > 0) & (e < rep))
        def _():
            came(caps.at[0], cap_recv.at[2 * CAPTION_PIECES + e - 1])
        score(e, 1, 0, early, 0, n)

    for at in range(early // (2 * n), H * V):
        beside_came(at)
    if early < C:
        score(0, rep + 1, early, C, 0, n)

    def row_copy(s):
        away, d = div(s, rep), mod(s, rep)
        uu = 2 * h + jnp.where(away == 0, near, 1 - near)
        at = half * rep + r
        return remote(
            rowsend.at[s], rowrecv.at[at], row_sent, row_came, member(uu, v, c, mod(r + d, rep))
        )

    def send_rows(s):
        peak = jnp.max(row_peak[s], axis=1, keepdims=True)
        total = jnp.sum(row_total[s] * jnp.exp2(row_peak[s] - peak), axis=1, keepdims=True)
        rowsend[s, 0:1, :] = to_row(peak)
        rowsend[s, 1:2, :] = to_row(total)
        rowsend[s, 2:3, :] = to_row(jnp.sum(row_match[s], axis=1, keepdims=True))
        stays = keeps_own & (s == 0)

        @pl.when(jnp.logical_not(stays))
        def _():
            row_copy(s).start()

        @pl.when(stays)
        def _():
            rowrecv[half * rep + r] = rowsend[s]

    @pl.loop(0, rep + 1)
    def _(s):
        send_rows(s)

    @pl.loop(1, rep)
    def _(d):
        @pl.loop(0, LAST_PIECES)
        def _(k):
            rows = n // LAST_PIECES
            came(
                caps.at[rep + d, pl.ds(0, rows)],
                cap_recv.at[2 * CAPTION_PIECES + rep - 1 + (d - 1) * LAST_PIECES + k],
            )

            score(rep + d, 1, 0, C, k * rows, rows)
        send_rows(rep + d)

    peak = jnp.max(col_peak[...], axis=0, keepdims=True)
    total = jnp.sum(col_total[...] * jnp.exp2(col_peak[...] - peak), axis=0, keepdims=True)
    match = jnp.sum(col_match[...], axis=0, keepdims=True)
    for at, di, dv in offsets:
        for k in range(2):
            slot = at * 2 + k
            cols = slice(slot * n, (slot + 1) * n)
            colsend[slot, 0:1, :] = peak[:, cols]
            colsend[slot, 1:2, :] = total[:, cols]
            colsend[slot, 2:3, :] = match[:, cols]
            if slot:
                back = group((H - di) % H, (V - dv) % V) * 2 + k
                remote(
                    colsend.at[slot], colrecv.at[back], col_sent, col_came,
                    image_member(di, dv, k),
                ).start()
    colrecv[0] = colsend[0]

    def joined(parts, count):
        peak = parts[0, 0:1, :]
        for s in range(1, count):
            peak = jnp.maximum(peak, parts[s, 0:1, :])
        total = jnp.zeros_like(peak)
        match = jnp.zeros_like(peak)
        for s in range(count):
            total += parts[s, 1:2, :] * jnp.exp2(parts[s, 0:1, :] - peak)
            match += parts[s, 2:3, :]
        return (peak - match) * ln_2 + jnp.log(total)

    @pl.when(keeps_own)
    def _():
        came(rowrecv.at[pl.ds(0, 2 * rep - 1)], row_came)

    @pl.when(jnp.logical_not(keeps_own))
    def _():
        came(rowrecv, row_came)

    caption_loss = own_ok * joined(rowrecv, 2 * rep)
    terms_ref[0:1, :] = caption_loss
    came(colrecv.at[pl.ds(0, H * B - 1)], col_came)
    image_loss = raw[0].astype(jnp.float32) * joined(colrecv, H * B)
    terms_ref[1:2, :] = image_loss
    own_sum = jnp.sum(caption_loss + image_loss, axis=1, keepdims=True)
    part[me] = jnp.broadcast_to(own_sum, (1, LANES))

    @pl.loop(1, N)
    def _(k):
        remote(part.at[me], part.at[me], part_sent, part_came, mod(me + k, N)).start()

    sent(words.at[pl.ds(0, U - 1)], line_sent)
    sent(words.at[pl.ds(0, (G - 1) * U)], plane_sent)
    sent(imgs.at[pl.ds(0, H * B - 1)], img_sent)

    @pl.when(keeps_own)
    def _():
        sent(caps.at[pl.ds(0, 2 * rep - 1)], cap_sent)
        sent(rowsend.at[pl.ds(0, 2 * rep - 1)], row_sent)

    @pl.when(jnp.logical_not(keeps_own))
    def _():
        sent(caps, cap_sent)
        sent(rowsend, row_sent)

    sent(colsend.at[pl.ds(0, H * B - 1)], col_sent)
    sent(part.at[pl.ds(0, N - 1)], part_sent)
    came(part.at[pl.ds(0, N - 1)], part_came)

    whole = jnp.sum(part[:, 0, :], axis=0, keepdims=True)
    terms_ref[2:3, 0:1] = whole[:, 0:1] / (2.0 * image_total)


def hand_out(terms_ref, closs_ref, iloss_ref, loss_ref):
    closs_ref[...] = terms_ref[0:1, :]
    iloss_ref[...] = terms_ref[1:2, :]
    loss_ref[...] = terms_ref[2:3, 0:1]


def local(blk, rep, captions, images, positives, valid):
    n, width = captions.shape
    U, V = grid_of(blk, rep)
    N = blk * rep
    H, B = U // 2, V * 2
    C = H * B * n
    f32, i32 = jnp.float32, jnp.int32
    _, _, image_sems, caption_sems = semaphore_counts(U, V, rep)
    dma = lambda count: pltpu.SemaphoreType.DMA((count,))
    vmem = pl.BlockSpec(memory_space=pltpu.VMEM)
    hbm = pl.BlockSpec(memory_space=pl.ANY)
    terms = pl.pallas_call(
        functools.partial(kernel, blk, rep),
        out_shape=pltpu.VMEM((SUBLANES, n), f32),
        in_specs=[hbm] * 4,
        out_specs=vmem,
        scratch_shapes=[
            pltpu.VMEM((n, width), captions.dtype),
            pltpu.VMEM((2 * rep, n, width), captions.dtype),
            pltpu.VMEM((H * B, n, width), images.dtype),
            pltpu.VMEM((2, 1, n), i32),
            pltpu.VMEM((N, 1, n), i32),
            pltpu.VMEM((1, C), f32),
            pltpu.VMEM((1, C), i32),
            pltpu.VMEM((2 * rep, n, LANES), i32),
            pltpu.VMEM((2 * rep, n, LANES), f32),
            pltpu.VMEM((2 * rep, n, LANES), f32),
            pltpu.VMEM((2 * rep, n, LANES), f32),
            pltpu.VMEM((2 * rep, n, LANES), f32),
            pltpu.VMEM((SUBLANES, C), f32),
            pltpu.VMEM((SUBLANES, C), f32),
            pltpu.VMEM((SUBLANES, C), f32),
            pltpu.VMEM((2 * rep, 8, n), f32),
            pltpu.VMEM((2 * rep, 8, n), f32),
            pltpu.VMEM((H * B, 8, n), f32),
            pltpu.VMEM((H * B, 8, n), f32),
            pltpu.VMEM((N, 1, LANES), f32),
            dma(5), dma(image_sems), dma(caption_sems), dma(7), dma(5),
        ],
        compiler_params=pltpu.CompilerParams(collective_id=0, has_side_effects=True),
    )(captions, images, positives.reshape(1, n), valid.reshape(1, n))
    caption_loss, image_loss, loss = pl.pallas_call(
        hand_out,
        out_shape=(
            jax.ShapeDtypeStruct((1, n), f32),
            jax.ShapeDtypeStruct((1, n), f32),
            jax.ShapeDtypeStruct((1, 1), f32),
        ),
        in_specs=[vmem],
        out_specs=(vmem,) * 3,
    )(pltpu.with_memory_space_constraint(terms, pltpu.VMEM))
    return caption_loss.reshape(n), image_loss.reshape(n), loss.reshape(())


def solution(mesh):
    placed = (
        P(("blk", "rep"), None),
        P(("blk", "rep"), None),
        P(("blk", "rep")),
        P(("blk", "rep")),
    )
    return jax.shard_map(
        functools.partial(local, mesh.shape["blk"], mesh.shape["rep"]),
        mesh=mesh,
        in_specs=placed,
        out_specs=(P(("blk", "rep")), P(("blk", "rep")), P()),
        check_vma=False,
    )
```

```python
import functools
import math

import jax
import jax.numpy as jnp
from jax import lax
from jax.experimental import pallas as pl
from jax.experimental.pallas import tpu as pltpu
from jax.sharding import PartitionSpec as P

very_low = -1e30
floor = -1e29
IMAGE_PIECES = 4
CAPTION_PIECES = 6
LAST_PIECES = 2
IMAGES_HELD = 1
CAPTIONS_HELD = 2
LANES = 128
SUBLANES = 8
log2_e = math.log2(math.e)
ln_2 = math.log(2)


def grid_of(blk, rep):
    chips = (blk // 2) * rep
    planes = 1
    while (planes * 2) ** 2 <= chips and (blk // 2) % (planes * 2) == 0:
        planes *= 2
    return planes, blk // 2 // planes


def mod(a, b):
    return a & (b - 1) if b & (b - 1) == 0 else lax.rem(a, b)


def div(a, b):
    return a >> (b.bit_length() - 1) if b & (b - 1) == 0 else lax.div(a, b)


def semaphore_counts(U, V, rep):
    H = U // 2
    along = (H - 1) * IMAGE_PIECES
    across = H * (V - 1) * IMAGE_PIECES
    return along, across, along + across + H * V, 2 * CAPTION_PIECES + (rep - 1) * (1 + LAST_PIECES)


def group_at(V, H, di, dv):
    if di == 0:
        return dv
    if dv == 0:
        return V + di - 1
    return V + H - 1 + (di - 1) * (V - 1) + dv - 1


def kernel(
    blk, rep, cap_ref, img_ref, pos_ref, val_ref, terms_ref,
    mine, caps, imgs, raw, words, image_bias, image_ids, target, caption_bias,
    row_peak, row_total, row_match, col_peak, col_total, col_match,
    rowsend, rowrecv, colsend, colrecv, part,
    loc_sem, img_recv, cap_recv, send_sem, recv_sem,
):
    U, V = grid_of(blk, rep)
    N = blk * rep
    G = N // U
    H = U // 2
    B = V * 2
    n, width = cap_ref.shape
    early = V + H - 1
    C = H * B * n
    along_sems, across_sems, _, _ = semaphore_counts(U, V, rep)
    b, r = lax.axis_index("blk"), lax.axis_index("rep")
    c = mod(b, 2)
    u = div(b, 2 * V)
    v = mod(div(b, 2), V)
    me = b * rep + r
    g = mod(me, G)
    half, h = div(u, H), mod(u, H)
    keeps_own = div(u, 2) == h
    img_sent, cap_sent, line_sent, plane_sent, row_sent, col_sent, part_sent = (
        send_sem.at[k] for k in range(7)
    )
    line_came, plane_came, row_came, col_came, part_came = (recv_sem.at[k] for k in range(5))

    def near_of(uu):
        return jnp.where(uu > 2 * mod(uu, H), 1, 0)

    near = near_of(u)

    def member(uu, vv, cc, rr):
        return ((uu * V + vv) * 2 + cc) * rep + rr

    def remote(src, dst, ss, rs, to):
        return pltpu.make_async_remote_copy(
            src_ref=src, dst_ref=dst, send_sem=ss, recv_sem=rs, device_id=to,
            device_id_type=pl.DeviceIdType.LOGICAL,
        )

    partner = member(u, v, 1 - c, r)

    def sent(ref, sem):
        remote(ref, ref, sem, img_recv.at[0], partner).wait_send()

    def came(ref, sem):
        remote(ref, ref, img_sent, sem, partner).wait_recv()

    barrier = pltpu.get_barrier_semaphore()
    others = [u * G + mod(g + k, G) for k in range(1, G)]
    others += [mod(u + k, U) * G + g for k in range(1, U)]
    for to in others:
        pl.semaphore_signal(
            barrier, inc=1, device_id=to, device_id_type=pl.DeviceIdType.LOGICAL
        )

    def group(di, dv):
        return group_at(V, H, di, dv)

    offsets = sorted((group(di, dv), di, dv) for di in range(H) for dv in range(V))

    def image_member(di, dv, k):
        return member(half * H + mod(h + di, H), mod(v + dv, V), c if k == 0 else 1 - c, r)

    load_val = pltpu.make_async_copy(val_ref, raw.at[0], loc_sem.at[0])
    load_pos = pltpu.make_async_copy(pos_ref, raw.at[1], loc_sem.at[1])
    load_img = pltpu.make_async_copy(img_ref, imgs.at[0], loc_sem.at[2])
    load_cap = pltpu.make_async_copy(cap_ref, mine, loc_sem.at[3])
    keep_cap = pltpu.make_async_copy(cap_ref, caps.at[0], loc_sem.at[4])
    load_val.start()
    load_pos.start()
    load_img.start()
    load_cap.start()

    @pl.when(keeps_own)
    def _():
        keep_cap.start()

    load_val.wait()
    load_pos.wait()
    words[g * U + u] = raw[1] * 2 + raw[0]
    load_img.wait()
    load_cap.wait()

    @pl.when(keeps_own)
    def _():
        keep_cap.wait()

    pl.semaphore_wait(barrier, len(others))

    def image_rows(k):
        return pl.ds(k * (n // IMAGE_PIECES), n // IMAGE_PIECES)

    def caption_rows(k):
        return pl.ds(k * (n // CAPTION_PIECES), n // CAPTION_PIECES)

    def img_copy(at, to_at, k, sem, to):
        rows = image_rows(k)
        return remote(imgs.at[at, rows], imgs.at[to_at, rows], img_sent, img_recv.at[sem], to)

    def across_sem(di, dv, k):
        return along_sems + (di * (V - 1) + dv - 1) * IMAGE_PIECES + k

    def img_along(d, k):
        to = member(half * H + mod(h + d, H), v, c, r)
        return img_copy(0, group(H - d, 0) * 2, k, (H - d - 1) * IMAGE_PIECES + k, to)

    def img_across(di, d, k):
        to = member(u, mod(v + d, V), c, r)
        return img_copy(
            group(di, 0) * 2, group(di, V - d) * 2, k, across_sem(di, V - d, k), to
        )

    def img_beside(di, dv, k):
        at = group(di, dv)
        return img_copy(at * 2, at * 2 + 1, k, along_sems + across_sems + at, partner)

    def along_came(di, k):
        came(imgs.at[group(di, 0) * 2, image_rows(k)], img_recv.at[(di - 1) * IMAGE_PIECES + k])

    def across_came(di, dv, k):
        came(imgs.at[group(di, dv) * 2, image_rows(k)], img_recv.at[across_sem(di, dv, k)])

    def beside_came(at):
        came(imgs.at[at * 2 + 1], img_recv.at[along_sems + across_sems + at])

    def cap_along(t, k):
        rows = caption_rows(k)
        to = t * H + div(u, 2)
        away = jnp.where(mod(u, 2) == near_of(to), 0, 1)
        return remote(
            mine.at[rows], caps.at[away * rep, rows], cap_sent,
            cap_recv.at[away * CAPTION_PIECES + k], member(to, v, c, r),
        )

    def cap_across(away, d, k):
        rows = caption_rows(k)
        seat = rep - d
        sem = 2 * CAPTION_PIECES + seat - 1
        if away:
            piece = k // (CAPTION_PIECES // LAST_PIECES)
            sem = 2 * CAPTION_PIECES + rep - 1 + (seat - 1) * LAST_PIECES + piece
        return remote(
            caps.at[away * rep, rows], caps.at[away * rep + seat, rows], cap_sent,
            cap_recv.at[sem], member(u, v, c, mod(r + d, rep)),
        )

    def relay_captions(away, k):
        came(caps.at[away * rep, caption_rows(k)], cap_recv.at[away * CAPTION_PIECES + k])
        for d in range(1, rep):
            cap_across(away, d, k).start()

    def line_copy(k):
        row = words.at[g * U + u]
        return remote(row, row, line_sent, line_came, mod(u + k, U) * G + g)

    def plane_copy(k):
        rows = words.at[pl.ds(g * U, U)]
        return remote(rows, rows, plane_sent, plane_came, u * G + mod(g + k, G))

    def own_across(k):
        for d in range(1, V):
            img_across(0, d, k).start()

    def own_captions_across(k):
        @pl.when(keeps_own)
        def _():
            for d in range(1, rep):
                cap_across(0, d, k).start()

    for k in range(1, U):
        line_copy(k).start()
    for k in range(IMAGE_PIECES):
        for d in range(1, H):
            img_along(d, k).start()
        if k < IMAGE_PIECES - IMAGES_HELD:
            own_across(k)
        img_beside(0, 0, k).start()
    for k in range(CAPTION_PIECES):
        for t in range(2):
            @pl.when(t * H + div(u, 2) != u)
            def _():
                cap_along(t, k).start()
        if k < CAPTION_PIECES - CAPTIONS_HELD:
            own_captions_across(k)

    for at, di, dv in offsets:
        for k in range(2):
            cols = slice((at * 2 + k) * n, (at * 2 + k + 1) * n)
            first = image_member(di, dv, k) * n
            image_ids[:, cols] = first + lax.broadcasted_iota(jnp.int32, (1, n), 1)
    col_peak[...] = jnp.full(col_peak.shape, floor, jnp.float32)
    col_total[...] = jnp.zeros(col_total.shape, jnp.float32)
    col_match[...] = jnp.zeros(col_match.shape, jnp.float32)
    row_peak[...] = jnp.full(row_peak.shape, floor, jnp.float32)
    row_total[...] = jnp.zeros(row_total.shape, jnp.float32)
    row_match[...] = jnp.zeros(row_match.shape, jnp.float32)

    came(words.at[pl.ds(0, U - 1)], line_came)
    for k in range(1, G):
        plane_copy(k).start()
    for k in range(IMAGE_PIECES - IMAGES_HELD, IMAGE_PIECES):
        own_across(k)
    for k in range(CAPTION_PIECES - CAPTIONS_HELD, CAPTION_PIECES):
        own_captions_across(k)

    def arrivals(lag):
        order = [((k + 1) / CAPTION_PIECES, False, k) for k in range(CAPTION_PIECES)]
        order += [((k + 1) / IMAGE_PIECES + lag, True, k) for k in range(IMAGE_PIECES)]
        return sorted(order)

    for _, is_image, k in arrivals(0):
        if not is_image:
            @pl.when(jnp.logical_not(keeps_own))
            def _():
                relay_captions(0, k)
        else:
            for di in range(1, H):
                along_came(di, k)
                for d in range(1, V):
                    img_across(di, d, k).start()
                img_beside(di, 0, k).start()
            for dv in range(1, V):
                across_came(0, dv, k)
                img_beside(0, dv, k).start()

    came(words.at[pl.ds(0, (G - 1) * U)], plane_came)

    eye = lax.broadcasted_iota(jnp.int32, (n, n), 0) == lax.broadcasted_iota(jnp.int32, (n, n), 1)

    def to_column(row):
        return jnp.sum(jnp.where(eye, row, 0.0), axis=1, keepdims=True)

    def to_row(column):
        return jnp.sum(jnp.where(eye, column, 0.0), axis=0, keepdims=True)

    flags = (words[:, 0, :] & 1).astype(jnp.float32)
    image_total = jnp.sum(jnp.sum(flags, axis=1, keepdims=True), axis=0, keepdims=True)

    def seat_row(s):
        away, d = div(s, rep), mod(s, rep)
        uu = 2 * h + jnp.where(away == 0, near, 1 - near)
        return ((v * 2 + c) * rep + mod(r + d, rep)) * U + uu

    aims = [words[seat_row(s)] >> 1 for s in range(2 * rep)] + [words[g * U + u] >> 1]
    aim = jnp.concatenate(aims, axis=1)
    order = lax.broadcasted_iota(jnp.int32, (N, aim.shape[1]), 0)
    starts = (mod(order, U) * G + div(order, U)) * n
    inside = (aim >= starts) & (aim < starts + n)
    picked = jnp.dot(
        flags.T.astype(jnp.bfloat16), jnp.where(inside, 1.0, 0.0).astype(jnp.bfloat16),
        preferred_element_type=jnp.float32,
    )
    start = jnp.sum(jnp.where(inside, starts, 0).astype(jnp.float32), axis=0, keepdims=True)
    low = aim - start.astype(jnp.int32)
    depth = lax.broadcasted_iota(jnp.int32, picked.shape, 0)
    ok = jnp.sum(jnp.where(depth == low, picked, 0.0), axis=0, keepdims=True)
    own_ok = ok[:, 2 * rep * n :] > 0
    for s in range(2 * rep):
        ok_row = ok[:, s * n : (s + 1) * n]
        bias = to_column(jnp.where(ok_row > 0, 0.0, very_low))
        caption_bias[s] = jnp.broadcast_to(bias, (n, LANES))
        aim_column = to_column(aims[s].astype(jnp.float32)).astype(jnp.int32)
        target[s] = jnp.broadcast_to(aim_column, (n, LANES))
    for at, di, dv in offsets:
        for k in range(2):
            to = image_member(di, dv, k)
            flag = words[mod(to, G) * U + div(to, G)] & 1
            cols = slice((at * 2 + k) * n, (at * 2 + k + 1) * n)
            image_bias[:, cols] = jnp.where(flag > 0, 0.0, very_low)

    def fold(x, op):
        y = x[:, :LANES]
        for j in range(1, x.shape[1] // LANES):
            y = op(y, x[:, j * LANES : (j + 1) * LANES])
        return y

    def tally(s, cols, scores, first, rows):
        scaled = scores * log2_e + image_bias[:, cols]
        ids = image_ids[:, cols]
        old_peak = col_peak[:, cols]
        peak, match = old_peak, col_match[:, cols]
        wide = lambda x: jnp.concatenate([x] * (scores.shape[1] // LANES), axis=1)
        held, peaks = [], []
        for q in range(rows // SUBLANES):
            at = pl.ds(first + q * SUBLANES, SUBLANES)
            x = scaled[q * SUBLANES : (q + 1) * SUBLANES] + wide(caption_bias[s, at])
            held.append(x)
            peaks.append(jnp.maximum(fold(x, jnp.maximum), row_peak[s, at]))
            peak = jnp.maximum(peak, x)
            picked = jnp.where(wide(target[s, at]) == ids, x, 0.0)
            row_match[s, at] = row_match[s, at] + fold(picked, jnp.add)
            match = match + picked
        total = col_total[:, cols] * jnp.exp2(old_peak - peak)
        for q in range(rows // SUBLANES):
            at = pl.ds(first + q * SUBLANES, SUBLANES)
            powers = jnp.exp2(held[q] - wide(peaks[q]))
            row_total[s, at] = row_total[s, at] * jnp.exp2(row_peak[s, at] - peaks[q]) + fold(
                powers, jnp.add
            )
            row_peak[s, at] = peaks[q]
            total = total + jnp.exp2(held[q] - peak)
        col_peak[:, cols] = peak
        col_total[:, cols] = total
        col_match[:, cols] = match

    def score(s, count, start, stop, first, rows):
        left = caps[pl.ds(s, count), pl.ds(first, rows)].reshape(count * rows, width)
        for at in range(start, stop):
            scores = lax.dot_general(
                left, imgs[2 * at : 2 * at + 2].reshape(2 * n, width), (((1,), (1,)), ((), ())),
                preferred_element_type=jnp.float32,
            )
            cols = slice(2 * at * n, 2 * (at + 1) * n)
            for k in range(count):
                tally(s + k, cols, scores[k * rows : (k + 1) * rows], first, rows)

    for at in range(early):
        beside_came(at)

    @pl.loop(0, rep + 1)
    def _(e):
        for step in range(rep + 1):
            @pl.when(e == step)
            def _():
                for share, is_image, k in arrivals(1 / IMAGE_PIECES):
                    if min(rep, math.ceil(share * CAPTION_PIECES) - 1) != step:
                        continue
                    if not is_image:
                        relay_captions(1, k)
                    else:
                        for di in range(1, H):
                            for dv in range(1, V):
                                across_came(di, dv, k)
                                img_beside(di, dv, k).start()

        @pl.when((e > 0) & (e < rep))
        def _():
            came(caps.at[0], cap_recv.at[2 * CAPTION_PIECES + e - 1])
        score(e, 1, 0, early, 0, n)

    for at in range(early, H * V):
        beside_came(at)
    score(0, rep + 1, early, H * V, 0, n)

    def row_copy(s):
        away, d = div(s, rep), mod(s, rep)
        uu = 2 * h + jnp.where(away == 0, near, 1 - near)
        at = half * rep + r
        return remote(
            rowsend.at[s], rowrecv.at[at], row_sent, row_came, member(uu, v, c, mod(r + d, rep))
        )

    def send_rows(s):
        peak = jnp.max(row_peak[s], axis=1, keepdims=True)
        total = jnp.sum(row_total[s] * jnp.exp2(row_peak[s] - peak), axis=1, keepdims=True)
        rowsend[s, 0:1, :] = to_row(peak)
        rowsend[s, 1:2, :] = to_row(total)
        rowsend[s, 2:3, :] = to_row(jnp.sum(row_match[s], axis=1, keepdims=True))
        stays = keeps_own & (s == 0)

        @pl.when(jnp.logical_not(stays))
        def _():
            row_copy(s).start()

        @pl.when(stays)
        def _():
            rowrecv[half * rep + r] = rowsend[s]

    for s in range(rep + 1):
        send_rows(s)

    @pl.loop(1, rep)
    def _(d):
        @pl.loop(0, LAST_PIECES)
        def _(k):
            rows = n // LAST_PIECES
            came(
                caps.at[rep + d, pl.ds(0, rows)],
                cap_recv.at[2 * CAPTION_PIECES + rep - 1 + (d - 1) * LAST_PIECES + k],
            )

            score(rep + d, 1, 0, H * V, k * rows, rows)
        send_rows(rep + d)

    peak = jnp.max(col_peak[...], axis=0, keepdims=True)
    total = jnp.sum(col_total[...] * jnp.exp2(col_peak[...] - peak), axis=0, keepdims=True)
    match = jnp.sum(col_match[...], axis=0, keepdims=True)
    for at, di, dv in offsets:
        for k in range(2):
            slot = at * 2 + k
            cols = slice(slot * n, (slot + 1) * n)
            colsend[slot, 0:1, :] = peak[:, cols]
            colsend[slot, 1:2, :] = total[:, cols]
            colsend[slot, 2:3, :] = match[:, cols]
            if slot:
                back = group((H - di) % H, (V - dv) % V) * 2 + k
                remote(
                    colsend.at[slot], colrecv.at[back], col_sent, col_came,
                    image_member(di, dv, k),
                ).start()
    colrecv[0] = colsend[0]

    def joined(parts, count):
        peak = parts[0, 0:1, :]
        for s in range(1, count):
            peak = jnp.maximum(peak, parts[s, 0:1, :])
        total = jnp.zeros_like(peak)
        match = jnp.zeros_like(peak)
        for s in range(count):
            total += parts[s, 1:2, :] * jnp.exp2(parts[s, 0:1, :] - peak)
            match += parts[s, 2:3, :]
        return (peak - match) * ln_2 + jnp.log(total)

    @pl.when(keeps_own)
    def _():
        came(rowrecv.at[pl.ds(0, 2 * rep - 1)], row_came)

    @pl.when(jnp.logical_not(keeps_own))
    def _():
        came(rowrecv, row_came)

    caption_loss = jnp.where(own_ok, joined(rowrecv, 2 * rep), 0.0)
    terms_ref[0:1, :] = caption_loss
    came(colrecv.at[pl.ds(0, H * B - 1)], col_came)
    image_loss = jnp.where(raw[0] > 0, joined(colrecv, H * B), 0.0)
    terms_ref[1:2, :] = image_loss
    own_sum = jnp.sum(caption_loss + image_loss, axis=1, keepdims=True)
    part[me] = jnp.broadcast_to(own_sum, (1, LANES))

    @pl.loop(1, N)
    def _(k):
        remote(part.at[me], part.at[me], part_sent, part_came, mod(me + k, N)).start()

    sent(words.at[pl.ds(0, U - 1)], line_sent)
    sent(words.at[pl.ds(0, (G - 1) * U)], plane_sent)
    sent(imgs.at[pl.ds(0, H * B - 1)], img_sent)

    @pl.when(keeps_own)
    def _():
        sent(caps.at[pl.ds(0, 2 * rep - 1)], cap_sent)
        sent(rowsend.at[pl.ds(0, 2 * rep - 1)], row_sent)

    @pl.when(jnp.logical_not(keeps_own))
    def _():
        sent(caps, cap_sent)
        sent(rowsend, row_sent)

    sent(colsend.at[pl.ds(0, H * B - 1)], col_sent)
    sent(part.at[pl.ds(0, N - 1)], part_sent)
    came(part.at[pl.ds(0, N - 1)], part_came)

    whole = jnp.sum(part[:, 0, :], axis=0, keepdims=True)
    terms_ref[2:3, 0:1] = whole[:, 0:1] / (2.0 * image_total)


def hand_out(terms_ref, closs_ref, iloss_ref, loss_ref):
    closs_ref[...] = terms_ref[0:1, :]
    iloss_ref[...] = terms_ref[1:2, :]
    loss_ref[...] = terms_ref[2:3, 0:1]


def local(blk, rep, captions, images, positives, valid):
    n, width = captions.shape
    U, V = grid_of(blk, rep)
    N = blk * rep
    H, B = U // 2, V * 2
    C = H * B * n
    f32, i32 = jnp.float32, jnp.int32
    _, _, image_sems, caption_sems = semaphore_counts(U, V, rep)
    dma = lambda count: pltpu.SemaphoreType.DMA((count,))
    vmem = pl.BlockSpec(memory_space=pltpu.VMEM)
    hbm = pl.BlockSpec(memory_space=pl.ANY)
    terms = pl.pallas_call(
        functools.partial(kernel, blk, rep),
        out_shape=pltpu.VMEM((SUBLANES, n), f32),
        in_specs=[hbm] * 4,
        out_specs=vmem,
        scratch_shapes=[
            pltpu.VMEM((n, width), captions.dtype),
            pltpu.VMEM((2 * rep, n, width), captions.dtype),
            pltpu.VMEM((H * B, n, width), images.dtype),
            pltpu.VMEM((2, 1, n), i32),
            pltpu.VMEM((N, 1, n), i32),
            pltpu.VMEM((1, C), f32),
            pltpu.VMEM((1, C), i32),
            pltpu.VMEM((2 * rep, n, LANES), i32),
            pltpu.VMEM((2 * rep, n, LANES), f32),
            pltpu.VMEM((2 * rep, n, LANES), f32),
            pltpu.VMEM((2 * rep, n, LANES), f32),
            pltpu.VMEM((2 * rep, n, LANES), f32),
            pltpu.VMEM((SUBLANES, C), f32),
            pltpu.VMEM((SUBLANES, C), f32),
            pltpu.VMEM((SUBLANES, C), f32),
            pltpu.VMEM((2 * rep, 8, n), f32),
            pltpu.VMEM((2 * rep, 8, n), f32),
            pltpu.VMEM((H * B, 8, n), f32),
            pltpu.VMEM((H * B, 8, n), f32),
            pltpu.VMEM((N, 1, LANES), f32),
            dma(5), dma(image_sems), dma(caption_sems), dma(7), dma(5),
        ],
        compiler_params=pltpu.CompilerParams(collective_id=0, has_side_effects=True),
    )(captions, images, positives.reshape(1, n), valid.reshape(1, n))
    caption_loss, image_loss, loss = pl.pallas_call(
        hand_out,
        out_shape=(
            jax.ShapeDtypeStruct((1, n), f32),
            jax.ShapeDtypeStruct((1, n), f32),
            jax.ShapeDtypeStruct((1, 1), f32),
        ),
        in_specs=[vmem],
        out_specs=(vmem,) * 3,
    )(pltpu.with_memory_space_constraint(terms, pltpu.VMEM))
    return caption_loss.reshape(n), image_loss.reshape(n), loss.reshape(())


def solution(mesh):
    placed = (
        P(("blk", "rep"), None),
        P(("blk", "rep"), None),
        P(("blk", "rep")),
        P(("blk", "rep")),
    )
    return jax.shard_map(
        functools.partial(local, mesh.shape["blk"], mesh.shape["rep"]),
        mesh=mesh,
        in_specs=placed,
        out_specs=(P(("blk", "rep")), P(("blk", "rep")), P()),
        check_vma=False,
    )
```

```python
import functools
import math

import jax
import jax.numpy as jnp
from jax import lax
from jax.experimental import pallas as pl
from jax.experimental.pallas import tpu as pltpu
from jax.sharding import PartitionSpec as P

very_low = -1e30
floor = -1e29
IMAGE_PIECES = 4
CAPTION_PIECES = 6
LAST_PIECES = 2
IMAGES_HELD = 1
CAPTIONS_HELD = 2
LANES = 128
SUBLANES = 8
log2_e = math.log2(math.e)
ln_2 = math.log(2)


def grid_of(blk, rep):
    chips = (blk // 2) * rep
    planes = 1
    while (planes * 2) ** 2 <= chips and (blk // 2) % (planes * 2) == 0:
        planes *= 2
    return planes, blk // 2 // planes


def mod(a, b):
    return a & (b - 1) if b & (b - 1) == 0 else lax.rem(a, b)


def div(a, b):
    return a >> (b.bit_length() - 1) if b & (b - 1) == 0 else lax.div(a, b)


def semaphore_counts(U, V, rep):
    H = U // 2
    along = (H - 1) * IMAGE_PIECES
    across = H * (V - 1) * IMAGE_PIECES
    return along, across, along + across + H * V, 2 * CAPTION_PIECES + (rep - 1) * (1 + LAST_PIECES)


def group_at(V, H, di, dv):
    if di == 0:
        return dv
    if dv == 0:
        return V + di - 1
    return V + H - 1 + (di - 1) * (V - 1) + dv - 1


def kernel(
    blk, rep, cap_ref, img_ref, pos_ref, val_ref, terms_ref,
    mine, caps, imgs, raw, words, image_bias, image_ids, target, caption_bias, caption_ok,
    row_peak, row_total, row_match, col_peak, col_total, col_match,
    rowsend, rowrecv, rowpool, colsend, colrecv, colpool, part, spare,
    loc_sem, img_recv, cap_recv, send_sem, recv_sem,
):
    U, V = grid_of(blk, rep)
    N = blk * rep
    G = N // U
    H = U // 2
    B = V * 2
    n, width = cap_ref.shape
    early = V + H - 1
    C = H * B * n
    along_sems, across_sems, _, _ = semaphore_counts(U, V, rep)
    b, r = lax.axis_index("blk"), lax.axis_index("rep")
    c = mod(b, 2)
    u = div(b, 2 * V)
    v = mod(div(b, 2), V)
    me = b * rep + r
    g = mod(me, G)
    half, h = div(u, H), mod(u, H)
    keeps_own = div(u, 2) == h
    img_sent, cap_sent, line_sent, plane_sent, row_sent, col_sent, row_given, col_given, part_sent = (
        send_sem.at[k] for k in range(9)
    )
    line_came, plane_came, row_came, col_came, row_pooled, col_pooled, part_came = (
        recv_sem.at[k] for k in range(7)
    )
    pools = (c == 1) & ((u == H - 1) | (u == H))

    def pool_of(uu, vv, rr):
        return member(H - 1 + div(uu, H), vv, 1, rr)

    def near_of(uu):
        return jnp.where(uu > 2 * mod(uu, H), 1, 0)

    near = near_of(u)

    def member(uu, vv, cc, rr):
        return ((uu * V + vv) * 2 + cc) * rep + rr

    def remote(src, dst, ss, rs, to):
        return pltpu.make_async_remote_copy(
            src_ref=src, dst_ref=dst, send_sem=ss, recv_sem=rs, device_id=to,
            device_id_type=pl.DeviceIdType.LOGICAL,
        )

    partner = member(u, v, 1 - c, r)

    def sent(ref, sem):
        remote(ref, ref, sem, img_recv.at[0], partner).wait_send()

    def came(ref, sem):
        remote(ref, ref, img_sent, sem, partner).wait_recv()

    barrier = pltpu.get_barrier_semaphore()
    others = [u * G + mod(g + k, G) for k in range(1, G)]
    others += [mod(u + k, U) * G + g for k in range(1, U)]
    for to in others:
        pl.semaphore_signal(
            barrier, inc=1, device_id=to, device_id_type=pl.DeviceIdType.LOGICAL
        )

    def group(di, dv):
        return group_at(V, H, di, dv)

    offsets = sorted((group(di, dv), di, dv) for di in range(H) for dv in range(V))

    def image_member(di, dv, k):
        return member(half * H + mod(h + di, H), mod(v + dv, V), c if k == 0 else 1 - c, r)

    load_val = pltpu.make_async_copy(val_ref, raw.at[0], loc_sem.at[0])
    load_pos = pltpu.make_async_copy(pos_ref, raw.at[1], loc_sem.at[1])
    load_img = pltpu.make_async_copy(img_ref, imgs.at[0], loc_sem.at[2])
    load_cap = pltpu.make_async_copy(cap_ref, mine, loc_sem.at[3])
    keep_cap = pltpu.make_async_copy(cap_ref, caps.at[0], loc_sem.at[4])
    load_val.start()
    load_pos.start()
    load_img.start()
    load_cap.start()

    @pl.when(keeps_own)
    def _():
        keep_cap.start()

    load_val.wait()
    load_pos.wait()
    words[g * U + u] = raw[1] * 2 + raw[0]
    load_img.wait()
    load_cap.wait()

    @pl.when(keeps_own)
    def _():
        keep_cap.wait()

    pl.semaphore_wait(barrier, len(others))

    def image_rows(k):
        return pl.ds(k * (n // IMAGE_PIECES), n // IMAGE_PIECES)

    def caption_rows(k):
        return pl.ds(k * (n // CAPTION_PIECES), n // CAPTION_PIECES)

    def img_copy(at, to_at, k, sem, to):
        rows = image_rows(k)
        return remote(imgs.at[at, rows], imgs.at[to_at, rows], img_sent, img_recv.at[sem], to)

    def across_sem(di, dv, k):
        return along_sems + (di * (V - 1) + dv - 1) * IMAGE_PIECES + k

    def img_along(d, k):
        to = member(half * H + mod(h + d, H), v, c, r)
        return img_copy(0, group(H - d, 0) * 2, k, (H - d - 1) * IMAGE_PIECES + k, to)

    def img_across(di, d, k):
        to = member(u, mod(v + d, V), c, r)
        return img_copy(
            group(di, 0) * 2, group(di, V - d) * 2, k, across_sem(di, V - d, k), to
        )

    def img_beside(di, dv, k):
        at = group(di, dv)
        return img_copy(at * 2, at * 2 + 1, k, along_sems + across_sems + at, partner)

    def along_came(di, k):
        came(imgs.at[group(di, 0) * 2, image_rows(k)], img_recv.at[(di - 1) * IMAGE_PIECES + k])

    def across_came(di, dv, k):
        came(imgs.at[group(di, dv) * 2, image_rows(k)], img_recv.at[across_sem(di, dv, k)])

    def beside_came(at):
        came(imgs.at[at * 2 + 1], img_recv.at[along_sems + across_sems + at])

    def cap_along(t, k):
        rows = caption_rows(k)
        to = t * H + div(u, 2)
        away = jnp.where(mod(u, 2) == near_of(to), 0, 1)
        return remote(
            mine.at[rows], caps.at[away * rep, rows], cap_sent,
            cap_recv.at[away * CAPTION_PIECES + k], member(to, v, c, r),
        )

    def cap_across(away, d, k):
        rows = caption_rows(k)
        seat = rep - d
        sem = 2 * CAPTION_PIECES + seat - 1
        if away:
            piece = k // (CAPTION_PIECES // LAST_PIECES)
            sem = 2 * CAPTION_PIECES + rep - 1 + (seat - 1) * LAST_PIECES + piece
        return remote(
            caps.at[away * rep, rows], caps.at[away * rep + seat, rows], cap_sent,
            cap_recv.at[sem], member(u, v, c, mod(r + d, rep)),
        )

    def relay_captions(away, k):
        came(caps.at[away * rep, caption_rows(k)], cap_recv.at[away * CAPTION_PIECES + k])
        for d in range(1, rep):
            cap_across(away, d, k).start()

    def line_copy(k):
        row = words.at[g * U + u]
        return remote(row, row, line_sent, line_came, mod(u + k, U) * G + g)

    def plane_copy(k):
        rows = words.at[pl.ds(g * U, U)]
        return remote(rows, rows, plane_sent, plane_came, u * G + mod(g + k, G))

    def own_across(k):
        for d in range(1, V):
            img_across(0, d, k).start()

    def own_captions_across(k):
        @pl.when(keeps_own)
        def _():
            for d in range(1, rep):
                cap_across(0, d, k).start()

    for k in range(1, U):
        line_copy(k).start()
    for k in range(IMAGE_PIECES):
        for d in range(1, H):
            img_along(d, k).start()
        if k < IMAGE_PIECES - IMAGES_HELD:
            own_across(k)
        img_beside(0, 0, k).start()
    for k in range(CAPTION_PIECES):
        for t in range(2):
            @pl.when(t * H + div(u, 2) != u)
            def _():
                cap_along(t, k).start()
        if k < CAPTION_PIECES - CAPTIONS_HELD:
            own_captions_across(k)

    for at, di, dv in offsets:
        for k in range(2):
            cols = slice((at * 2 + k) * n, (at * 2 + k + 1) * n)
            first = image_member(di, dv, k) * n
            image_ids[:, cols] = first + lax.broadcasted_iota(jnp.int32, (1, n), 1)
    col_peak[...] = jnp.full(col_peak.shape, floor, jnp.float32)
    col_total[...] = jnp.zeros(col_total.shape, jnp.float32)
    col_match[...] = jnp.zeros(col_match.shape, jnp.float32)
    row_peak[...] = jnp.full(row_peak.shape, floor, jnp.float32)
    row_total[...] = jnp.zeros(row_total.shape, jnp.float32)
    row_match[...] = jnp.zeros(row_match.shape, jnp.float32)

    came(words.at[pl.ds(0, U - 1)], line_came)
    for k in range(1, G):
        plane_copy(k).start()
    for k in range(IMAGE_PIECES - IMAGES_HELD, IMAGE_PIECES):
        own_across(k)
    for k in range(CAPTION_PIECES - CAPTIONS_HELD, CAPTION_PIECES):
        own_captions_across(k)

    def arrivals(lag):
        order = [((k + 1) / CAPTION_PIECES, False, k) for k in range(CAPTION_PIECES)]
        order += [((k + 1) / IMAGE_PIECES + lag, True, k) for k in range(IMAGE_PIECES)]
        return sorted(order)

    for _, is_image, k in arrivals(0):
        if not is_image:
            @pl.when(jnp.logical_not(keeps_own))
            def _():
                relay_captions(0, k)
        else:
            for di in range(1, H):
                along_came(di, k)
                for d in range(1, V):
                    img_across(di, d, k).start()
                img_beside(di, 0, k).start()
            for dv in range(1, V):
                across_came(0, dv, k)
                img_beside(0, dv, k).start()

    came(words.at[pl.ds(0, (G - 1) * U)], plane_came)

    eye = lax.broadcasted_iota(jnp.int32, (n, n), 0) == lax.broadcasted_iota(jnp.int32, (n, n), 1)

    def to_column(row):
        return jnp.sum(jnp.where(eye, row, 0.0), axis=1, keepdims=True)

    def to_row(column):
        return jnp.sum(jnp.where(eye, column, 0.0), axis=0, keepdims=True)

    flags = (words[:, 0, :] & 1).astype(jnp.float32)
    image_total = jnp.sum(jnp.sum(flags, axis=1, keepdims=True), axis=0, keepdims=True)

    def seat_row(s):
        away, d = div(s, rep), mod(s, rep)
        uu = 2 * h + jnp.where(away == 0, near, 1 - near)
        return ((v * 2 + c) * rep + mod(r + d, rep)) * U + uu

    aims = [words[seat_row(s)] >> 1 for s in range(2 * rep)]
    aim = jnp.concatenate(aims, axis=1)
    order = lax.broadcasted_iota(jnp.int32, (N, aim.shape[1]), 0)
    starts = (mod(order, U) * G + div(order, U)) * n
    inside = (aim >= starts) & (aim < starts + n)
    picked = jnp.dot(
        flags.T.astype(jnp.bfloat16), jnp.where(inside, 1.0, 0.0).astype(jnp.bfloat16),
        preferred_element_type=jnp.float32,
    )
    start = jnp.sum(jnp.where(inside, starts, 0).astype(jnp.float32), axis=0, keepdims=True)
    low = aim - start.astype(jnp.int32)
    depth = lax.broadcasted_iota(jnp.int32, picked.shape, 0)
    ok = jnp.sum(jnp.where(depth == low, picked, 0.0), axis=0, keepdims=True)
    for s in range(2 * rep):
        ok_row = ok[:, s * n : (s + 1) * n]
        caption_ok[s] = ok_row
        bias = to_column(jnp.where(ok_row > 0, 0.0, very_low))
        caption_bias[s] = jnp.broadcast_to(bias, (n, LANES))
        aim_column = to_column(aims[s].astype(jnp.float32)).astype(jnp.int32)
        target[s] = jnp.broadcast_to(aim_column, (n, LANES))
    for at, di, dv in offsets:
        for k in range(2):
            to = image_member(di, dv, k)
            flag = words[mod(to, G) * U + div(to, G)] & 1
            cols = slice((at * 2 + k) * n, (at * 2 + k + 1) * n)
            image_bias[:, cols] = jnp.where(flag > 0, 0.0, very_low)

    def fold(x, op):
        y = x[:, :LANES]
        for j in range(1, x.shape[1] // LANES):
            y = op(y, x[:, j * LANES : (j + 1) * LANES])
        return y

    def tally(s, cols, scores, first, rows):
        scaled = scores * log2_e + image_bias[:, cols]
        ids = image_ids[:, cols]
        old_peak = col_peak[:, cols]
        peak, match = old_peak, col_match[:, cols]
        wide = lambda x: jnp.concatenate([x] * (scores.shape[1] // LANES), axis=1)
        held, peaks = [], []
        for q in range(rows // SUBLANES):
            at = pl.ds(first + q * SUBLANES, SUBLANES)
            x = scaled[q * SUBLANES : (q + 1) * SUBLANES] + wide(caption_bias[s, at])
            held.append(x)
            peaks.append(jnp.maximum(fold(x, jnp.maximum), row_peak[s, at]))
            peak = jnp.maximum(peak, x)
            picked = jnp.where(wide(target[s, at]) == ids, x, 0.0)
            row_match[s, at] = row_match[s, at] + fold(picked, jnp.add)
            match = match + picked
        total = col_total[:, cols] * jnp.exp2(old_peak - peak)
        for q in range(rows // SUBLANES):
            at = pl.ds(first + q * SUBLANES, SUBLANES)
            powers = jnp.exp2(held[q] - wide(peaks[q]))
            row_total[s, at] = row_total[s, at] * jnp.exp2(row_peak[s, at] - peaks[q]) + fold(
                powers, jnp.add
            )
            row_peak[s, at] = peaks[q]
            total = total + jnp.exp2(held[q] - peak)
        col_peak[:, cols] = peak
        col_total[:, cols] = total
        col_match[:, cols] = match

    def score(s, count, start, stop, first, rows):
        left = caps[pl.ds(s, count), pl.ds(first, rows)].reshape(count * rows, width)
        for at in range(start, stop):
            scores = lax.dot_general(
                left, imgs[2 * at : 2 * at + 2].reshape(2 * n, width), (((1,), (1,)), ((), ())),
                preferred_element_type=jnp.float32,
            )
            cols = slice(2 * at * n, 2 * (at + 1) * n)
            for k in range(count):
                tally(s + k, cols, scores[k * rows : (k + 1) * rows], first, rows)

    for at in range(early):
        beside_came(at)

    @pl.loop(0, rep + 1)
    def _(e):
        for step in range(rep + 1):
            @pl.when(e == step)
            def _():
                for share, is_image, k in arrivals(1 / IMAGE_PIECES):
                    if min(rep, math.ceil(share * CAPTION_PIECES) - 1) != step:
                        continue
                    if not is_image:
                        relay_captions(1, k)
                    else:
                        for di in range(1, H):
                            for dv in range(1, V):
                                across_came(di, dv, k)
                                img_beside(di, dv, k).start()

        @pl.when((e > 0) & (e < rep))
        def _():
            came(caps.at[0], cap_recv.at[2 * CAPTION_PIECES + e - 1])
        score(e, 1, 0, early, 0, n)

    for at in range(early, H * V):
        beside_came(at)
    score(0, rep + 1, early, H * V, 0, n)

    stride = pl.cdiv(n, LANES) * LANES

    def pack(ref, at, ok, first, peak, total, match):
        ref[at, :, 0:n] = jnp.where(ok, peak, 0.0)
        ref[at, :, stride : stride + n] = jnp.where(ok, total, jnp.where(first, 1.0, 0.0))
        ref[at, :, 2 * stride : 2 * stride + n] = jnp.where(ok, match, 0.0)

    def send_rows(s):
        away, d = div(s, rep), mod(s, rep)
        uu = 2 * h + jnp.where(away == 0, near, 1 - near)
        rr = mod(r + d, rep)
        at = half * rep + r
        peak = jnp.max(row_peak[s], axis=1, keepdims=True)
        total = jnp.sum(row_total[s] * jnp.exp2(row_peak[s] - peak), axis=1, keepdims=True)
        match = jnp.sum(row_match[s], axis=1, keepdims=True)
        pack(rowsend, s, caption_ok[s] > 0, at == 0, to_row(peak), to_row(total), to_row(match))
        remote(
            rowsend.at[s], rowpool.at[(mod(uu, H) * 2 + c) * 2 * rep + at], row_given, row_pooled,
            pool_of(uu, v, rr),
        ).start()
        stays = keeps_own & (s == 0)

        @pl.when(jnp.logical_not(stays))
        def _():
            remote(
                rowsend.at[s], rowrecv.at[at], row_sent, row_came, member(uu, v, c, rr)
            ).start()

        @pl.when(stays)
        def _():
            rowrecv[at] = rowsend[s]

    for s in range(rep + 1):
        send_rows(s)

    @pl.loop(1, rep)
    def _(d):
        @pl.loop(0, LAST_PIECES)
        def _(k):
            rows = n // LAST_PIECES
            came(
                caps.at[rep + d, pl.ds(0, rows)],
                cap_recv.at[2 * CAPTION_PIECES + rep - 1 + (d - 1) * LAST_PIECES + k],
            )

            score(rep + d, 1, 0, H * V, k * rows, rows)
        send_rows(rep + d)

    peak = jnp.max(col_peak[...], axis=0, keepdims=True)
    total = jnp.sum(col_total[...] * jnp.exp2(col_peak[...] - peak), axis=0, keepdims=True)
    match = jnp.sum(col_match[...], axis=0, keepdims=True)
    for at, di, dv in offsets:
        for k in range(2):
            slot = at * 2 + k
            cols = slice(slot * n, (slot + 1) * n)
            back = group((H - di) % H, (V - dv) % V) * 2 + k
            pack(
                colsend, slot, image_bias[:, cols] == 0, back == 0, peak[:, cols], total[:, cols],
                match[:, cols],
            )
    for at, di, dv in reversed(offsets):
        for k in range(2):
            slot = at * 2 + k
            back = group((H - di) % H, (V - dv) % V) * 2 + k
            cc = c if k == 0 else 1 - c
            seat = (mod(h + di, H) * 2 + cc) * H * B + back

            def give():
                remote(
                    colsend.at[slot], colpool.at[seat], col_given, col_pooled,
                    pool_of(u, mod(v + dv, V), r),
                ).start()

            if dv:
                give()
            else:
                @pl.when(pools)
                def _():
                    colpool[seat] = colsend[slot]

                pl.when(jnp.logical_not(pools))(give)
    for at, di, dv in reversed(offsets):
        for k in range(2):
            slot = at * 2 + k
            if slot:
                back = group((H - di) % H, (V - dv) % V) * 2 + k
                remote(
                    colsend.at[slot], colrecv.at[back], col_sent, col_came,
                    image_member(di, dv, k),
                ).start()
    colrecv[0] = colsend[0]

    def joined(parts, first, count):
        piece = lambda s, k: parts[first + s, :, k * stride : k * stride + n]
        peak = piece(0, 0)
        for s in range(1, count):
            peak = jnp.maximum(peak, piece(s, 0))
        total = jnp.zeros_like(peak)
        match = jnp.zeros_like(peak)
        for s in range(count):
            total += piece(s, 1) * jnp.exp2(piece(s, 0) - peak)
            match += piece(s, 2)
        return (peak - match) * ln_2 + jnp.log(total)

    pool_count = 2 * V * rep
    own_pool = (half * V + v) * rep + r

    @pl.when(pools)
    def _():
        came(rowpool, row_pooled)
        whole = jnp.zeros((1, n), jnp.float32)
        for k in range(2 * H):
            whole += joined(rowpool, k * 2 * rep, 2 * rep)
        came(colpool.at[pl.ds(0, 2 * H * (H * B - 1))], col_pooled)
        for k in range(2 * H):
            whole += joined(colpool, k * H * B, H * B)
        part[own_pool] = jnp.broadcast_to(jnp.sum(whole, axis=1, keepdims=True), (1, LANES))

        @pl.loop(0, N)
        def _(k):
            uu = div(k, G)
            to = jnp.where(u < H, U - 1 - uu, uu) * G + mod(k, G)

            @pl.when(to != me)
            def _():
                remote(part.at[own_pool], part.at[own_pool], part_sent, part_came, to).start()

    @pl.when(keeps_own)
    def _():
        came(rowrecv.at[pl.ds(0, 2 * rep - 1)], row_came)

    @pl.when(jnp.logical_not(keeps_own))
    def _():
        came(rowrecv, row_came)

    terms_ref[0:1, :] = joined(rowrecv, 0, 2 * rep)
    came(colrecv.at[pl.ds(0, H * B - 1)], col_came)
    terms_ref[1:2, :] = joined(colrecv, 0, H * B)

    sent(words.at[pl.ds(0, U - 1)], line_sent)
    sent(words.at[pl.ds(0, (G - 1) * U)], plane_sent)
    sent(imgs.at[pl.ds(0, H * B - 1)], img_sent)

    @pl.when(keeps_own)
    def _():
        sent(caps.at[pl.ds(0, 2 * rep - 1)], cap_sent)
        sent(rowsend.at[pl.ds(0, 2 * rep - 1)], row_sent)

    @pl.when(jnp.logical_not(keeps_own))
    def _():
        sent(caps, cap_sent)
        sent(rowsend, row_sent)

    sent(rowsend, row_given)
    sent(colsend.at[pl.ds(0, H * B - 1)], col_sent)

    @pl.when(pools)
    def _():
        sent(colsend.at[pl.ds(0, H * B - 2 * H)], col_given)
        sent(spare.at[pl.ds(0, N - 1)], part_sent)
        came(part.at[pl.ds(0, pool_count - 1)], part_came)

    @pl.when(jnp.logical_not(pools))
    def _():
        sent(colsend, col_given)
        came(part, part_came)

    whole = jnp.sum(part[:, 0, :], axis=0, keepdims=True)
    terms_ref[2:3, 0:1] = whole[:, 0:1] / (2.0 * image_total)


def hand_out(terms_ref, closs_ref, iloss_ref, loss_ref):
    closs_ref[...] = terms_ref[0:1, :]
    iloss_ref[...] = terms_ref[1:2, :]
    loss_ref[...] = terms_ref[2:3, 0:1]


def local(blk, rep, captions, images, positives, valid):
    n, width = captions.shape
    U, V = grid_of(blk, rep)
    N = blk * rep
    H, B = U // 2, V * 2
    C = H * B * n
    packed = 3 * pl.cdiv(n, LANES) * LANES
    f32, i32 = jnp.float32, jnp.int32
    _, _, image_sems, caption_sems = semaphore_counts(U, V, rep)
    dma = lambda count: pltpu.SemaphoreType.DMA((count,))
    vmem = pl.BlockSpec(memory_space=pltpu.VMEM)
    hbm = pl.BlockSpec(memory_space=pl.ANY)
    terms = pl.pallas_call(
        functools.partial(kernel, blk, rep),
        out_shape=pltpu.VMEM((SUBLANES, n), f32),
        in_specs=[hbm] * 4,
        out_specs=vmem,
        scratch_shapes=[
            pltpu.VMEM((n, width), captions.dtype),
            pltpu.VMEM((2 * rep, n, width), captions.dtype),
            pltpu.VMEM((H * B, n, width), images.dtype),
            pltpu.VMEM((2, 1, n), i32),
            pltpu.VMEM((N, 1, n), i32),
            pltpu.VMEM((1, C), f32),
            pltpu.VMEM((1, C), i32),
            pltpu.VMEM((2 * rep, n, LANES), i32),
            pltpu.VMEM((2 * rep, n, LANES), f32),
            pltpu.VMEM((2 * rep, 1, n), f32),
            pltpu.VMEM((2 * rep, n, LANES), f32),
            pltpu.VMEM((2 * rep, n, LANES), f32),
            pltpu.VMEM((2 * rep, n, LANES), f32),
            pltpu.VMEM((SUBLANES, C), f32),
            pltpu.VMEM((SUBLANES, C), f32),
            pltpu.VMEM((SUBLANES, C), f32),
            pltpu.VMEM((2 * rep, 1, packed), f32),
            pltpu.VMEM((2 * rep, 1, packed), f32),
            pltpu.VMEM((2 * H * 2 * rep, 1, packed), f32),
            pltpu.VMEM((H * B, 1, packed), f32),
            pltpu.VMEM((H * B, 1, packed), f32),
            pltpu.VMEM((2 * H * H * B, 1, packed), f32),
            pltpu.VMEM((2 * V * rep, 1, LANES), f32),
            pltpu.VMEM((N, 1, LANES), f32),
            dma(5), dma(image_sems), dma(caption_sems), dma(9), dma(7),
        ],
        compiler_params=pltpu.CompilerParams(collective_id=0, has_side_effects=True),
    )(captions, images, positives.reshape(1, n), valid.reshape(1, n))
    caption_loss, image_loss, loss = pl.pallas_call(
        hand_out,
        out_shape=(
            jax.ShapeDtypeStruct((1, n), f32),
            jax.ShapeDtypeStruct((1, n), f32),
            jax.ShapeDtypeStruct((1, 1), f32),
        ),
        in_specs=[vmem],
        out_specs=(vmem,) * 3,
    )(pltpu.with_memory_space_constraint(terms, pltpu.VMEM))
    return caption_loss.reshape(n), image_loss.reshape(n), loss.reshape(())


def solution(mesh):
    placed = (
        P(("blk", "rep"), None),
        P(("blk", "rep"), None),
        P(("blk", "rep")),
        P(("blk", "rep")),
    )
    return jax.shard_map(
        functools.partial(local, mesh.shape["blk"], mesh.shape["rep"]),
        mesh=mesh,
        in_specs=placed,
        out_specs=(P(("blk", "rep")), P(("blk", "rep")), P()),
        check_vma=False,
    )
```

```python
import functools
import math

import jax
import jax.numpy as jnp
from jax import lax
from jax.experimental import pallas as pl
from jax.experimental.pallas import tpu as pltpu
from jax.sharding import PartitionSpec as P

very_low = -1e30
floor = -1e29
IMAGE_PIECES = 4
CAPTION_PIECES = 6
LAST_PIECES = 2
IMAGES_HELD = 1
CAPTIONS_HELD = 2
FAR_FIRST = 2
LATE_LAST = 2
LANES = 128
SUBLANES = 8
log2_e = math.log2(math.e)
ln_2 = math.log(2)


def grid_of(blk, rep):
    chips = (blk // 2) * rep
    planes = 1
    while (planes * 2) ** 2 <= chips and (blk // 2) % (planes * 2) == 0:
        planes *= 2
    return planes, blk // 2 // planes


def mod(a, b):
    return a & (b - 1) if b & (b - 1) == 0 else lax.rem(a, b)


def div(a, b):
    return a >> (b.bit_length() - 1) if b & (b - 1) == 0 else lax.div(a, b)


def semaphore_counts(U, V, rep):
    H = U // 2
    along = (H - 1) * IMAGE_PIECES
    across = H * (V - 1) * IMAGE_PIECES
    return along, across, along + across + H * V, 2 * CAPTION_PIECES + (rep - 1) * (1 + LAST_PIECES)


def group_at(V, H, di, dv):
    if di == 0:
        return dv
    if dv == 0:
        return V + di - 1
    return V + H - 1 + (di - 1) * (V - 1) + dv - 1


def kernel(
    blk, rep, cap_ref, img_ref, pos_ref, val_ref, terms_ref,
    mine, caps, imgs, raw, words, image_bias, image_ids, target, caption_bias, caption_ok,
    row_peak, row_total, row_match, col_peak, col_total, col_match,
    rowsend, rowrecv, rowpool, colsend, colrecv, colpool, part, spare,
    loc_sem, img_recv, cap_recv, send_sem, recv_sem,
):
    U, V = grid_of(blk, rep)
    N = blk * rep
    G = N // U
    H = U // 2
    B = V * 2
    n, width = cap_ref.shape
    early = V + H - 1
    C = H * B * n
    along_sems, across_sems, _, _ = semaphore_counts(U, V, rep)
    b, r = lax.axis_index("blk"), lax.axis_index("rep")
    c = mod(b, 2)
    u = div(b, 2 * V)
    v = mod(div(b, 2), V)
    me = b * rep + r
    g = mod(me, G)
    half, h = div(u, H), mod(u, H)
    keeps_own = div(u, 2) == h
    img_sent, cap_sent, line_sent, plane_sent, row_sent, col_sent, row_given, col_given, part_sent = (
        send_sem.at[k] for k in range(9)
    )
    line_came, plane_came, row_came, col_came, row_pooled, col_pooled, part_came = (
        recv_sem.at[k] for k in range(7)
    )
    pools = (c == 1) & ((u == H - 1) | (u == H))

    def pool_of(uu, vv, rr):
        return member(H - 1 + div(uu, H), vv, 1, rr)

    def near_of(uu):
        return jnp.where(uu > 2 * mod(uu, H), 1, 0)

    near = near_of(u)

    def member(uu, vv, cc, rr):
        return ((uu * V + vv) * 2 + cc) * rep + rr

    def remote(src, dst, ss, rs, to):
        return pltpu.make_async_remote_copy(
            src_ref=src, dst_ref=dst, send_sem=ss, recv_sem=rs, device_id=to,
            device_id_type=pl.DeviceIdType.LOGICAL,
        )

    partner = member(u, v, 1 - c, r)

    def sent(ref, sem):
        remote(ref, ref, sem, img_recv.at[0], partner).wait_send()

    def came(ref, sem):
        remote(ref, ref, img_sent, sem, partner).wait_recv()

    barrier = pltpu.get_barrier_semaphore()
    others = [u * G + mod(g + k, G) for k in range(1, G)]
    others += [mod(u + k, U) * G + g for k in range(1, U)]
    for to in others:
        pl.semaphore_signal(
            barrier, inc=1, device_id=to, device_id_type=pl.DeviceIdType.LOGICAL
        )

    def group(di, dv):
        return group_at(V, H, di, dv)

    offsets = sorted((group(di, dv), di, dv) for di in range(H) for dv in range(V))

    def image_member(di, dv, k):
        return member(half * H + mod(h + di, H), mod(v + dv, V), c if k == 0 else 1 - c, r)

    load_val = pltpu.make_async_copy(val_ref, raw.at[0], loc_sem.at[0])
    load_pos = pltpu.make_async_copy(pos_ref, raw.at[1], loc_sem.at[1])
    load_img = pltpu.make_async_copy(img_ref, imgs.at[0], loc_sem.at[2])
    load_cap = pltpu.make_async_copy(cap_ref, mine, loc_sem.at[3])
    keep_cap = pltpu.make_async_copy(cap_ref, caps.at[0], loc_sem.at[4])
    load_img.start()
    load_val.start()
    load_pos.start()
    load_cap.start()

    @pl.when(keeps_own)
    def _():
        keep_cap.start()

    load_val.wait()
    load_pos.wait()
    words[g * U + u] = raw[1] * 2 + raw[0]
    load_img.wait()

    pl.semaphore_wait(barrier, len(others))

    def image_rows(k):
        return pl.ds(k * (n // IMAGE_PIECES), n // IMAGE_PIECES)

    def caption_rows(k):
        return pl.ds(k * (n // CAPTION_PIECES), n // CAPTION_PIECES)

    def img_copy(at, to_at, k, sem, to):
        rows = image_rows(k)
        return remote(imgs.at[at, rows], imgs.at[to_at, rows], img_sent, img_recv.at[sem], to)

    def across_sem(di, dv, k):
        return along_sems + (di * (V - 1) + dv - 1) * IMAGE_PIECES + k

    def img_along(d, k):
        to = member(half * H + mod(h + d, H), v, c, r)
        return img_copy(0, group(H - d, 0) * 2, k, (H - d - 1) * IMAGE_PIECES + k, to)

    def img_across(di, d, k):
        to = member(u, mod(v + d, V), c, r)
        return img_copy(
            group(di, 0) * 2, group(di, V - d) * 2, k, across_sem(di, V - d, k), to
        )

    def img_beside(di, dv, k):
        at = group(di, dv)
        return img_copy(at * 2, at * 2 + 1, k, along_sems + across_sems + at, partner)

    def along_came(di, k):
        came(imgs.at[group(di, 0) * 2, image_rows(k)], img_recv.at[(di - 1) * IMAGE_PIECES + k])

    def across_came(di, dv, k):
        came(imgs.at[group(di, dv) * 2, image_rows(k)], img_recv.at[across_sem(di, dv, k)])

    def beside_came(at):
        came(imgs.at[at * 2 + 1], img_recv.at[along_sems + across_sems + at])

    def cap_along(t, k):
        rows = caption_rows(k)
        to = t * H + div(u, 2)
        away = jnp.where(mod(u, 2) == near_of(to), 0, 1)
        return remote(
            mine.at[rows], caps.at[away * rep, rows], cap_sent,
            cap_recv.at[away * CAPTION_PIECES + k], member(to, v, c, r),
        )

    def cap_across(away, d, k, block=None):
        rows = caption_rows(k)
        seat = rep - d
        sem = 2 * CAPTION_PIECES + seat - 1
        if away:
            piece = k // (CAPTION_PIECES // LAST_PIECES)
            sem = 2 * CAPTION_PIECES + rep - 1 + (seat - 1) * LAST_PIECES + piece
        return remote(
            (caps.at[away * rep] if block is None else block).at[rows],
            caps.at[away * rep + seat, rows], cap_sent,
            cap_recv.at[sem], member(u, v, c, mod(r + d, rep)),
        )

    def relay_captions(away, k):
        came(caps.at[away * rep, caption_rows(k)], cap_recv.at[away * CAPTION_PIECES + k])
        for d in range(1, rep):
            cap_across(away, d, k).start()

    def line_copy(k):
        row = words.at[g * U + u]
        return remote(row, row, line_sent, line_came, mod(u + k, U) * G + g)

    def plane_copy(k):
        rows = words.at[pl.ds(g * U, U)]
        return remote(rows, rows, plane_sent, plane_came, u * G + mod(g + k, G))

    def own_across(k):
        for d in range(1, V):
            img_across(0, d, k).start()

    def own_captions_across(k):
        @pl.when(keeps_own)
        def _():
            for d in range(1, rep):
                cap_across(0, d, k, mine).start()

    for k in range(1, U):
        line_copy(k).start()
    for k in range(IMAGE_PIECES):
        for d in range(1, H):
            img_along(d, k).start()
        if k < IMAGE_PIECES - IMAGES_HELD:
            own_across(k)
        img_beside(0, 0, k).start()
    load_cap.wait()
    for k in range(CAPTION_PIECES):
        for t in range(2):
            @pl.when(t * H + div(u, 2) != u)
            def _():
                cap_along(t, k).start()
        if k < CAPTION_PIECES - CAPTIONS_HELD:
            own_captions_across(k)

    for at, di, dv in offsets:
        for k in range(2):
            cols = slice((at * 2 + k) * n, (at * 2 + k + 1) * n)
            first = image_member(di, dv, k) * n
            image_ids[:, cols] = first + lax.broadcasted_iota(jnp.int32, (1, n), 1)
    col_peak[...] = jnp.full(col_peak.shape, floor, jnp.float32)
    col_total[...] = jnp.zeros(col_total.shape, jnp.float32)
    col_match[...] = jnp.zeros(col_match.shape, jnp.float32)
    row_peak[...] = jnp.full(row_peak.shape, floor, jnp.float32)
    row_total[...] = jnp.zeros(row_total.shape, jnp.float32)
    row_match[...] = jnp.zeros(row_match.shape, jnp.float32)

    came(words.at[pl.ds(0, U - 1)], line_came)
    for k in range(1, G):
        plane_copy(k).start()
    for k in range(IMAGE_PIECES - IMAGES_HELD, IMAGE_PIECES):
        own_across(k)
    for k in range(CAPTION_PIECES - CAPTIONS_HELD, CAPTION_PIECES):
        own_captions_across(k)

    def relay_along(k):
        for di in range(1, H):
            along_came(di, k)
            for d in range(1, V):
                img_across(di, d, k).start()
            img_beside(di, 0, k).start()

    def relay_own(k):
        for dv in range(1, V):
            across_came(0, dv, k)
            img_beside(0, dv, k).start()

    def relay_late(k):
        for di in range(1, H):
            for dv in range(1, V):
                across_came(di, dv, k)
                img_beside(di, dv, k).start()

    def relay_near(k):
        @pl.when(jnp.logical_not(keeps_own))
        def _():
            relay_captions(0, k)

    relay_far = functools.partial(relay_captions, 1)
    relays = [((k + 1) / IMAGE_PIECES, 0, relay_along, k) for k in range(IMAGE_PIECES)]
    relays += [((k + 1) / IMAGE_PIECES + 0.12, 1, relay_own, k) for k in range(IMAGE_PIECES)]
    relays += [((k + 1) / CAPTION_PIECES, 2, relay_near, k) for k in range(CAPTION_PIECES)]
    relays += [(1.02 + k / CAPTION_PIECES, 3, relay_far, k) for k in range(FAR_FIRST)]
    for _, _, relay, k in sorted(relays, key=lambda x: x[:2]):
        relay(k)

    came(words.at[pl.ds(0, (G - 1) * U)], plane_came)

    eye = lax.broadcasted_iota(jnp.int32, (n, n), 0) == lax.broadcasted_iota(jnp.int32, (n, n), 1)

    def to_column(row):
        return jnp.sum(jnp.where(eye, row, 0.0), axis=1, keepdims=True)

    def to_row(column):
        return jnp.sum(jnp.where(eye, column, 0.0), axis=0, keepdims=True)

    flags = (words[:, 0, :] & 1).astype(jnp.float32)
    image_total = jnp.sum(jnp.sum(flags, axis=1, keepdims=True), axis=0, keepdims=True)

    def seat_row(s):
        away, d = div(s, rep), mod(s, rep)
        uu = 2 * h + jnp.where(away == 0, near, 1 - near)
        return ((v * 2 + c) * rep + mod(r + d, rep)) * U + uu

    aims = [words[seat_row(s)] >> 1 for s in range(2 * rep)]
    aim = jnp.concatenate(aims, axis=1)
    order = lax.broadcasted_iota(jnp.int32, (N, aim.shape[1]), 0)
    starts = (mod(order, U) * G + div(order, U)) * n
    inside = (aim >= starts) & (aim < starts + n)
    picked = jnp.dot(
        flags.T.astype(jnp.bfloat16), jnp.where(inside, 1.0, 0.0).astype(jnp.bfloat16),
        preferred_element_type=jnp.float32,
    )
    start = jnp.sum(jnp.where(inside, starts, 0).astype(jnp.float32), axis=0, keepdims=True)
    low = aim - start.astype(jnp.int32)
    depth = lax.broadcasted_iota(jnp.int32, picked.shape, 0)
    ok = jnp.sum(jnp.where(depth == low, picked, 0.0), axis=0, keepdims=True)
    for s in range(2 * rep):
        ok_row = ok[:, s * n : (s + 1) * n]
        caption_ok[s] = ok_row
        bias = to_column(jnp.where(ok_row > 0, 0.0, very_low))
        caption_bias[s] = jnp.broadcast_to(bias, (n, LANES))
        aim_column = to_column(aims[s].astype(jnp.float32)).astype(jnp.int32)
        target[s] = jnp.broadcast_to(aim_column, (n, LANES))
    for at, di, dv in offsets:
        for k in range(2):
            to = image_member(di, dv, k)
            flag = words[mod(to, G) * U + div(to, G)] & 1
            cols = slice((at * 2 + k) * n, (at * 2 + k + 1) * n)
            image_bias[:, cols] = jnp.where(flag > 0, 0.0, very_low)

    def fold(x, op):
        y = x[:, :LANES]
        for j in range(1, x.shape[1] // LANES):
            y = op(y, x[:, j * LANES : (j + 1) * LANES])
        return y

    def tally(s, cols, scores, first, rows):
        scaled = scores * log2_e + image_bias[:, cols]
        ids = image_ids[:, cols]
        old_peak = col_peak[:, cols]
        peak, match = old_peak, col_match[:, cols]
        wide = lambda x: jnp.concatenate([x] * (scores.shape[1] // LANES), axis=1)
        held, peaks = [], []
        for q in range(rows // SUBLANES):
            at = pl.ds(first + q * SUBLANES, SUBLANES)
            x = scaled[q * SUBLANES : (q + 1) * SUBLANES] + wide(caption_bias[s, at])
            held.append(x)
            peaks.append(jnp.maximum(fold(x, jnp.maximum), row_peak[s, at]))
            peak = jnp.maximum(peak, x)
            picked = jnp.where(wide(target[s, at]) == ids, x, 0.0)
            row_match[s, at] = row_match[s, at] + fold(picked, jnp.add)
            match = match + picked
        total = col_total[:, cols] * jnp.exp2(old_peak - peak)
        for q in range(rows // SUBLANES):
            at = pl.ds(first + q * SUBLANES, SUBLANES)
            powers = jnp.exp2(held[q] - wide(peaks[q]))
            row_total[s, at] = row_total[s, at] * jnp.exp2(row_peak[s, at] - peaks[q]) + fold(
                powers, jnp.add
            )
            row_peak[s, at] = peaks[q]
            total = total + jnp.exp2(held[q] - peak)
        col_peak[:, cols] = peak
        col_total[:, cols] = total
        col_match[:, cols] = match

    def score(s, count, start, stop, first, rows):
        left = caps[pl.ds(s, count), pl.ds(first, rows)].reshape(count * rows, width)
        for at in range(start, stop):
            scores = lax.dot_general(
                left, imgs[2 * at : 2 * at + 2].reshape(2 * n, width), (((1,), (1,)), ((), ())),
                preferred_element_type=jnp.float32,
            )
            cols = slice(2 * at * n, 2 * (at + 1) * n)
            for k in range(count):
                tally(s + k, cols, scores[k * rows : (k + 1) * rows], first, rows)

    @pl.when(keeps_own)
    def _():
        keep_cap.wait()

    for at in range(early):
        beside_came(at)

    @pl.loop(0, rep + 1)
    def _(e):
        for step in range(rep + 1):
            @pl.when(e == step)
            def _():
                for k in range(FAR_FIRST, CAPTION_PIECES):
                    if step == min(k - FAR_FIRST, rep):
                        relay_far(k)
                        late = k - FAR_FIRST - 1
                        if 0 <= late < IMAGE_PIECES - LATE_LAST:
                            relay_late(late)

        @pl.when((e > 0) & (e < rep))
        def _():
            came(caps.at[0], cap_recv.at[2 * CAPTION_PIECES + e - 1])
        score(e, 1, 0, early, 0, n)

    for k in range(min(CAPTION_PIECES - FAR_FIRST - 1, IMAGE_PIECES - LATE_LAST), IMAGE_PIECES):
        relay_late(k)

    def last_came(d, k):
        came(
            caps.at[rep + d, pl.ds(0, n // LAST_PIECES)],
            cap_recv.at[2 * CAPTION_PIECES + rep - 1 + (d - 1) * LAST_PIECES + k],
        )

    def last_early(k):
        @pl.loop(1, rep)
        def _(d):
            last_came(d, k)
            score(rep + d, 1, 0, early, k * (n // LAST_PIECES), n // LAST_PIECES)

    @pl.loop(0, LAST_PIECES - 1)
    def _(k):
        last_early(k)

    for at in range(early, H * V):
        beside_came(at)
    score(0, rep + 1, early, H * V, 0, n)

    stride = pl.cdiv(n, LANES) * LANES

    def pack(ref, at, ok, first, peak, total, match):
        ref[at, :, 0:n] = jnp.where(ok, peak, 0.0)
        ref[at, :, stride : stride + n] = jnp.where(ok, total, jnp.where(first, 1.0, 0.0))
        ref[at, :, 2 * stride : 2 * stride + n] = jnp.where(ok, match, 0.0)

    def send_rows(s):
        away, d = div(s, rep), mod(s, rep)
        uu = 2 * h + jnp.where(away == 0, near, 1 - near)
        rr = mod(r + d, rep)
        at = half * rep + r
        peak = jnp.max(row_peak[s], axis=1, keepdims=True)
        total = jnp.sum(row_total[s] * jnp.exp2(row_peak[s] - peak), axis=1, keepdims=True)
        match = jnp.sum(row_match[s], axis=1, keepdims=True)
        pack(rowsend, s, caption_ok[s] > 0, at == 0, to_row(peak), to_row(total), to_row(match))
        remote(
            rowsend.at[s], rowpool.at[(mod(uu, H) * 2 + c) * 2 * rep + at], row_given, row_pooled,
            pool_of(uu, v, rr),
        ).start()
        stays = keeps_own & (s == 0)

        @pl.when(jnp.logical_not(stays))
        def _():
            remote(
                rowsend.at[s], rowrecv.at[at], row_sent, row_came, member(uu, v, c, rr)
            ).start()

        @pl.when(stays)
        def _():
            rowrecv[at] = rowsend[s]

    for s in range(rep + 1):
        send_rows(s)

    last_early(LAST_PIECES - 1)

    @pl.loop(1, rep)
    def _(d):
        score(rep + d, 1, early, H * V, 0, n)
        send_rows(rep + d)

    peak = jnp.max(col_peak[...], axis=0, keepdims=True)
    total = jnp.sum(col_total[...] * jnp.exp2(col_peak[...] - peak), axis=0, keepdims=True)
    match = jnp.sum(col_match[...], axis=0, keepdims=True)
    for at, di, dv in offsets:
        for k in range(2):
            slot = at * 2 + k
            cols = slice(slot * n, (slot + 1) * n)
            back = group((H - di) % H, (V - dv) % V) * 2 + k
            pack(
                colsend, slot, image_bias[:, cols] == 0, back == 0, peak[:, cols], total[:, cols],
                match[:, cols],
            )
    for at, di, dv in reversed(offsets):
        for k in range(2):
            slot = at * 2 + k
            back = group((H - di) % H, (V - dv) % V) * 2 + k
            cc = c if k == 0 else 1 - c
            seat = (mod(h + di, H) * 2 + cc) * H * B + back

            def give():
                remote(
                    colsend.at[slot], colpool.at[seat], col_given, col_pooled,
                    pool_of(u, mod(v + dv, V), r),
                ).start()

            if dv:
                give()
            else:
                @pl.when(pools)
                def _():
                    colpool[seat] = colsend[slot]

                pl.when(jnp.logical_not(pools))(give)
    for at, di, dv in reversed(offsets):
        for k in range(2):
            slot = at * 2 + k
            if slot:
                back = group((H - di) % H, (V - dv) % V) * 2 + k
                remote(
                    colsend.at[slot], colrecv.at[back], col_sent, col_came,
                    image_member(di, dv, k),
                ).start()
    colrecv[0] = colsend[0]

    def joined(parts, first, count):
        piece = lambda s, k: parts[first + s, :, k * stride : k * stride + n]
        peak = piece(0, 0)
        for s in range(1, count):
            peak = jnp.maximum(peak, piece(s, 0))
        total = jnp.zeros_like(peak)
        match = jnp.zeros_like(peak)
        for s in range(count):
            total += piece(s, 1) * jnp.exp2(piece(s, 0) - peak)
            match += piece(s, 2)
        return (peak - match) * ln_2 + jnp.log(total)

    pool_count = 2 * V * rep
    own_pool = (half * V + v) * rep + r

    @pl.when(pools)
    def _():
        came(rowpool, row_pooled)
        whole = jnp.zeros((1, n), jnp.float32)
        for k in range(2 * H):
            whole += joined(rowpool, k * 2 * rep, 2 * rep)
        came(colpool.at[pl.ds(0, 2 * H * (H * B - 1))], col_pooled)
        for k in range(2 * H):
            whole += joined(colpool, k * H * B, H * B)
        part[own_pool] = jnp.broadcast_to(jnp.sum(whole, axis=1, keepdims=True), (1, LANES))

        @pl.loop(0, N)
        def _(k):
            uu = div(k, G)
            to = jnp.where(u < H, U - 1 - uu, uu) * G + mod(k, G)

            @pl.when(to != me)
            def _():
                remote(part.at[own_pool], part.at[own_pool], part_sent, part_came, to).start()

    @pl.when(keeps_own)
    def _():
        came(rowrecv.at[pl.ds(0, 2 * rep - 1)], row_came)

    @pl.when(jnp.logical_not(keeps_own))
    def _():
        came(rowrecv, row_came)

    terms_ref[0:1, :] = joined(rowrecv, 0, 2 * rep)
    came(colrecv.at[pl.ds(0, H * B - 1)], col_came)
    terms_ref[1:2, :] = joined(colrecv, 0, H * B)

    sent(words.at[pl.ds(0, U - 1)], line_sent)
    sent(words.at[pl.ds(0, (G - 1) * U)], plane_sent)
    sent(imgs.at[pl.ds(0, H * B - 1)], img_sent)

    @pl.when(keeps_own)
    def _():
        sent(caps.at[pl.ds(0, 2 * rep - 1)], cap_sent)
        sent(rowsend.at[pl.ds(0, 2 * rep - 1)], row_sent)

    @pl.when(jnp.logical_not(keeps_own))
    def _():
        sent(caps, cap_sent)
        sent(rowsend, row_sent)

    sent(rowsend, row_given)
    sent(colsend.at[pl.ds(0, H * B - 1)], col_sent)

    @pl.when(pools)
    def _():
        sent(colsend.at[pl.ds(0, H * B - 2 * H)], col_given)
        sent(spare.at[pl.ds(0, N - 1)], part_sent)
        came(part.at[pl.ds(0, pool_count - 1)], part_came)

    @pl.when(jnp.logical_not(pools))
    def _():
        sent(colsend, col_given)
        came(part, part_came)

    whole = jnp.sum(part[:, 0, :], axis=0, keepdims=True)
    terms_ref[2:3, 0:1] = whole[:, 0:1] / (2.0 * image_total)


def hand_out(terms_ref, closs_ref, iloss_ref, loss_ref):
    closs_ref[...] = terms_ref[0:1, :]
    iloss_ref[...] = terms_ref[1:2, :]
    loss_ref[...] = terms_ref[2:3, 0:1]


def local(blk, rep, captions, images, positives, valid):
    n, width = captions.shape
    U, V = grid_of(blk, rep)
    N = blk * rep
    H, B = U // 2, V * 2
    C = H * B * n
    packed = 3 * pl.cdiv(n, LANES) * LANES
    f32, i32 = jnp.float32, jnp.int32
    _, _, image_sems, caption_sems = semaphore_counts(U, V, rep)
    dma = lambda count: pltpu.SemaphoreType.DMA((count,))
    vmem = pl.BlockSpec(memory_space=pltpu.VMEM)
    hbm = pl.BlockSpec(memory_space=pl.ANY)
    terms = pl.pallas_call(
        functools.partial(kernel, blk, rep),
        out_shape=pltpu.VMEM((SUBLANES, n), f32),
        in_specs=[hbm] * 4,
        out_specs=vmem,
        scratch_shapes=[
            pltpu.VMEM((n, width), captions.dtype),
            pltpu.VMEM((2 * rep, n, width), captions.dtype),
            pltpu.VMEM((H * B, n, width), images.dtype),
            pltpu.VMEM((2, 1, n), i32),
            pltpu.VMEM((N, 1, n), i32),
            pltpu.VMEM((1, C), f32),
            pltpu.VMEM((1, C), i32),
            pltpu.VMEM((2 * rep, n, LANES), i32),
            pltpu.VMEM((2 * rep, n, LANES), f32),
            pltpu.VMEM((2 * rep, 1, n), f32),
            pltpu.VMEM((2 * rep, n, LANES), f32),
            pltpu.VMEM((2 * rep, n, LANES), f32),
            pltpu.VMEM((2 * rep, n, LANES), f32),
            pltpu.VMEM((SUBLANES, C), f32),
            pltpu.VMEM((SUBLANES, C), f32),
            pltpu.VMEM((SUBLANES, C), f32),
            pltpu.VMEM((2 * rep, 1, packed), f32),
            pltpu.VMEM((2 * rep, 1, packed), f32),
            pltpu.VMEM((2 * H * 2 * rep, 1, packed), f32),
            pltpu.VMEM((H * B, 1, packed), f32),
            pltpu.VMEM((H * B, 1, packed), f32),
            pltpu.VMEM((2 * H * H * B, 1, packed), f32),
            pltpu.VMEM((2 * V * rep, 1, LANES), f32),
            pltpu.VMEM((N, 1, LANES), f32),
            dma(5), dma(image_sems), dma(caption_sems), dma(9), dma(7),
        ],
        compiler_params=pltpu.CompilerParams(collective_id=0, has_side_effects=True),
    )(captions, images, positives.reshape(1, n), valid.reshape(1, n))
    caption_loss, image_loss, loss = pl.pallas_call(
        hand_out,
        out_shape=(
            jax.ShapeDtypeStruct((1, n), f32),
            jax.ShapeDtypeStruct((1, n), f32),
            jax.ShapeDtypeStruct((1, 1), f32),
        ),
        in_specs=[vmem],
        out_specs=(vmem,) * 3,
    )(pltpu.with_memory_space_constraint(terms, pltpu.VMEM))
    return caption_loss.reshape(n), image_loss.reshape(n), loss.reshape(())


def solution(mesh):
    placed = (
        P(("blk", "rep"), None),
        P(("blk", "rep"), None),
        P(("blk", "rep")),
        P(("blk", "rep")),
    )
    return jax.shard_map(
        functools.partial(local, mesh.shape["blk"], mesh.shape["rep"]),
        mesh=mesh,
        in_specs=placed,
        out_specs=(P(("blk", "rep")), P(("blk", "rep")), P()),
        check_vma=False,
    )
```

```python
import functools
import math

import jax
import jax.numpy as jnp
from jax import lax
from jax.experimental import pallas as pl
from jax.experimental.pallas import tpu as pltpu
from jax.sharding import PartitionSpec as P

very_low = -1e30
floor = -1e29
IMAGE_PIECES = 4
CAPTION_PIECES = 6
IMAGES_HELD = 1
CAPTIONS_HELD = 2
FAR_FIRST = 2
LANES = 128
SUBLANES = 8
log2_e = math.log2(math.e)
ln_2 = math.log(2)


def grid_of(blk, rep):
    chips = (blk // 2) * rep
    planes = 1
    while (planes * 2) ** 2 <= chips and (blk // 2) % (planes * 2) == 0:
        planes *= 2
    return planes, blk // 2 // planes


def mod(a, b):
    return a & (b - 1) if b & (b - 1) == 0 else lax.rem(a, b)


def div(a, b):
    return a >> (b.bit_length() - 1) if b & (b - 1) == 0 else lax.div(a, b)


def semaphore_counts(U, V, rep):
    H = U // 2
    along = (H - 1) * IMAGE_PIECES
    across = H * (V - 1) * IMAGE_PIECES
    return along, across, along + across + H * V, 2 * CAPTION_PIECES + 2 * (rep - 1)


def group_at(V, H, di, dv):
    if di == 0:
        return dv
    if dv == 0:
        return V + di - 1
    return V + H - 1 + (di - 1) * (V - 1) + dv - 1


def kernel(
    blk, rep, cap_ref, img_ref, pos_ref, val_ref, terms_ref,
    mine, caps, imgs, raw, words, image_bias, image_ids, target, caption_bias, caption_ok,
    row_peak, row_total, row_match, col_peak, col_total, col_match,
    rowsend, rowrecv, rowpool, colsend, colrecv, colpool, part, spare,
    loc_sem, img_recv, cap_recv, send_sem, recv_sem,
):
    U, V = grid_of(blk, rep)
    N = blk * rep
    G = N // U
    H = U // 2
    B = V * 2
    n, width = cap_ref.shape
    early = V + H - 1
    C = H * B * n
    along_sems, across_sems, _, _ = semaphore_counts(U, V, rep)
    b, r = lax.axis_index("blk"), lax.axis_index("rep")
    c = mod(b, 2)
    u = div(b, 2 * V)
    v = mod(div(b, 2), V)
    me = b * rep + r
    g = mod(me, G)
    half, h = div(u, H), mod(u, H)
    keeps_own = div(u, 2) == h
    img_sent, cap_sent, line_sent, plane_sent, row_sent, col_sent, row_given, col_given, part_sent = (
        send_sem.at[k] for k in range(9)
    )
    line_came, plane_came, row_came, col_came, row_pooled, col_pooled, part_came = (
        recv_sem.at[k] for k in range(7)
    )
    pools = (c == 1) & ((u == H - 1) | (u == H))

    def pool_of(uu, vv, rr):
        return member(H - 1 + div(uu, H), vv, 1, rr)

    def near_of(uu):
        return jnp.where(uu > 2 * mod(uu, H), 1, 0)

    near = near_of(u)

    def member(uu, vv, cc, rr):
        return ((uu * V + vv) * 2 + cc) * rep + rr

    def remote(src, dst, ss, rs, to):
        return pltpu.make_async_remote_copy(
            src_ref=src, dst_ref=dst, send_sem=ss, recv_sem=rs, device_id=to,
            device_id_type=pl.DeviceIdType.LOGICAL,
        )

    partner = member(u, v, 1 - c, r)

    def sent(ref, sem):
        remote(ref, ref, sem, img_recv.at[0], partner).wait_send()

    def came(ref, sem):
        remote(ref, ref, img_sent, sem, partner).wait_recv()

    barrier = pltpu.get_barrier_semaphore()
    others = [u * G + mod(g + k, G) for k in range(1, G)]
    others += [mod(u + k, U) * G + g for k in range(1, U)]
    for to in others:
        pl.semaphore_signal(
            barrier, inc=1, device_id=to, device_id_type=pl.DeviceIdType.LOGICAL
        )

    def group(di, dv):
        return group_at(V, H, di, dv)

    offsets = sorted((group(di, dv), di, dv) for di in range(H) for dv in range(V))

    def image_member(di, dv, k):
        return member(half * H + mod(h + di, H), mod(v + dv, V), c if k == 0 else 1 - c, r)

    load_val = pltpu.make_async_copy(val_ref, raw.at[0], loc_sem.at[0])
    load_pos = pltpu.make_async_copy(pos_ref, raw.at[1], loc_sem.at[1])
    load_img = pltpu.make_async_copy(img_ref, imgs.at[0], loc_sem.at[2])
    load_cap = pltpu.make_async_copy(cap_ref, mine, loc_sem.at[3])
    keep_cap = pltpu.make_async_copy(cap_ref, caps.at[0], loc_sem.at[4])
    load_img.start()
    load_val.start()
    load_pos.start()
    load_cap.start()

    @pl.when(keeps_own)
    def _():
        keep_cap.start()

    load_val.wait()
    load_pos.wait()
    words[g * U + u] = raw[1] * 2 + raw[0]
    load_img.wait()

    pl.semaphore_wait(barrier, len(others))

    def image_rows(k):
        return pl.ds(k * (n // IMAGE_PIECES), n // IMAGE_PIECES)

    def caption_rows(k):
        return pl.ds(k * (n // CAPTION_PIECES), n // CAPTION_PIECES)

    def img_copy(at, to_at, k, sem, to):
        rows = image_rows(k)
        return remote(imgs.at[at, rows], imgs.at[to_at, rows], img_sent, img_recv.at[sem], to)

    def across_sem(di, dv, k):
        return along_sems + (di * (V - 1) + dv - 1) * IMAGE_PIECES + k

    def img_along(d, k):
        to = member(half * H + mod(h + d, H), v, c, r)
        return img_copy(0, group(H - d, 0) * 2, k, (H - d - 1) * IMAGE_PIECES + k, to)

    def img_across(di, d, k):
        to = member(u, mod(v + d, V), c, r)
        return img_copy(
            group(di, 0) * 2, group(di, V - d) * 2, k, across_sem(di, V - d, k), to
        )

    def img_beside(di, dv, k):
        at = group(di, dv)
        return img_copy(at * 2, at * 2 + 1, k, along_sems + across_sems + at, partner)

    def along_came(di, k):
        came(imgs.at[group(di, 0) * 2, image_rows(k)], img_recv.at[(di - 1) * IMAGE_PIECES + k])

    def across_came(di, dv, k):
        came(imgs.at[group(di, dv) * 2, image_rows(k)], img_recv.at[across_sem(di, dv, k)])

    def beside_came(at):
        came(imgs.at[at * 2 + 1], img_recv.at[along_sems + across_sems + at])

    def cap_along(t, k):
        rows = caption_rows(k)
        to = t * H + div(u, 2)
        away = jnp.where(mod(u, 2) == near_of(to), 0, 1)
        return remote(
            mine.at[rows], caps.at[away * rep, rows], cap_sent,
            cap_recv.at[away * CAPTION_PIECES + k], member(to, v, c, r),
        )

    def cap_across(away, d, k, block=None):
        rows = caption_rows(k)
        seat = rep - d
        sem = 2 * CAPTION_PIECES + away * (rep - 1) + seat - 1
        return remote(
            (caps.at[away * rep] if block is None else block).at[rows],
            caps.at[away * rep + seat, rows], cap_sent,
            cap_recv.at[sem], member(u, v, c, mod(r + d, rep)),
        )

    def relay_captions(away, k):
        came(caps.at[away * rep, caption_rows(k)], cap_recv.at[away * CAPTION_PIECES + k])
        for d in range(1, rep):
            cap_across(away, d, k).start()

    def line_copy(k):
        row = words.at[g * U + u]
        return remote(row, row, line_sent, line_came, mod(u + k, U) * G + g)

    def plane_copy(k):
        rows = words.at[pl.ds(g * U, U)]
        return remote(rows, rows, plane_sent, plane_came, u * G + mod(g + k, G))

    def own_across(k):
        for d in range(1, V):
            img_across(0, d, k).start()

    def own_captions_across(k):
        @pl.when(keeps_own)
        def _():
            for d in range(1, rep):
                cap_across(0, d, k, mine).start()

    for k in range(1, U):
        line_copy(k).start()
    for k in range(IMAGE_PIECES):
        for d in range(1, H):
            img_along(d, k).start()
        if k < IMAGE_PIECES - IMAGES_HELD:
            own_across(k)
        img_beside(0, 0, k).start()
    load_cap.wait()
    for k in range(CAPTION_PIECES):
        for t in range(2):
            @pl.when(t * H + div(u, 2) != u)
            def _():
                cap_along(t, k).start()
        if k < CAPTION_PIECES - CAPTIONS_HELD:
            own_captions_across(k)

    for at, di, dv in offsets:
        for k in range(2):
            cols = slice((at * 2 + k) * n, (at * 2 + k + 1) * n)
            first = image_member(di, dv, k) * n
            image_ids[:, cols] = first + lax.broadcasted_iota(jnp.int32, (1, n), 1)
    col_peak[...] = jnp.full(col_peak.shape, floor, jnp.float32)
    col_total[...] = jnp.zeros(col_total.shape, jnp.float32)
    col_match[...] = jnp.zeros(col_match.shape, jnp.float32)
    row_peak[...] = jnp.full(row_peak.shape, floor, jnp.float32)
    row_total[...] = jnp.zeros(row_total.shape, jnp.float32)
    row_match[...] = jnp.zeros(row_match.shape, jnp.float32)

    came(words.at[pl.ds(0, U - 1)], line_came)
    for k in range(1, G):
        plane_copy(k).start()
    for k in range(IMAGE_PIECES - IMAGES_HELD, IMAGE_PIECES):
        own_across(k)
    for k in range(CAPTION_PIECES - CAPTIONS_HELD, CAPTION_PIECES):
        own_captions_across(k)

    def relay_along(k):
        for di in range(1, H):
            along_came(di, k)
            for d in range(1, V):
                img_across(di, d, k).start()
            img_beside(di, 0, k).start()

    def relay_own(k):
        for dv in range(1, V):
            across_came(0, dv, k)
            img_beside(0, dv, k).start()

    def relay_late(k):
        for di in range(1, H):
            for dv in range(1, V):
                across_came(di, dv, k)
                img_beside(di, dv, k).start()

    def late_pieces(first, stop):
        for k in range(min(first, IMAGE_PIECES), min(stop, IMAGE_PIECES)):
            relay_late(k)

    def far_pieces(first, to_end):
        for k in range(first, CAPTION_PIECES if to_end else min(first + 1, CAPTION_PIECES)):
            relay_far(k)

    def relay_near(k):
        @pl.when(jnp.logical_not(keeps_own))
        def _():
            relay_captions(0, k)

    def relay_far(k):
        relay_captions(1, k)

    def relay_far_early(k):
        pl.when(keeps_own)(functools.partial(relay_far, k))

    relays = [((k + 1) / IMAGE_PIECES, 0, relay_along, k) for k in range(IMAGE_PIECES)]
    relays += [((k + 1) / IMAGE_PIECES + 0.12, 1, relay_own, k) for k in range(IMAGE_PIECES)]
    relays += [((k + 1) / CAPTION_PIECES, 2, relay_near, k) for k in range(CAPTION_PIECES)]
    relays += [(1.02 + k / CAPTION_PIECES, 3, relay_far_early, k) for k in range(FAR_FIRST)]
    for _, _, relay, k in sorted(relays, key=lambda x: x[:2]):
        relay(k)

    came(words.at[pl.ds(0, (G - 1) * U)], plane_came)

    eye = lax.broadcasted_iota(jnp.int32, (n, n), 0) == lax.broadcasted_iota(jnp.int32, (n, n), 1)

    def to_column(row):
        return jnp.sum(jnp.where(eye, row, 0.0), axis=1, keepdims=True)

    def to_row(column):
        return jnp.sum(jnp.where(eye, column, 0.0), axis=0, keepdims=True)

    flags = (words[:, 0, :] & 1).astype(jnp.float32)
    image_total = jnp.sum(jnp.sum(flags, axis=1, keepdims=True), axis=0, keepdims=True)

    def seat_row(s):
        away, d = div(s, rep), mod(s, rep)
        uu = 2 * h + jnp.where(away == 0, near, 1 - near)
        return ((v * 2 + c) * rep + mod(r + d, rep)) * U + uu

    aims = [words[seat_row(s)] >> 1 for s in range(2 * rep)]
    aim = jnp.concatenate(aims, axis=1)
    order = lax.broadcasted_iota(jnp.int32, (N, aim.shape[1]), 0)
    starts = (mod(order, U) * G + div(order, U)) * n
    inside = (aim >= starts) & (aim < starts + n)
    picked = jnp.dot(
        flags.T.astype(jnp.bfloat16), jnp.where(inside, 1.0, 0.0).astype(jnp.bfloat16),
        preferred_element_type=jnp.float32,
    )
    start = jnp.sum(jnp.where(inside, starts, 0).astype(jnp.float32), axis=0, keepdims=True)
    low = aim - start.astype(jnp.int32)
    depth = lax.broadcasted_iota(jnp.int32, picked.shape, 0)
    ok = jnp.sum(jnp.where(depth == low, picked, 0.0), axis=0, keepdims=True)
    for s in range(2 * rep):
        ok_row = ok[:, s * n : (s + 1) * n]
        caption_ok[s] = ok_row
        bias = to_column(jnp.where(ok_row > 0, 0.0, very_low))
        caption_bias[s] = jnp.broadcast_to(bias, (n, LANES))
        aim_column = to_column(aims[s].astype(jnp.float32)).astype(jnp.int32)
        target[s] = jnp.broadcast_to(aim_column, (n, LANES))
    for at, di, dv in offsets:
        for k in range(2):
            to = image_member(di, dv, k)
            flag = words[mod(to, G) * U + div(to, G)] & 1
            cols = slice((at * 2 + k) * n, (at * 2 + k + 1) * n)
            image_bias[:, cols] = jnp.where(flag > 0, 0.0, very_low)

    def fold(x, op):
        y = x[:, :LANES]
        for j in range(1, x.shape[1] // LANES):
            y = op(y, x[:, j * LANES : (j + 1) * LANES])
        return y

    def tally(s, cols, scores, first, rows):
        scaled = scores * log2_e + image_bias[:, cols]
        ids = image_ids[:, cols]
        old_peak = col_peak[:, cols]
        peak, match = old_peak, col_match[:, cols]
        wide = lambda x: jnp.concatenate([x] * (scores.shape[1] // LANES), axis=1)
        held, peaks = [], []
        for q in range(rows // SUBLANES):
            at = pl.ds(first + q * SUBLANES, SUBLANES)
            x = scaled[q * SUBLANES : (q + 1) * SUBLANES] + wide(caption_bias[s, at])
            held.append(x)
            peaks.append(jnp.maximum(fold(x, jnp.maximum), row_peak[s, at]))
            peak = jnp.maximum(peak, x)
            picked = jnp.where(wide(target[s, at]) == ids, x, 0.0)
            row_match[s, at] = row_match[s, at] + fold(picked, jnp.add)
            match = match + picked
        total = col_total[:, cols] * jnp.exp2(old_peak - peak)
        for q in range(rows // SUBLANES):
            at = pl.ds(first + q * SUBLANES, SUBLANES)
            powers = jnp.exp2(held[q] - wide(peaks[q]))
            row_total[s, at] = row_total[s, at] * jnp.exp2(row_peak[s, at] - peaks[q]) + fold(
                powers, jnp.add
            )
            row_peak[s, at] = peaks[q]
            total = total + jnp.exp2(held[q] - peak)
        col_peak[:, cols] = peak
        col_total[:, cols] = total
        col_match[:, cols] = match

    def score(s, count, start, stop, first, rows):
        left = caps[pl.ds(s, count), pl.ds(first, rows)].reshape(count * rows, width)
        for at in range(start, stop):
            scores = lax.dot_general(
                left, imgs[2 * at : 2 * at + 2].reshape(2 * n, width), (((1,), (1,)), ((), ())),
                preferred_element_type=jnp.float32,
            )
            cols = slice(2 * at * n, 2 * (at + 1) * n)
            for k in range(count):
                tally(s + k, cols, scores[k * rows : (k + 1) * rows], first, rows)

    @pl.when(keeps_own)
    def _():
        keep_cap.wait()

    @pl.when(keeps_own)
    def _():
        far_pieces(FAR_FIRST, False)

    @pl.when(jnp.logical_not(keeps_own))
    def _():
        far_pieces(0, False)

    for at in range(early):
        beside_came(at)

    @pl.loop(0, rep + 1)
    def _(e):
        for step in range(rep + 1):
            @pl.when(e == step)
            def _():
                @pl.when(keeps_own)
                def _():
                    if step:
                        late_pieces(step - 1, step)
                    far_pieces(FAR_FIRST + 1 + step, step == rep)
                    if step == rep:
                        late_pieces(step, IMAGE_PIECES)

                @pl.when(jnp.logical_not(keeps_own))
                def _():
                    far_pieces(1 + step, False)
                    if step == rep:
                        late_pieces(0, IMAGE_PIECES // 2)
                        far_pieces(2 + step, False)
                        late_pieces(IMAGE_PIECES // 2, IMAGE_PIECES)
                        far_pieces(3 + step, True)

        @pl.when((e > 0) & (e < rep))
        def _():
            came(caps.at[0], cap_recv.at[2 * CAPTION_PIECES + e - 1])
        score(e, 1, 0, early, 0, n)

    for at in range(early, H * V):
        beside_came(at)
    score(0, rep + 1, early, H * V, 0, n)

    stride = pl.cdiv(n, LANES) * LANES

    def pack(ref, at, ok, first, peak, total, match):
        ref[at, :, 0:n] = jnp.where(ok, peak, 0.0)
        ref[at, :, stride : stride + n] = jnp.where(ok, total, jnp.where(first, 1.0, 0.0))
        ref[at, :, 2 * stride : 2 * stride + n] = jnp.where(ok, match, 0.0)

    def pack_rows(s):
        peak = jnp.max(row_peak[s], axis=1, keepdims=True)
        total = jnp.sum(row_total[s] * jnp.exp2(row_peak[s] - peak), axis=1, keepdims=True)
        match = jnp.sum(row_match[s], axis=1, keepdims=True)
        pack(
            rowsend, s, caption_ok[s] > 0, half * rep + r == 0, to_row(peak), to_row(total),
            to_row(match),
        )

    def row_place(s):
        away, d = s // rep, s % rep
        uu = 2 * h + (near if away == 0 else 1 - near)
        return uu, mod(r + d, rep)

    def pool_rows(s):
        uu, rr = row_place(s)
        at = (mod(uu, H) * 2 + c) * 2 * rep + half * rep + r
        remote(rowsend.at[s], rowpool.at[at], row_given, row_pooled, pool_of(uu, v, rr)).start()

    def send_rows(s):
        uu, rr = row_place(s)
        at = half * rep + r

        def go():
            remote(
                rowsend.at[s], rowrecv.at[at], row_sent, row_came, member(uu, v, c, rr)
            ).start()

        if s:
            go()
        else:
            pl.when(jnp.logical_not(keeps_own))(go)

            @pl.when(keeps_own)
            def _():
                rowrecv[at] = rowsend[s]

    for s in range(rep + 1):
        pack_rows(s)
    for s in range(rep + 1):
        pool_rows(s)
        send_rows(s)

    @pl.loop(1, rep)
    def _(d):
        came(caps.at[rep + d], cap_recv.at[2 * CAPTION_PIECES + rep - 1 + d - 1])
        score(rep + d, 1, 0, H * V, 0, n)

    for s in range(rep + 1, 2 * rep):
        pack_rows(s)
    peak = jnp.max(col_peak[...], axis=0, keepdims=True)
    total = jnp.sum(col_total[...] * jnp.exp2(col_peak[...] - peak), axis=0, keepdims=True)
    match = jnp.sum(col_match[...], axis=0, keepdims=True)
    for at, di, dv in offsets:
        for k in range(2):
            slot = at * 2 + k
            cols = slice(slot * n, (slot + 1) * n)
            back = group((H - di) % H, (V - dv) % V) * 2 + k
            pack(
                colsend, slot, image_bias[:, cols] == 0, back == 0, peak[:, cols], total[:, cols],
                match[:, cols],
            )
    for s in range(rep + 1, 2 * rep):
        pool_rows(s)
    for at, di, dv in reversed(offsets):
        for k in range(2):
            slot = at * 2 + k
            back = group((H - di) % H, (V - dv) % V) * 2 + k
            cc = c if k == 0 else 1 - c
            seat = (mod(h + di, H) * 2 + cc) * H * B + back

            def give():
                remote(
                    colsend.at[slot], colpool.at[seat], col_given, col_pooled,
                    pool_of(u, mod(v + dv, V), r),
                ).start()

            if dv:
                give()
            else:
                @pl.when(pools)
                def _():
                    colpool[seat] = colsend[slot]

                pl.when(jnp.logical_not(pools))(give)
    for s in range(rep + 1, 2 * rep):
        send_rows(s)
    for at, di, dv in reversed(offsets):
        for k in range(2):
            slot = at * 2 + k
            if slot:
                back = group((H - di) % H, (V - dv) % V) * 2 + k
                remote(
                    colsend.at[slot], colrecv.at[back], col_sent, col_came,
                    image_member(di, dv, k),
                ).start()
    colrecv[0] = colsend[0]

    def joined(parts, first, count):
        piece = lambda s, k: parts[first + s, :, k * stride : k * stride + n]
        peak = piece(0, 0)
        for s in range(1, count):
            peak = jnp.maximum(peak, piece(s, 0))
        total = jnp.zeros_like(peak)
        match = jnp.zeros_like(peak)
        for s in range(count):
            total += piece(s, 1) * jnp.exp2(piece(s, 0) - peak)
            match += piece(s, 2)
        return (peak - match) * ln_2 + jnp.log(total)

    pool_count = 2 * V * rep
    own_pool = (half * V + v) * rep + r

    @pl.when(pools)
    def _():
        came(rowpool, row_pooled)
        whole = jnp.zeros((1, n), jnp.float32)
        for k in range(2 * H):
            whole += joined(rowpool, k * 2 * rep, 2 * rep)
        came(colpool.at[pl.ds(0, 2 * H * (H * B - 1))], col_pooled)
        for k in range(2 * H):
            whole += joined(colpool, k * H * B, H * B)
        part[own_pool] = jnp.broadcast_to(jnp.sum(whole, axis=1, keepdims=True), (1, LANES))

        @pl.loop(0, N)
        def _(k):
            uu = div(k, G)
            to = jnp.where(u < H, U - 1 - uu, uu) * G + mod(k, G)

            @pl.when(to != me)
            def _():
                remote(part.at[own_pool], part.at[own_pool], part_sent, part_came, to).start()

    @pl.when(keeps_own)
    def _():
        came(rowrecv.at[pl.ds(0, 2 * rep - 1)], row_came)

    @pl.when(jnp.logical_not(keeps_own))
    def _():
        came(rowrecv, row_came)

    terms_ref[0:1, :] = joined(rowrecv, 0, 2 * rep)
    came(colrecv.at[pl.ds(0, H * B - 1)], col_came)
    terms_ref[1:2, :] = joined(colrecv, 0, H * B)

    sent(words.at[pl.ds(0, U - 1)], line_sent)
    sent(words.at[pl.ds(0, (G - 1) * U)], plane_sent)
    sent(imgs.at[pl.ds(0, H * B - 1)], img_sent)

    @pl.when(keeps_own)
    def _():
        sent(caps.at[pl.ds(0, 2 * rep - 1)], cap_sent)
        sent(rowsend.at[pl.ds(0, 2 * rep - 1)], row_sent)

    @pl.when(jnp.logical_not(keeps_own))
    def _():
        sent(caps, cap_sent)
        sent(rowsend, row_sent)

    sent(rowsend, row_given)
    sent(colsend.at[pl.ds(0, H * B - 1)], col_sent)

    @pl.when(pools)
    def _():
        sent(colsend.at[pl.ds(0, H * B - 2 * H)], col_given)
        sent(spare.at[pl.ds(0, N - 1)], part_sent)
        came(part.at[pl.ds(0, pool_count - 1)], part_came)

    @pl.when(jnp.logical_not(pools))
    def _():
        sent(colsend, col_given)
        came(part, part_came)

    whole = jnp.sum(part[:, 0, :], axis=0, keepdims=True)
    terms_ref[2:3, 0:1] = whole[:, 0:1] / (2.0 * image_total)


def hand_out(terms_ref, closs_ref, iloss_ref, loss_ref):
    closs_ref[...] = terms_ref[0:1, :]
    iloss_ref[...] = terms_ref[1:2, :]
    loss_ref[...] = terms_ref[2:3, 0:1]


def local(blk, rep, captions, images, positives, valid):
    n, width = captions.shape
    U, V = grid_of(blk, rep)
    N = blk * rep
    H, B = U // 2, V * 2
    C = H * B * n
    packed = 3 * pl.cdiv(n, LANES) * LANES
    f32, i32 = jnp.float32, jnp.int32
    _, _, image_sems, caption_sems = semaphore_counts(U, V, rep)
    dma = lambda count: pltpu.SemaphoreType.DMA((count,))
    vmem = pl.BlockSpec(memory_space=pltpu.VMEM)
    hbm = pl.BlockSpec(memory_space=pl.ANY)
    terms = pl.pallas_call(
        functools.partial(kernel, blk, rep),
        out_shape=pltpu.VMEM((SUBLANES, n), f32),
        in_specs=[hbm] * 4,
        out_specs=vmem,
        scratch_shapes=[
            pltpu.VMEM((n, width), captions.dtype),
            pltpu.VMEM((2 * rep, n, width), captions.dtype),
            pltpu.VMEM((H * B, n, width), images.dtype),
            pltpu.VMEM((2, 1, n), i32),
            pltpu.VMEM((N, 1, n), i32),
            pltpu.VMEM((1, C), f32),
            pltpu.VMEM((1, C), i32),
            pltpu.VMEM((2 * rep, n, LANES), i32),
            pltpu.VMEM((2 * rep, n, LANES), f32),
            pltpu.VMEM((2 * rep, 1, n), f32),
            pltpu.VMEM((2 * rep, n, LANES), f32),
            pltpu.VMEM((2 * rep, n, LANES), f32),
            pltpu.VMEM((2 * rep, n, LANES), f32),
            pltpu.VMEM((SUBLANES, C), f32),
            pltpu.VMEM((SUBLANES, C), f32),
            pltpu.VMEM((SUBLANES, C), f32),
            pltpu.VMEM((2 * rep, 1, packed), f32),
            pltpu.VMEM((2 * rep, 1, packed), f32),
            pltpu.VMEM((2 * H * 2 * rep, 1, packed), f32),
            pltpu.VMEM((H * B, 1, packed), f32),
            pltpu.VMEM((H * B, 1, packed), f32),
            pltpu.VMEM((2 * H * H * B, 1, packed), f32),
            pltpu.VMEM((2 * V * rep, 1, LANES), f32),
            pltpu.VMEM((N, 1, LANES), f32),
            dma(5), dma(image_sems), dma(caption_sems), dma(9), dma(7),
        ],
        compiler_params=pltpu.CompilerParams(collective_id=0, has_side_effects=True),
    )(captions, images, positives.reshape(1, n), valid.reshape(1, n))
    caption_loss, image_loss, loss = pl.pallas_call(
        hand_out,
        out_shape=(
            jax.ShapeDtypeStruct((1, n), f32),
            jax.ShapeDtypeStruct((1, n), f32),
            jax.ShapeDtypeStruct((1, 1), f32),
        ),
        in_specs=[vmem],
        out_specs=(vmem,) * 3,
    )(pltpu.with_memory_space_constraint(terms, pltpu.VMEM))
    return caption_loss.reshape(n), image_loss.reshape(n), loss.reshape(())


def solution(mesh):
    placed = (
        P(("blk", "rep"), None),
        P(("blk", "rep"), None),
        P(("blk", "rep")),
        P(("blk", "rep")),
    )
    return jax.shard_map(
        functools.partial(local, mesh.shape["blk"], mesh.shape["rep"]),
        mesh=mesh,
        in_specs=placed,
        out_specs=(P(("blk", "rep")), P(("blk", "rep")), P()),
        check_vma=False,
    )
```

```python
import functools
import math

import jax
import jax.numpy as jnp
from jax import lax
from jax.experimental import pallas as pl
from jax.experimental.pallas import tpu as pltpu
from jax.sharding import PartitionSpec as P

very_low = -1e30
floor = -1e29
IMAGE_PIECES = 4
CAPTION_PIECES = 6
IMAGES_HELD = 1
CAPTIONS_HELD = 2
FAR_FIRST = 2
LANES = 128
SUBLANES = 8
log2_e = math.log2(math.e)
ln_2 = math.log(2)


def grid_of(blk, rep):
    chips = (blk // 2) * rep
    planes = 1
    while (planes * 2) ** 2 <= chips and (blk // 2) % (planes * 2) == 0:
        planes *= 2
    return planes, blk // 2 // planes


def mod(a, b):
    return a & (b - 1) if b & (b - 1) == 0 else lax.rem(a, b)


def div(a, b):
    return a >> (b.bit_length() - 1) if b & (b - 1) == 0 else lax.div(a, b)


def semaphore_counts(U, V, rep):
    H = U // 2
    along = (H - 1) * IMAGE_PIECES
    across = H * (V - 1) * IMAGE_PIECES
    return along, across, along + across + H * V, 2 * CAPTION_PIECES + 2 * (rep - 1)


def group_at(V, H, di, dv):
    if di == 0:
        return dv
    if dv == 0:
        return V + di - 1
    return V + H - 1 + (di - 1) * (V - 1) + dv - 1


def kernel(
    blk, rep, cap_ref, img_ref, pos_ref, val_ref, terms_ref,
    mine, caps, imgs, raw, words, image_bias, image_ids, target, caption_bias, caption_ok,
    row_peak, row_total, row_match, col_peak, col_total, col_match,
    rowsend, rowrecv, rowpool, colsend, colrecv, colpool, part, spare,
    loc_sem, img_recv, cap_recv, send_sem, recv_sem,
):
    U, V = grid_of(blk, rep)
    N = blk * rep
    G = N // U
    H = U // 2
    B = V * 2
    n, width = cap_ref.shape
    early = V + H - 1
    C = H * B * n
    along_sems, across_sems, _, _ = semaphore_counts(U, V, rep)
    b, r = lax.axis_index("blk"), lax.axis_index("rep")
    c = mod(b, 2)
    u = div(b, 2 * V)
    v = mod(div(b, 2), V)
    me = b * rep + r
    g = mod(me, G)
    half, h = div(u, H), mod(u, H)
    keeps_own = div(u, 2) == h
    img_sent, cap_sent, line_sent, plane_sent, row_sent, col_sent, row_given, col_given, part_sent = (
        send_sem.at[k] for k in range(9)
    )
    line_came, plane_came, row_came, col_came, row_pooled, col_pooled, part_came = (
        recv_sem.at[k] for k in range(7)
    )
    pools = (c == 1) & ((u == H - 1) | (u == H))

    def pool_of(uu, vv, rr):
        return member(H - 1 + div(uu, H), vv, 1, rr)

    def near_of(uu):
        return jnp.where(uu > 2 * mod(uu, H), 1, 0)

    near = near_of(u)

    def member(uu, vv, cc, rr):
        return ((uu * V + vv) * 2 + cc) * rep + rr

    def remote(src, dst, ss, rs, to):
        return pltpu.make_async_remote_copy(
            src_ref=src, dst_ref=dst, send_sem=ss, recv_sem=rs, device_id=to,
            device_id_type=pl.DeviceIdType.LOGICAL,
        )

    partner = member(u, v, 1 - c, r)

    def sent(ref, sem):
        remote(ref, ref, sem, img_recv.at[0], partner).wait_send()

    def came(ref, sem):
        remote(ref, ref, img_sent, sem, partner).wait_recv()

    barrier = pltpu.get_barrier_semaphore()
    others = [u * G + mod(g + k, G) for k in range(1, G)]
    others += [mod(u + k, U) * G + g for k in range(1, U)]
    for to in others:
        pl.semaphore_signal(
            barrier, inc=1, device_id=to, device_id_type=pl.DeviceIdType.LOGICAL
        )

    def group(di, dv):
        return group_at(V, H, di, dv)

    offsets = sorted((group(di, dv), di, dv) for di in range(H) for dv in range(V))

    def image_member(di, dv, k):
        return member(half * H + mod(h + di, H), mod(v + dv, V), c if k == 0 else 1 - c, r)

    load_val = pltpu.make_async_copy(val_ref, raw.at[0], loc_sem.at[0])
    load_pos = pltpu.make_async_copy(pos_ref, raw.at[1], loc_sem.at[1])
    load_img = pltpu.make_async_copy(img_ref, imgs.at[0], loc_sem.at[2])
    load_cap = pltpu.make_async_copy(cap_ref, mine, loc_sem.at[3])
    keep_cap = pltpu.make_async_copy(cap_ref, caps.at[0], loc_sem.at[4])
    load_img.start()
    load_val.start()
    load_pos.start()
    load_cap.start()

    @pl.when(keeps_own)
    def _():
        keep_cap.start()

    load_val.wait()
    load_pos.wait()
    words[g * U + u] = raw[1] * 2 + raw[0]
    load_img.wait()

    pl.semaphore_wait(barrier, len(others))

    def image_rows(k):
        return pl.ds(k * (n // IMAGE_PIECES), n // IMAGE_PIECES)

    def caption_rows(k):
        return pl.ds(k * (n // CAPTION_PIECES), n // CAPTION_PIECES)

    def img_copy(at, to_at, k, sem, to):
        rows = image_rows(k)
        return remote(imgs.at[at, rows], imgs.at[to_at, rows], img_sent, img_recv.at[sem], to)

    def across_sem(di, dv, k):
        return along_sems + (di * (V - 1) + dv - 1) * IMAGE_PIECES + k

    def img_along(d, k):
        to = member(half * H + mod(h + d, H), v, c, r)
        return img_copy(0, group(H - d, 0) * 2, k, (H - d - 1) * IMAGE_PIECES + k, to)

    def img_across(di, d, k):
        to = member(u, mod(v + d, V), c, r)
        return img_copy(
            group(di, 0) * 2, group(di, V - d) * 2, k, across_sem(di, V - d, k), to
        )

    def img_beside(di, dv, k):
        at = group(di, dv)
        return img_copy(at * 2, at * 2 + 1, k, along_sems + across_sems + at, partner)

    def along_came(di, k):
        came(imgs.at[group(di, 0) * 2, image_rows(k)], img_recv.at[(di - 1) * IMAGE_PIECES + k])

    def across_came(di, dv, k):
        came(imgs.at[group(di, dv) * 2, image_rows(k)], img_recv.at[across_sem(di, dv, k)])

    def beside_came(at):
        came(imgs.at[at * 2 + 1], img_recv.at[along_sems + across_sems + at])

    def cap_along(t, k):
        rows = caption_rows(k)
        to = t * H + div(u, 2)
        away = jnp.where(mod(u, 2) == near_of(to), 0, 1)
        return remote(
            mine.at[rows], caps.at[away * rep, rows], cap_sent,
            cap_recv.at[away * CAPTION_PIECES + k], member(to, v, c, r),
        )

    def cap_across(away, d, k, block=None):
        rows = caption_rows(k)
        seat = rep - d
        sem = 2 * CAPTION_PIECES + away * (rep - 1) + seat - 1
        return remote(
            (caps.at[away * rep] if block is None else block).at[rows],
            caps.at[away * rep + seat, rows], cap_sent,
            cap_recv.at[sem], member(u, v, c, mod(r + d, rep)),
        )

    def relay_captions(away, k):
        came(caps.at[away * rep, caption_rows(k)], cap_recv.at[away * CAPTION_PIECES + k])
        for d in range(1, rep):
            cap_across(away, d, k).start()

    def line_copy(k):
        row = words.at[g * U + u]
        return remote(row, row, line_sent, line_came, mod(u + k, U) * G + g)

    def plane_copy(k):
        rows = words.at[pl.ds(g * U, U)]
        return remote(rows, rows, plane_sent, plane_came, u * G + mod(g + k, G))

    def own_across(k):
        for d in range(1, V):
            img_across(0, d, k).start()

    def own_captions_across(k):
        @pl.when(keeps_own)
        def _():
            for d in range(1, rep):
                cap_across(0, d, k, mine).start()

    for k in range(1, U):
        line_copy(k).start()
    for k in range(IMAGE_PIECES):
        for d in range(1, H):
            img_along(d, k).start()
        if k < IMAGE_PIECES - IMAGES_HELD:
            own_across(k)
        img_beside(0, 0, k).start()
    load_cap.wait()
    for k in range(CAPTION_PIECES):
        for t in range(2):
            @pl.when(t * H + div(u, 2) != u)
            def _():
                cap_along(t, k).start()
        if k < CAPTION_PIECES - CAPTIONS_HELD:
            own_captions_across(k)

    for at, di, dv in offsets:
        for k in range(2):
            cols = slice((at * 2 + k) * n, (at * 2 + k + 1) * n)
            first = image_member(di, dv, k) * n
            image_ids[:, cols] = first + lax.broadcasted_iota(jnp.int32, (1, n), 1)
    col_peak[...] = jnp.full(col_peak.shape, floor, jnp.float32)
    col_total[...] = jnp.zeros(col_total.shape, jnp.float32)
    col_match[...] = jnp.zeros(col_match.shape, jnp.float32)
    row_peak[...] = jnp.full(row_peak.shape, floor, jnp.float32)
    row_total[...] = jnp.zeros(row_total.shape, jnp.float32)
    row_match[...] = jnp.zeros(row_match.shape, jnp.float32)

    def relay_along(k):
        for di in range(1, H):
            along_came(di, k)
            for d in range(1, V):
                img_across(di, d, k).start()
            img_beside(di, 0, k).start()

    def relay_own(k):
        for dv in range(1, V):
            across_came(0, dv, k)
            img_beside(0, dv, k).start()

    def relay_late(k):
        for di in range(1, H):
            for dv in range(1, V):
                across_came(di, dv, k)
                img_beside(di, dv, k).start()

    def late_pieces(first, stop):
        for k in range(min(first, IMAGE_PIECES), min(stop, IMAGE_PIECES)):
            relay_late(k)

    def far_pieces(first, stop):
        for k in range(first, stop):
            relay_far(k)

    def relay_near(k):
        @pl.when(jnp.logical_not(keeps_own))
        def _():
            relay_captions(0, k)

    def relay_far(k):
        relay_captions(1, k)

    def relay_far_early(k):
        pl.when(keeps_own)(functools.partial(relay_far, k))

    relay_near(0)

    came(words.at[pl.ds(0, U - 1)], line_came)
    for k in range(1, G):
        plane_copy(k).start()
    for k in range(IMAGE_PIECES - IMAGES_HELD, IMAGE_PIECES):
        own_across(k)
    for k in range(CAPTION_PIECES - CAPTIONS_HELD, CAPTION_PIECES):
        own_captions_across(k)

    relays = [((k + 1) / IMAGE_PIECES, 0, relay_along, k) for k in range(IMAGE_PIECES)]
    relays += [((k + 1) / IMAGE_PIECES + 0.12, 1, relay_own, k) for k in range(IMAGE_PIECES)]
    relays += [((k + 1) / CAPTION_PIECES, 2, relay_near, k) for k in range(1, CAPTION_PIECES)]
    relays += [(1.02 + k / CAPTION_PIECES, 3, relay_far_early, k) for k in range(FAR_FIRST)]
    for _, _, relay, k in sorted(relays, key=lambda x: x[:2]):
        relay(k)

    came(words.at[pl.ds(0, (G - 1) * U)], plane_came)

    eye = lax.broadcasted_iota(jnp.int32, (n, n), 0) == lax.broadcasted_iota(jnp.int32, (n, n), 1)

    def to_column(row):
        return jnp.sum(jnp.where(eye, row, 0.0), axis=1, keepdims=True)

    def to_row(column):
        return jnp.sum(jnp.where(eye, column, 0.0), axis=0, keepdims=True)

    flags = (words[:, 0, :] & 1).astype(jnp.float32)
    image_total = jnp.sum(jnp.sum(flags, axis=1, keepdims=True), axis=0, keepdims=True)

    def seat_row(s):
        away, d = div(s, rep), mod(s, rep)
        uu = 2 * h + jnp.where(away == 0, near, 1 - near)
        return ((v * 2 + c) * rep + mod(r + d, rep)) * U + uu

    aims = [words[seat_row(s)] >> 1 for s in range(2 * rep)]
    aim = jnp.concatenate(aims, axis=1)
    order = lax.broadcasted_iota(jnp.int32, (N, aim.shape[1]), 0)
    starts = (mod(order, U) * G + div(order, U)) * n
    inside = (aim >= starts) & (aim < starts + n)
    picked = jnp.dot(
        flags.T.astype(jnp.bfloat16), jnp.where(inside, 1.0, 0.0).astype(jnp.bfloat16),
        preferred_element_type=jnp.float32,
    )
    start = jnp.sum(jnp.where(inside, starts, 0).astype(jnp.float32), axis=0, keepdims=True)
    low = aim - start.astype(jnp.int32)
    depth = lax.broadcasted_iota(jnp.int32, picked.shape, 0)
    ok = jnp.sum(jnp.where(depth == low, picked, 0.0), axis=0, keepdims=True)
    for s in range(2 * rep):
        ok_row = ok[:, s * n : (s + 1) * n]
        caption_ok[s] = ok_row
        bias = to_column(jnp.where(ok_row > 0, 0.0, very_low))
        caption_bias[s] = jnp.broadcast_to(bias, (n, LANES))
        aim_column = to_column(aims[s].astype(jnp.float32)).astype(jnp.int32)
        target[s] = jnp.broadcast_to(aim_column, (n, LANES))
    for at, di, dv in offsets:
        for k in range(2):
            to = image_member(di, dv, k)
            flag = words[mod(to, G) * U + div(to, G)] & 1
            cols = slice((at * 2 + k) * n, (at * 2 + k + 1) * n)
            image_bias[:, cols] = jnp.where(flag > 0, 0.0, very_low)

    def fold(x, op):
        y = x[:, :LANES]
        for j in range(1, x.shape[1] // LANES):
            y = op(y, x[:, j * LANES : (j + 1) * LANES])
        return y

    def tally(s, cols, scores, first, rows):
        scaled = scores * log2_e + image_bias[:, cols]
        ids = image_ids[:, cols]
        old_peak = col_peak[:, cols]
        peak, match = old_peak, col_match[:, cols]
        wide = lambda x: jnp.concatenate([x] * (scores.shape[1] // LANES), axis=1)
        held, peaks = [], []
        for q in range(rows // SUBLANES):
            at = pl.ds(first + q * SUBLANES, SUBLANES)
            x = scaled[q * SUBLANES : (q + 1) * SUBLANES] + wide(caption_bias[s, at])
            held.append(x)
            peaks.append(jnp.maximum(fold(x, jnp.maximum), row_peak[s, at]))
            peak = jnp.maximum(peak, x)
            picked = jnp.where(wide(target[s, at]) == ids, x, 0.0)
            row_match[s, at] = row_match[s, at] + fold(picked, jnp.add)
            match = match + picked
        total = col_total[:, cols] * jnp.exp2(old_peak - peak)
        for q in range(rows // SUBLANES):
            at = pl.ds(first + q * SUBLANES, SUBLANES)
            powers = jnp.exp2(held[q] - wide(peaks[q]))
            row_total[s, at] = row_total[s, at] * jnp.exp2(row_peak[s, at] - peaks[q]) + fold(
                powers, jnp.add
            )
            row_peak[s, at] = peaks[q]
            total = total + jnp.exp2(held[q] - peak)
        col_peak[:, cols] = peak
        col_total[:, cols] = total
        col_match[:, cols] = match

    def score(s, count, start, stop, first, rows):
        left = caps[pl.ds(s, count), pl.ds(first, rows)].reshape(count * rows, width)
        for at in range(start, stop):
            scores = lax.dot_general(
                left, imgs[2 * at : 2 * at + 2].reshape(2 * n, width), (((1,), (1,)), ((), ())),
                preferred_element_type=jnp.float32,
            )
            cols = slice(2 * at * n, 2 * (at + 1) * n)
            for k in range(count):
                tally(s + k, cols, scores[k * rows : (k + 1) * rows], first, rows)

    @pl.when(keeps_own)
    def _():
        keep_cap.wait()

    @pl.when(keeps_own)
    def _():
        far_pieces(FAR_FIRST, FAR_FIRST + 1)

    @pl.when(jnp.logical_not(keeps_own))
    def _():
        far_pieces(0, 1)

    for at in range(early):
        beside_came(at)

    @pl.loop(0, rep)
    def _(e):
        for step in range(rep):
            @pl.when(e == step)
            def _():
                @pl.when(keeps_own)
                def _():
                    if step:
                        late_pieces(step - 1, step)
                    far_pieces(FAR_FIRST + 1 + step, FAR_FIRST + 2 + step)

                @pl.when(jnp.logical_not(keeps_own))
                def _():
                    far_pieces(1 + step, 2 + step)

        @pl.when(e > 0)
        def _():
            came(caps.at[0], cap_recv.at[2 * CAPTION_PIECES + e - 1])
        score(e, 1, 0, early, 0, n)

    @pl.when(keeps_own)
    def _():
        late_pieces(rep - 1, rep)
        far_pieces(FAR_FIRST + 1 + rep, CAPTION_PIECES)

    @pl.when(jnp.logical_not(keeps_own))
    def _():
        far_pieces(1 + rep, CAPTION_PIECES - 2)

    upper = n // CAPTION_PIECES * (CAPTION_PIECES - 2)
    score(rep, 1, 0, early, 0, upper)

    @pl.when(keeps_own)
    def _():
        late_pieces(rep, IMAGE_PIECES)

    @pl.when(jnp.logical_not(keeps_own))
    def _():
        late_pieces(0, IMAGE_PIECES - 2)
        far_pieces(CAPTION_PIECES - 2, CAPTION_PIECES - 1)
        late_pieces(IMAGE_PIECES - 2, IMAGE_PIECES)
        far_pieces(CAPTION_PIECES - 1, CAPTION_PIECES)

    score(rep, 1, 0, early, upper, n - upper)

    for at in range(early, H * V):
        beside_came(at)
    score(0, rep + 1, early, H * V, 0, n)

    stride = pl.cdiv(n, LANES) * LANES

    sums = slice(0, 2 * stride)

    def pack(ref, at, ok, first, peak, total, match):
        ref[at, :, 0:n] = jnp.where(ok, peak, 0.0)
        ref[at, :, stride : stride + n] = jnp.where(ok, total, jnp.where(first, 1.0, 0.0))
        ref[at, :, 2 * stride : 2 * stride + n] = jnp.where(ok, match, 0.0)

    def pack_rows(s):
        peak = jnp.max(row_peak[s], axis=1, keepdims=True)
        total = jnp.sum(row_total[s] * jnp.exp2(row_peak[s] - peak), axis=1, keepdims=True)
        match = jnp.sum(row_match[s], axis=1, keepdims=True)
        pack(
            rowsend, s, caption_ok[s] > 0, half * rep + r == 0, to_row(peak), to_row(total),
            to_row(match),
        )

    def row_place(s):
        away, d = s // rep, s % rep
        uu = 2 * h + (near if away == 0 else 1 - near)
        return uu, mod(r + d, rep)

    def pool_rows(s):
        uu, rr = row_place(s)
        at = (mod(uu, H) * 2 + c) * 2 * rep + half * rep + r
        remote(
            rowsend.at[s], rowpool.at[at], row_given, row_pooled,
            pool_of(uu, v, mod(rr + 1, rep)),
        ).start()

    def send_rows(s):
        uu, rr = row_place(s)
        at = half * rep + r

        def go():
            remote(
                rowsend.at[s], rowrecv.at[at], row_sent, row_came, member(uu, v, c, rr)
            ).start()

        if s:
            go()
        else:
            pl.when(jnp.logical_not(keeps_own))(go)

            @pl.when(keeps_own)
            def _():
                rowrecv[at] = rowsend[s]

    for s in range(rep + 1):
        pack_rows(s)
    for s in range(rep + 1):
        pool_rows(s)
        send_rows(s)

    @pl.loop(1, rep)
    def _(d):
        came(caps.at[rep + d], cap_recv.at[2 * CAPTION_PIECES + rep - 1 + d - 1])
        score(rep + d, 1, 0, H * V, 0, n)

    for s in range(rep + 1, 2 * rep):
        pack_rows(s)
    peak = jnp.max(col_peak[...], axis=0, keepdims=True)
    total = jnp.sum(col_total[...] * jnp.exp2(col_peak[...] - peak), axis=0, keepdims=True)
    match = jnp.sum(col_match[...], axis=0, keepdims=True)
    for at, di, dv in offsets:
        for k in range(2):
            slot = at * 2 + k
            cols = slice(slot * n, (slot + 1) * n)
            back = group((H - di) % H, (V - dv) % V) * 2 + k
            pack(
                colsend, slot, image_bias[:, cols] == 0, back == 0, peak[:, cols], total[:, cols],
                match[:, cols],
            )
    for s in range(rep + 1, 2 * rep):
        pool_rows(s)
    for at, di, dv in reversed(offsets):
        for k in range(2):
            slot = at * 2 + k
            back = group((H - di) % H, (V - dv) % V) * 2 + k
            cc = c if k == 0 else 1 - c
            seat = (mod(h + di, H) * 2 + cc) * H * B + back

            def give():
                remote(
                    colsend.at[slot, :, sums], colpool.at[seat], col_given, col_pooled,
                    pool_of(u, mod(v + dv, V), r),
                ).start()

            if dv:
                give()
            else:
                @pl.when(pools)
                def _():
                    colpool[seat] = colsend[slot, :, sums]

                pl.when(jnp.logical_not(pools))(give)
    for s in range(rep + 1, 2 * rep):
        send_rows(s)
    for at, di, dv in reversed(offsets):
        for k in range(2):
            slot = at * 2 + k
            if slot:
                back = group((H - di) % H, (V - dv) % V) * 2 + k
                remote(
                    colsend.at[slot], colrecv.at[back], col_sent, col_came,
                    image_member(di, dv, k),
                ).start()
    colrecv[0] = colsend[0]

    def joined(parts, first, count, matches=1):
        piece = lambda s, k: parts[first + s, :, k * stride : k * stride + n]
        peak = piece(0, 0)
        for s in range(1, count):
            peak = jnp.maximum(peak, piece(s, 0))
        total = jnp.zeros_like(peak)
        match = jnp.zeros_like(peak)
        for s in range(count):
            total += piece(s, 1) * jnp.exp2(piece(s, 0) - peak)
            if matches:
                match += piece(s, 2)
        return (peak - matches * match) * ln_2 + jnp.log(total)

    pool_count = 2 * V * rep
    own_pool = (half * V + v) * rep + r

    @pl.when(pools)
    def _():
        came(rowpool, row_pooled)
        whole = jnp.zeros((1, n), jnp.float32)
        for k in range(2 * H):
            whole += joined(rowpool, k * 2 * rep, 2 * rep, 2)
        came(colpool.at[pl.ds(0, 2 * H * (H * B - 1))], col_pooled)
        for k in range(2 * H):
            whole += joined(colpool, k * H * B, H * B, 0)
        part[own_pool] = jnp.broadcast_to(jnp.sum(whole, axis=1, keepdims=True), (1, LANES))

        @pl.loop(0, N)
        def _(k):
            uu = div(k, G)
            to = jnp.where(u < H, U - 1 - uu, uu) * G + mod(k, G)

            @pl.when(to != me)
            def _():
                remote(part.at[own_pool], part.at[own_pool], part_sent, part_came, to).start()

    @pl.when(keeps_own)
    def _():
        came(rowrecv.at[pl.ds(0, 2 * rep - 1)], row_came)

    @pl.when(jnp.logical_not(keeps_own))
    def _():
        came(rowrecv, row_came)

    terms_ref[0:1, :] = joined(rowrecv, 0, 2 * rep)
    came(colrecv.at[pl.ds(0, H * B - 1)], col_came)
    terms_ref[1:2, :] = joined(colrecv, 0, H * B)

    sent(words.at[pl.ds(0, U - 1)], line_sent)
    sent(words.at[pl.ds(0, (G - 1) * U)], plane_sent)
    sent(imgs.at[pl.ds(0, H * B - 1)], img_sent)

    @pl.when(keeps_own)
    def _():
        sent(caps.at[pl.ds(0, 2 * rep - 1)], cap_sent)
        sent(rowsend.at[pl.ds(0, 2 * rep - 1)], row_sent)

    @pl.when(jnp.logical_not(keeps_own))
    def _():
        sent(caps, cap_sent)
        sent(rowsend, row_sent)

    sent(rowsend, row_given)
    sent(colsend.at[pl.ds(0, H * B - 1)], col_sent)

    @pl.when(pools)
    def _():
        sent(colsend.at[pl.ds(0, H * B - 2 * H), :, sums], col_given)
        sent(spare.at[pl.ds(0, N - 1)], part_sent)
        came(part.at[pl.ds(0, pool_count - 1)], part_came)

    @pl.when(jnp.logical_not(pools))
    def _():
        sent(colsend.at[:, :, sums], col_given)
        came(part, part_came)

    whole = jnp.sum(part[:, 0, :], axis=0, keepdims=True)
    terms_ref[2:3, 0:1] = whole[:, 0:1] / (2.0 * image_total)


def hand_out(terms_ref, closs_ref, iloss_ref, loss_ref):
    closs_ref[...] = terms_ref[0:1, :]
    iloss_ref[...] = terms_ref[1:2, :]
    loss_ref[...] = terms_ref[2:3, 0:1]


def local(blk, rep, captions, images, positives, valid):
    n, width = captions.shape
    U, V = grid_of(blk, rep)
    N = blk * rep
    H, B = U // 2, V * 2
    C = H * B * n
    packed = 3 * pl.cdiv(n, LANES) * LANES
    f32, i32 = jnp.float32, jnp.int32
    _, _, image_sems, caption_sems = semaphore_counts(U, V, rep)
    dma = lambda count: pltpu.SemaphoreType.DMA((count,))
    vmem = pl.BlockSpec(memory_space=pltpu.VMEM)
    hbm = pl.BlockSpec(memory_space=pl.ANY)
    terms = pl.pallas_call(
        functools.partial(kernel, blk, rep),
        out_shape=pltpu.VMEM((SUBLANES, n), f32),
        in_specs=[hbm] * 4,
        out_specs=vmem,
        scratch_shapes=[
            pltpu.VMEM((n, width), captions.dtype),
            pltpu.VMEM((2 * rep, n, width), captions.dtype),
            pltpu.VMEM((H * B, n, width), images.dtype),
            pltpu.VMEM((2, 1, n), i32),
            pltpu.VMEM((N, 1, n), i32),
            pltpu.VMEM((1, C), f32),
            pltpu.VMEM((1, C), i32),
            pltpu.VMEM((2 * rep, n, LANES), i32),
            pltpu.VMEM((2 * rep, n, LANES), f32),
            pltpu.VMEM((2 * rep, 1, n), f32),
            pltpu.VMEM((2 * rep, n, LANES), f32),
            pltpu.VMEM((2 * rep, n, LANES), f32),
            pltpu.VMEM((2 * rep, n, LANES), f32),
            pltpu.VMEM((SUBLANES, C), f32),
            pltpu.VMEM((SUBLANES, C), f32),
            pltpu.VMEM((SUBLANES, C), f32),
            pltpu.VMEM((2 * rep, 1, packed), f32),
            pltpu.VMEM((2 * rep, 1, packed), f32),
            pltpu.VMEM((2 * H * 2 * rep, 1, packed), f32),
            pltpu.VMEM((H * B, 1, packed), f32),
            pltpu.VMEM((H * B, 1, packed), f32),
            pltpu.VMEM((2 * H * H * B, 1, packed // 3 * 2), f32),
            pltpu.VMEM((2 * V * rep, 1, LANES), f32),
            pltpu.VMEM((N, 1, LANES), f32),
            dma(5), dma(image_sems), dma(caption_sems), dma(9), dma(7),
        ],
        compiler_params=pltpu.CompilerParams(collective_id=0, has_side_effects=True),
    )(captions, images, positives.reshape(1, n), valid.reshape(1, n))
    caption_loss, image_loss, loss = pl.pallas_call(
        hand_out,
        out_shape=(
            jax.ShapeDtypeStruct((1, n), f32),
            jax.ShapeDtypeStruct((1, n), f32),
            jax.ShapeDtypeStruct((1, 1), f32),
        ),
        in_specs=[vmem],
        out_specs=(vmem,) * 3,
    )(pltpu.with_memory_space_constraint(terms, pltpu.VMEM))
    return caption_loss.reshape(n), image_loss.reshape(n), loss.reshape(())


def solution(mesh):
    placed = (
        P(("blk", "rep"), None),
        P(("blk", "rep"), None),
        P(("blk", "rep")),
        P(("blk", "rep")),
    )
    return jax.shard_map(
        functools.partial(local, mesh.shape["blk"], mesh.shape["rep"]),
        mesh=mesh,
        in_specs=placed,
        out_specs=(P(("blk", "rep")), P(("blk", "rep")), P()),
        check_vma=False,
    )
```

```python
import functools
import math

import jax
import jax.numpy as jnp
from jax import lax
from jax.experimental import pallas as pl
from jax.experimental.pallas import tpu as pltpu
from jax.sharding import PartitionSpec as P

very_low = -1e30
floor = -1e29
IMAGE_PIECES = 3
CAPTION_PIECES = 6
IMAGES_HELD = 1
CAPTIONS_HELD = 2
FAR_FIRST = 2
LANES = 128
SUBLANES = 8
log2_e = math.log2(math.e)
ln_2 = math.log(2)


def grid_of(blk, rep):
    chips = (blk // 2) * rep
    planes = 1
    while (planes * 2) ** 2 <= chips and (blk // 2) % (planes * 2) == 0:
        planes *= 2
    return planes, blk // 2 // planes


def mod(a, b):
    return a & (b - 1) if b & (b - 1) == 0 else lax.rem(a, b)


def div(a, b):
    return a >> (b.bit_length() - 1) if b & (b - 1) == 0 else lax.div(a, b)


def semaphore_counts(U, V, rep):
    H = U // 2
    along = (H - 1) * IMAGE_PIECES
    across = H * (V - 1) * IMAGE_PIECES
    return along, across, along + across + H * V, 2 * CAPTION_PIECES + 2 * (rep - 1)


def group_at(V, H, di, dv):
    if di == 0:
        return dv
    if dv == 0:
        return V + di - 1
    return V + H - 1 + (di - 1) * (V - 1) + dv - 1


def kernel(
    blk, rep, cap_ref, img_ref, pos_ref, val_ref, terms_ref,
    mine, caps, imgs, raw, words, image_bias, image_ids, target, caption_bias, caption_ok,
    row_peak, row_total, row_match, col_peak, col_total, col_match,
    rowsend, rowrecv, rowpool, colsend, colrecv, colpool, part, spare,
    loc_sem, img_recv, cap_recv, send_sem, recv_sem,
):
    U, V = grid_of(blk, rep)
    N = blk * rep
    G = N // U
    H = U // 2
    B = V * 2
    n, width = cap_ref.shape
    early = V + H - 1
    C = H * B * n
    along_sems, across_sems, _, _ = semaphore_counts(U, V, rep)
    b, r = lax.axis_index("blk"), lax.axis_index("rep")
    c = mod(b, 2)
    u = div(b, 2 * V)
    v = mod(div(b, 2), V)
    me = b * rep + r
    g = mod(me, G)
    half, h = div(u, H), mod(u, H)
    keeps_own = div(u, 2) == h
    img_sent, cap_sent, words_sent, row_sent, col_sent, col_given, part_sent = (
        send_sem.at[k] for k in range(7)
    )
    line_came, plane_came, row_came, col_came, row_pooled, col_pooled, part_came = (
        recv_sem.at[k] for k in range(7)
    )
    pools = (c == 1) & ((u == H - 1) | (u == H))

    def pool_of(uu, vv, rr):
        return member(H - 1 + div(uu, H), vv, 1, rr)

    def near_of(uu):
        return jnp.where(uu > 2 * mod(uu, H), 1, 0)

    near = near_of(u)

    def member(uu, vv, cc, rr):
        return ((uu * V + vv) * 2 + cc) * rep + rr

    def remote(src, dst, ss, rs, to):
        return pltpu.make_async_remote_copy(
            src_ref=src, dst_ref=dst, send_sem=ss, recv_sem=rs, device_id=to,
            device_id_type=pl.DeviceIdType.LOGICAL,
        )

    partner = member(u, v, 1 - c, r)

    def sent(ref, sem):
        remote(ref, ref, sem, img_recv.at[0], partner).wait_send()

    def came(ref, sem):
        remote(ref, ref, img_sent, sem, partner).wait_recv()

    barrier = pltpu.get_barrier_semaphore()
    others = [u * G + mod(g + k, G) for k in range(1, G)]
    others += [mod(u + k, U) * G + g for k in range(1, U)]
    for to in others:
        pl.semaphore_signal(
            barrier, inc=1, device_id=to, device_id_type=pl.DeviceIdType.LOGICAL
        )

    def group(di, dv):
        return group_at(V, H, di, dv)

    offsets = sorted((group(di, dv), di, dv) for di in range(H) for dv in range(V))

    def image_member(di, dv, k):
        return member(half * H + mod(h + di, H), mod(v + dv, V), c if k == 0 else 1 - c, r)

    load_val = pltpu.make_async_copy(val_ref, raw.at[0], loc_sem.at[0])
    load_pos = pltpu.make_async_copy(pos_ref, raw.at[1], loc_sem.at[1])
    load_img = pltpu.make_async_copy(img_ref, imgs.at[0], loc_sem.at[2])
    load_cap = pltpu.make_async_copy(cap_ref, mine, loc_sem.at[3])
    keep_cap = pltpu.make_async_copy(cap_ref, caps.at[0], loc_sem.at[4])
    load_img.start()
    load_val.start()
    load_pos.start()
    load_cap.start()

    @pl.when(keeps_own)
    def _():
        keep_cap.start()

    load_val.wait()
    load_pos.wait()
    words[g * U + u] = raw[1] * 2 + raw[0]
    load_img.wait()

    pl.semaphore_wait(barrier, len(others))

    def image_rows(k):
        return pl.ds(k * (n // IMAGE_PIECES), n // IMAGE_PIECES)

    def caption_rows(k):
        return pl.ds(k * (n // CAPTION_PIECES), n // CAPTION_PIECES)

    def img_copy(at, to_at, k, sem, to):
        rows = image_rows(k)
        return remote(imgs.at[at, rows], imgs.at[to_at, rows], img_sent, img_recv.at[sem], to)

    def across_sem(di, dv, k):
        return along_sems + (di * (V - 1) + dv - 1) * IMAGE_PIECES + k

    def img_along(d, k):
        to = member(half * H + mod(h + d, H), v, c, r)
        return img_copy(0, group(H - d, 0) * 2, k, (H - d - 1) * IMAGE_PIECES + k, to)

    def img_across(di, d, k):
        to = member(u, mod(v + d, V), c, r)
        return img_copy(
            group(di, 0) * 2, group(di, V - d) * 2, k, across_sem(di, V - d, k), to
        )

    def img_beside(di, dv, k):
        at = group(di, dv)
        return img_copy(at * 2, at * 2 + 1, k, along_sems + across_sems + at, partner)

    def along_came(di, k):
        came(imgs.at[group(di, 0) * 2, image_rows(k)], img_recv.at[(di - 1) * IMAGE_PIECES + k])

    def across_came(di, dv, k):
        came(imgs.at[group(di, dv) * 2, image_rows(k)], img_recv.at[across_sem(di, dv, k)])

    def beside_came(at):
        came(imgs.at[at * 2 + 1], img_recv.at[along_sems + across_sems + at])

    def cap_along(t, k):
        rows = caption_rows(k)
        to = t * H + div(u, 2)
        away = jnp.where(mod(u, 2) == near_of(to), 0, 1)
        return remote(
            mine.at[rows], caps.at[away * rep, rows], cap_sent,
            cap_recv.at[away * CAPTION_PIECES + k], member(to, v, c, r),
        )

    def cap_across(away, d, k, block=None):
        rows = caption_rows(k)
        seat = rep - d
        sem = 2 * CAPTION_PIECES + away * (rep - 1) + seat - 1
        return remote(
            (caps.at[away * rep] if block is None else block).at[rows],
            caps.at[away * rep + seat, rows], cap_sent,
            cap_recv.at[sem], member(u, v, c, mod(r + d, rep)),
        )

    def relay_captions(away, k):
        came(caps.at[away * rep, caption_rows(k)], cap_recv.at[away * CAPTION_PIECES + k])
        for d in range(1, rep):
            cap_across(away, d, k).start()

    def line_copy(k):
        row = words.at[g * U + u]
        return remote(row, row, words_sent, line_came, mod(u + k, U) * G + g)

    def plane_copy(k):
        rows = words.at[pl.ds(g * U, U)]
        return remote(rows, rows, words_sent, plane_came, u * G + mod(g + k, G))

    def own_across(k):
        for d in range(1, V):
            img_across(0, d, k).start()

    def own_captions_across(k):
        @pl.when(keeps_own)
        def _():
            for d in range(1, rep):
                cap_across(0, d, k, mine).start()

    for k in range(1, U):
        line_copy(k).start()
    for k in range(IMAGE_PIECES):
        for d in range(1, H):
            img_along(d, k).start()
        if k < IMAGE_PIECES - IMAGES_HELD:
            own_across(k)
        img_beside(0, 0, k).start()
    load_cap.wait()
    for k in range(CAPTION_PIECES):
        for t in range(2):
            @pl.when(t * H + div(u, 2) != u)
            def _():
                cap_along(t, k).start()
        if k < CAPTION_PIECES - CAPTIONS_HELD:
            own_captions_across(k)

    for at, di, dv in offsets:
        for k in range(2):
            cols = slice((at * 2 + k) * n, (at * 2 + k + 1) * n)
            first = image_member(di, dv, k) * n
            image_ids[:, cols] = first + lax.broadcasted_iota(jnp.int32, (1, n), 1)
    col_peak[...] = jnp.full(col_peak.shape, floor, jnp.float32)
    col_total[...] = jnp.zeros(col_total.shape, jnp.float32)
    col_match[...] = jnp.zeros(col_match.shape, jnp.float32)
    row_peak[...] = jnp.full(row_peak.shape, floor, jnp.float32)
    row_total[...] = jnp.zeros(row_total.shape, jnp.float32)
    row_match[...] = jnp.zeros(row_match.shape, jnp.float32)

    def relay_along(k):
        for di in range(1, H):
            along_came(di, k)
            for d in range(1, V):
                img_across(di, d, k).start()
            img_beside(di, 0, k).start()

    def relay_own(k):
        for dv in range(1, V):
            across_came(0, dv, k)
            img_beside(0, dv, k).start()

    def relay_late(k):
        for di in range(1, H):
            for dv in range(1, V):
                across_came(di, dv, k)
                img_beside(di, dv, k).start()

    def late_pieces(first, stop):
        for k in range(min(first, IMAGE_PIECES), min(stop, IMAGE_PIECES)):
            relay_late(k)

    def far_pieces(first, stop):
        for k in range(first, stop):
            relay_far(k)

    def relay_near(k):
        @pl.when(jnp.logical_not(keeps_own))
        def _():
            relay_captions(0, k)

    def relay_far(k):
        relay_captions(1, k)

    def relay_far_early(k):
        pl.when(keeps_own)(functools.partial(relay_far, k))

    relay_near(0)

    came(words.at[pl.ds(0, U - 1)], line_came)
    for k in range(1, G):
        plane_copy(k).start()
    for k in range(IMAGE_PIECES - IMAGES_HELD, IMAGE_PIECES):
        own_across(k)
    for k in range(CAPTION_PIECES - CAPTIONS_HELD, CAPTION_PIECES):
        own_captions_across(k)

    relays = [((k + 1) / IMAGE_PIECES, 0, relay_along, k) for k in range(IMAGE_PIECES)]
    relays += [((k + 1) / IMAGE_PIECES + 0.12, 1, relay_own, k) for k in range(IMAGE_PIECES)]
    relays += [((k + 1) / CAPTION_PIECES, 2, relay_near, k) for k in range(1, CAPTION_PIECES)]
    relays += [(1.02 + k / CAPTION_PIECES, 3, relay_far_early, k) for k in range(FAR_FIRST)]
    for _, _, relay, k in sorted(relays, key=lambda x: x[:2]):
        relay(k)

    came(words.at[pl.ds(0, (G - 1) * U)], plane_came)

    eye = lax.broadcasted_iota(jnp.int32, (n, n), 0) == lax.broadcasted_iota(jnp.int32, (n, n), 1)

    def to_column(row):
        return jnp.sum(jnp.where(eye, row, 0.0), axis=1, keepdims=True)

    def to_row(column):
        return jnp.sum(jnp.where(eye, column, 0.0), axis=0, keepdims=True)

    flags = (words[:, 0, :] & 1).astype(jnp.float32)
    image_total = jnp.sum(jnp.sum(flags, axis=1, keepdims=True), axis=0, keepdims=True)

    def seat_row(s):
        away, d = div(s, rep), mod(s, rep)
        uu = 2 * h + jnp.where(away == 0, near, 1 - near)
        return ((v * 2 + c) * rep + mod(r + d, rep)) * U + uu

    aims = [words[seat_row(s)] >> 1 for s in range(2 * rep)]
    aim = jnp.concatenate(aims, axis=1)
    order = lax.broadcasted_iota(jnp.int32, (N, aim.shape[1]), 0)
    starts = (mod(order, U) * G + div(order, U)) * n
    inside = (aim >= starts) & (aim < starts + n)
    picked = jnp.dot(
        flags.T.astype(jnp.bfloat16), jnp.where(inside, 1.0, 0.0).astype(jnp.bfloat16),
        preferred_element_type=jnp.float32,
    )
    start = jnp.sum(jnp.where(inside, starts, 0).astype(jnp.float32), axis=0, keepdims=True)
    low = aim - start.astype(jnp.int32)
    depth = lax.broadcasted_iota(jnp.int32, picked.shape, 0)
    ok = jnp.sum(jnp.where(depth == low, picked, 0.0), axis=0, keepdims=True)
    for s in range(2 * rep):
        ok_row = ok[:, s * n : (s + 1) * n]
        caption_ok[s] = ok_row
        bias = to_column(jnp.where(ok_row > 0, 0.0, very_low))
        caption_bias[s] = jnp.broadcast_to(bias, (n, LANES))
        aim_column = to_column(aims[s].astype(jnp.float32)).astype(jnp.int32)
        target[s] = jnp.broadcast_to(aim_column, (n, LANES))
    for at, di, dv in offsets:
        for k in range(2):
            to = image_member(di, dv, k)
            flag = words[mod(to, G) * U + div(to, G)] & 1
            cols = slice((at * 2 + k) * n, (at * 2 + k + 1) * n)
            image_bias[:, cols] = jnp.where(flag > 0, 0.0, very_low)

    def fold(x, op):
        y = x[:, :LANES]
        for j in range(1, x.shape[1] // LANES):
            y = op(y, x[:, j * LANES : (j + 1) * LANES])
        return y

    def tally(s, cols, scores, first, rows):
        scaled = scores * log2_e + image_bias[:, cols]
        ids = image_ids[:, cols]
        old_peak = col_peak[:, cols]
        peak, match = old_peak, col_match[:, cols]
        wide = lambda x: jnp.concatenate([x] * (scores.shape[1] // LANES), axis=1)
        held, peaks = [], []
        for q in range(rows // SUBLANES):
            at = pl.ds(first + q * SUBLANES, SUBLANES)
            x = scaled[q * SUBLANES : (q + 1) * SUBLANES] + wide(caption_bias[s, at])
            held.append(x)
            peaks.append(jnp.maximum(fold(x, jnp.maximum), row_peak[s, at]))
            peak = jnp.maximum(peak, x)
            picked = jnp.where(wide(target[s, at]) == ids, x, 0.0)
            row_match[s, at] = row_match[s, at] + fold(picked, jnp.add)
            match = match + picked
        total = col_total[:, cols] * jnp.exp2(old_peak - peak)
        for q in range(rows // SUBLANES):
            at = pl.ds(first + q * SUBLANES, SUBLANES)
            powers = jnp.exp2(held[q] - wide(peaks[q]))
            row_total[s, at] = row_total[s, at] * jnp.exp2(row_peak[s, at] - peaks[q]) + fold(
                powers, jnp.add
            )
            row_peak[s, at] = peaks[q]
            total = total + jnp.exp2(held[q] - peak)
        col_peak[:, cols] = peak
        col_total[:, cols] = total
        col_match[:, cols] = match

    def score(s, count, start, stop, first, rows):
        left = caps[pl.ds(s, count), pl.ds(first, rows)].reshape(count * rows, width)
        for at in range(start, stop):
            scores = lax.dot_general(
                left, imgs[2 * at : 2 * at + 2].reshape(2 * n, width), (((1,), (1,)), ((), ())),
                preferred_element_type=jnp.float32,
            )
            cols = slice(2 * at * n, 2 * (at + 1) * n)
            for k in range(count):
                tally(s + k, cols, scores[k * rows : (k + 1) * rows], first, rows)

    @pl.when(keeps_own)
    def _():
        keep_cap.wait()

    @pl.when(keeps_own)
    def _():
        far_pieces(FAR_FIRST, FAR_FIRST + 1)

    @pl.when(jnp.logical_not(keeps_own))
    def _():
        far_pieces(0, 1)

    for at in range(early):
        beside_came(at)

    @pl.loop(0, rep)
    def _(e):
        for step in range(rep):
            @pl.when(e == step)
            def _():
                @pl.when(keeps_own)
                def _():
                    if step:
                        late_pieces(step - 1, step)
                    far_pieces(FAR_FIRST + 1 + step, FAR_FIRST + 2 + step)

                @pl.when(jnp.logical_not(keeps_own))
                def _():
                    far_pieces(1 + step, 2 + step)

        @pl.when(e > 0)
        def _():
            came(caps.at[0], cap_recv.at[2 * CAPTION_PIECES + e - 1])
        score(e, 1, 0, early, 0, n)

    @pl.when(keeps_own)
    def _():
        late_pieces(rep - 1, rep)
        far_pieces(FAR_FIRST + 1 + rep, CAPTION_PIECES)

    @pl.when(jnp.logical_not(keeps_own))
    def _():
        far_pieces(1 + rep, CAPTION_PIECES - 2)

    upper = n // CAPTION_PIECES * (CAPTION_PIECES - 2)
    score(rep, 1, 0, early, 0, upper)

    @pl.when(keeps_own)
    def _():
        late_pieces(rep, IMAGE_PIECES)

    @pl.when(jnp.logical_not(keeps_own))
    def _():
        late_pieces(0, IMAGE_PIECES - 2)
        far_pieces(CAPTION_PIECES - 2, CAPTION_PIECES - 1)
        late_pieces(IMAGE_PIECES - 2, IMAGE_PIECES)
        far_pieces(CAPTION_PIECES - 1, CAPTION_PIECES)

    score(rep, 1, 0, early, upper, n - upper)

    for at in range(early, H * V):
        beside_came(at)
    score(0, rep + 1, early, H * V, 0, n)

    stride = pl.cdiv(n, LANES) * LANES

    sums = slice(0, 2 * stride)

    def pack(ref, at, ok, first, peak, total, match):
        ref[at, :, 0:n] = jnp.where(ok, peak, 0.0)
        ref[at, :, stride : stride + n] = jnp.where(ok, total, jnp.where(first, 1.0, 0.0))
        ref[at, :, 2 * stride : 2 * stride + n] = jnp.where(ok, match, 0.0)

    def pack_rows(s):
        peak = jnp.max(row_peak[s], axis=1, keepdims=True)
        total = jnp.sum(row_total[s] * jnp.exp2(row_peak[s] - peak), axis=1, keepdims=True)
        match = jnp.sum(row_match[s], axis=1, keepdims=True)
        pack(
            rowsend, s, caption_ok[s] > 0, half * rep + r == 0, to_row(peak), to_row(total),
            to_row(match),
        )

    def row_place(s):
        away, d = s // rep, s % rep
        uu = 2 * h + (near if away == 0 else 1 - near)
        return uu, mod(r + d, rep)

    def pool_rows(s):
        uu, rr = row_place(s)
        at = (mod(uu, H) * 2 + c) * 2 * rep + half * rep + r
        remote(
            rowsend.at[s], rowpool.at[at], row_sent, row_pooled,
            pool_of(uu, v, mod(rr + 1, rep)),
        ).start()

    def send_rows(s):
        uu, rr = row_place(s)
        at = half * rep + r

        def go():
            remote(
                rowsend.at[s], rowrecv.at[at], row_sent, row_came, member(uu, v, c, rr)
            ).start()

        if s:
            go()
        else:
            pl.when(jnp.logical_not(keeps_own))(go)

            @pl.when(keeps_own)
            def _():
                rowrecv[at] = rowsend[s]

    for s in range(rep + 1):
        pack_rows(s)
    for s in range(rep + 1):
        pool_rows(s)
        send_rows(s)

    @pl.loop(1, rep)
    def _(d):
        came(caps.at[rep + d], cap_recv.at[2 * CAPTION_PIECES + rep - 1 + d - 1])
        score(rep + d, 1, 0, H * V, 0, n)

    for s in range(rep + 1, 2 * rep):
        pack_rows(s)
    peak = jnp.max(col_peak[...], axis=0, keepdims=True)
    total = jnp.sum(col_total[...] * jnp.exp2(col_peak[...] - peak), axis=0, keepdims=True)
    match = jnp.sum(col_match[...], axis=0, keepdims=True)
    for at, di, dv in offsets:
        for k in range(2):
            slot = at * 2 + k
            cols = slice(slot * n, (slot + 1) * n)
            back = group((H - di) % H, (V - dv) % V) * 2 + k
            pack(
                colsend, slot, image_bias[:, cols] == 0, back == 0, peak[:, cols], total[:, cols],
                match[:, cols],
            )
    for s in range(rep + 1, 2 * rep):
        pool_rows(s)
    for at, di, dv in reversed(offsets):
        for k in range(2):
            slot = at * 2 + k
            back = group((H - di) % H, (V - dv) % V) * 2 + k
            cc = c if k == 0 else 1 - c
            seat = (mod(h + di, H) * 2 + cc) * H * B + back

            def give():
                remote(
                    colsend.at[slot, :, sums], colpool.at[seat], col_given, col_pooled,
                    pool_of(u, mod(v + dv, V), r),
                ).start()

            if dv:
                give()
            else:
                @pl.when(pools)
                def _():
                    colpool[seat] = colsend[slot, :, sums]

                pl.when(jnp.logical_not(pools))(give)
    for s in range(rep + 1, 2 * rep):
        send_rows(s)
    for at, di, dv in reversed(offsets):
        for k in range(2):
            slot = at * 2 + k
            if slot:
                back = group((H - di) % H, (V - dv) % V) * 2 + k
                remote(
                    colsend.at[slot], colrecv.at[back], col_sent, col_came,
                    image_member(di, dv, k),
                ).start()
    colrecv[0] = colsend[0]

    def joined(parts, first, count, matches=1):
        piece = lambda s, k: parts[first + s, :, k * stride : k * stride + n]
        peak = piece(0, 0)
        for s in range(1, count):
            peak = jnp.maximum(peak, piece(s, 0))
        total = jnp.zeros_like(peak)
        match = jnp.zeros_like(peak)
        for s in range(count):
            total += piece(s, 1) * jnp.exp2(piece(s, 0) - peak)
            if matches:
                match += piece(s, 2)
        return (peak - matches * match) * ln_2 + jnp.log(total)

    pool_count = 2 * V * rep
    own_pool = (half * V + v) * rep + r

    @pl.when(pools)
    def _():
        came(rowpool, row_pooled)
        whole = jnp.zeros((1, n), jnp.float32)
        for k in range(2 * H):
            whole += joined(rowpool, k * 2 * rep, 2 * rep, 2)
        came(colpool.at[pl.ds(0, 2 * H * (H * B - 1))], col_pooled)
        for k in range(2 * H):
            whole += joined(colpool, k * H * B, H * B, 0)
        part[own_pool] = jnp.broadcast_to(jnp.sum(whole, axis=1, keepdims=True), (1, LANES))

        @pl.loop(0, N, unroll=4)
        def _(k):
            uu = div(k, G)
            to = jnp.where(u < H, U - 1 - uu, uu) * G + mod(k, G)

            @pl.when(to != me)
            def _():
                remote(part.at[own_pool], part.at[own_pool], part_sent, part_came, to).start()

    @pl.when(keeps_own)
    def _():
        came(rowrecv.at[pl.ds(0, 2 * rep - 1)], row_came)

    @pl.when(jnp.logical_not(keeps_own))
    def _():
        came(rowrecv, row_came)

    terms_ref[0:1, :] = joined(rowrecv, 0, 2 * rep)
    came(colrecv.at[pl.ds(0, H * B - 1)], col_came)
    terms_ref[1:2, :] = joined(colrecv, 0, H * B)

    sent(words.at[pl.ds(0, N - 1)], words_sent)
    sent(imgs.at[pl.ds(0, H * B - 1)], img_sent)

    @pl.when(keeps_own)
    def _():
        sent(caps.at[pl.ds(0, 2 * rep - 1)], cap_sent)
        sent(rowpool.at[pl.ds(0, 4 * rep - 1)], row_sent)

    @pl.when(jnp.logical_not(keeps_own))
    def _():
        sent(caps, cap_sent)
        sent(rowpool.at[pl.ds(0, 4 * rep)], row_sent)

    sent(colsend.at[pl.ds(0, H * B - 1)], col_sent)

    @pl.when(pools)
    def _():
        sent(colsend.at[pl.ds(0, H * B - 2 * H), :, sums], col_given)
        sent(spare.at[pl.ds(0, N - 1)], part_sent)
        came(part.at[pl.ds(0, pool_count - 1)], part_came)

    @pl.when(jnp.logical_not(pools))
    def _():
        sent(colsend.at[:, :, sums], col_given)
        came(part, part_came)

    whole = jnp.sum(part[:, 0, :], axis=0, keepdims=True)
    terms_ref[2:3, 0:1] = whole[:, 0:1] / (2.0 * image_total)


def hand_out(terms_ref, closs_ref, iloss_ref, loss_ref):
    closs_ref[...] = terms_ref[0:1, :]
    iloss_ref[...] = terms_ref[1:2, :]
    loss_ref[...] = terms_ref[2:3, 0:1]


def local(blk, rep, captions, images, positives, valid):
    n, width = captions.shape
    U, V = grid_of(blk, rep)
    N = blk * rep
    H, B = U // 2, V * 2
    C = H * B * n
    packed = 3 * pl.cdiv(n, LANES) * LANES
    f32, i32 = jnp.float32, jnp.int32
    _, _, image_sems, caption_sems = semaphore_counts(U, V, rep)
    dma = lambda count: pltpu.SemaphoreType.DMA((count,))
    vmem = pl.BlockSpec(memory_space=pltpu.VMEM)
    hbm = pl.BlockSpec(memory_space=pl.ANY)
    terms = pl.pallas_call(
        functools.partial(kernel, blk, rep),
        out_shape=pltpu.VMEM((SUBLANES, n), f32),
        in_specs=[hbm] * 4,
        out_specs=vmem,
        scratch_shapes=[
            pltpu.VMEM((n, width), captions.dtype),
            pltpu.VMEM((2 * rep, n, width), captions.dtype),
            pltpu.VMEM((H * B, n, width), images.dtype),
            pltpu.VMEM((2, 1, n), i32),
            pltpu.VMEM((N, 1, n), i32),
            pltpu.VMEM((1, C), f32),
            pltpu.VMEM((1, C), i32),
            pltpu.VMEM((2 * rep, n, LANES), i32),
            pltpu.VMEM((2 * rep, n, LANES), f32),
            pltpu.VMEM((2 * rep, 1, n), f32),
            pltpu.VMEM((2 * rep, n, LANES), f32),
            pltpu.VMEM((2 * rep, n, LANES), f32),
            pltpu.VMEM((2 * rep, n, LANES), f32),
            pltpu.VMEM((SUBLANES, C), f32),
            pltpu.VMEM((SUBLANES, C), f32),
            pltpu.VMEM((SUBLANES, C), f32),
            pltpu.VMEM((2 * rep, 1, packed), f32),
            pltpu.VMEM((2 * rep, 1, packed), f32),
            pltpu.VMEM((2 * H * 2 * rep, 1, packed), f32),
            pltpu.VMEM((H * B, 1, packed), f32),
            pltpu.VMEM((H * B, 1, packed), f32),
            pltpu.VMEM((2 * H * H * B, 1, packed // 3 * 2), f32),
            pltpu.VMEM((2 * V * rep, 1, LANES), f32),
            pltpu.VMEM((N, 1, LANES), f32),
            dma(5), dma(image_sems), dma(caption_sems), dma(7), dma(7),
        ],
        compiler_params=pltpu.CompilerParams(collective_id=0, has_side_effects=True),
    )(captions, images, positives.reshape(1, n), valid.reshape(1, n))
    caption_loss, image_loss, loss = pl.pallas_call(
        hand_out,
        out_shape=(
            jax.ShapeDtypeStruct((1, n), f32),
            jax.ShapeDtypeStruct((1, n), f32),
            jax.ShapeDtypeStruct((1, 1), f32),
        ),
        in_specs=[vmem],
        out_specs=(vmem,) * 3,
    )(pltpu.with_memory_space_constraint(terms, pltpu.VMEM))
    return caption_loss.reshape(n), image_loss.reshape(n), loss.reshape(())


def solution(mesh):
    placed = (
        P(("blk", "rep"), None),
        P(("blk", "rep"), None),
        P(("blk", "rep")),
        P(("blk", "rep")),
    )
    return jax.shard_map(
        functools.partial(local, mesh.shape["blk"], mesh.shape["rep"]),
        mesh=mesh,
        in_specs=placed,
        out_specs=(P(("blk", "rep")), P(("blk", "rep")), P()),
        check_vma=False,
    )
```
